256 devices in a mesh: member: 16 (over x, y_hi, core), tensor: 16 (over z, y_lo).
Axes of the slice: x: 4, y: 4 (y_hi: 2, y_lo: 2; y = y_hi * 2 + y_lo), z: 8, core: 2. Of those that a mesh axis runs over, the one named last changes fastest.
Arguments:
- prompt_acts: bfloat16 [128, 5120], P(None, 'member'), may hold values from -6 to 6
- gate_weight: bfloat16 [5120, 13824], P('member', 'tensor'), may hold values from -0.078125 to 0.078125
- up_weight: bfloat16 [5120, 13824], P('member', 'tensor'), may hold values from -0.078125 to 0.078125
- down_weight: bfloat16 [13824, 5120], P('tensor', 'member'), may hold values from -0.0546875 to 0.0546875
- d_table: bfloat16 [256, 3, 4, 5120], P('member'), may hold values from -6 to 6
- f_table: bfloat16 [256, 3, 4, 13824], P('member', None, None, 'tensor'), may hold values from -6 to 6
- seeds: int32 [128], P('member'), may hold values from 0 to 15
- fitness: float32 [128], P('member'), may hold values from -6 to 6
Outputs:
- outputs: bfloat16 [128, 128, 5120], P('member', None, 'tensor')
- delta_gate: bfloat16 [5120, 13824], P('member', 'tensor')
- delta_up: bfloat16 [5120, 13824], P('member', 'tensor')
- delta_down: bfloat16 [13824, 5120], P('tensor', 'member')
The draws below stay inside these ranges and needn't reach their ends.
Inputs may be any that keep to these rules, and one draw needn't show every extreme that they name: Member m uses row (m // 8) * 16 + seeds[m] of both tables, a row in its own group's block.
All inputs are finite; a program needn't handle non-finite values.
Results may differ from the reference program's by a relative error of at most 0.025.
Values may be sent and summed in bfloat16 or wider, within the bound.
A program may use at most 128 MiB of HBM per device.

```python
import math
import jax
import jax.numpy as jnp
from jax import lax

D = 5120
FFW = 13824
RANK = 4
MEM_DEV = 8
PROMPT = 128
POP = 128
POOL_DEV = 16
POOL = 256
N_TENSOR = 16


def set_ends(array, own_key, smallest, high):
    longest = array.shape.index(max(array.shape))
    spots = []
    for shift in (0, 1):
        where = [jax.random.randint(jax.random.fold_in(own_key, axis), (), 0, length) for axis, length in enumerate(array.shape)]
        where[longest] = (where[longest] + shift) % array.shape[longest]
        spots.append(tuple(where))
    return array.at[spots[0]].set(smallest).at[spots[1]].set(high)


def level_of(stream_key, shape, pieces, smallest, largest):
    factor_of = 1.0
    for dim, shards_of in pieces:
        heights = jax.random.uniform(jax.random.fold_in(jax.random.fold_in(stream_key, 6), dim), (shards_of,), jnp.float32, smallest / len(pieces), largest / len(pieces))
        factor_of = factor_of * jnp.repeat(jnp.exp(heights), shape[dim] // shards_of).reshape((-1,) + (1,) * (len(shape) - 1 - dim))
    return factor_of


def gaussian(stream_key, dims, width, bound, pieces=(), kind=jnp.bfloat16):
    result = jax.random.normal(stream_key, dims, jnp.float32) * width
    if len(pieces) > 0:
        result = level_of(stream_key, dims, pieces, -0.22, 0.18) * result
    return jnp.clip(result, min=-bound, max=bound).astype(kind)


def setup_inputs(seed: int = 0) -> dict:
    streams_of = jax.random.split(jax.random.key(seed), 9)
    return {
        "prompt_acts": gaussian(streams_of[0], (PROMPT, D), 1.0, 6.0, ((1, 16),)),
        "gate_weight": gaussian(streams_of[1], (D, FFW), D ** -0.5, 0.078125, ((0, 16), (1, 16))),
        "up_weight": gaussian(streams_of[2], (D, FFW), D ** -0.5, 0.078125, ((0, 16), (1, 16))),
        "down_weight": gaussian(streams_of[3], (FFW, D), FFW ** -0.5, 0.0546875, ((0, 16), (1, 16))),
        "d_table": gaussian(streams_of[4], (POOL, 3, RANK, D), 1.0, 6.0, ((0, 16),)),
        "f_table": gaussian(streams_of[5], (POOL, 3, RANK, FFW), 1.0, 6.0, ((0, 16), (3, 16))),
        "seeds": set_ends(jax.random.randint(streams_of[6], (POP,), 0, POOL_DEV), jax.random.fold_in(streams_of[6], 1), 0, POOL_DEV - 1).astype(jnp.int32),
        "fitness": gaussian(streams_of[7], (POP,), 1.0, 6.0, ((0, 16),), jnp.float32),
    }


perturb_gain = 0.5

def reference(prompt_acts, gate_weight, up_weight, down_weight, d_table, f_table, seeds, fitness):
    members = jnp.arange(POP, dtype=jnp.int32)
    factor_rows = (members // MEM_DEV * POOL_DEV + seeds).astype(jnp.int32)
    down_factor_rows = jnp.take(d_table, factor_rows, axis=0)
    f_rows = jnp.take(f_table, factor_rows, axis=0)
    base_gate = jnp.dot(prompt_acts, gate_weight, preferred_element_type=jnp.float32).astype(jnp.bfloat16)
    base_up = jnp.dot(prompt_acts, up_weight, preferred_element_type=jnp.float32).astype(jnp.bfloat16)
    shard = FFW // N_TENSOR
    down_blocks = down_weight.reshape(N_TENSOR, shard, D).astype(jnp.float32)

    def member_out(pair):
        d_fac, f_fac = pair
        proj_gate = (jnp.dot(prompt_acts, d_fac[0].T, preferred_element_type=jnp.float32) / math.sqrt(D)).astype(jnp.bfloat16)
        proj_up = (jnp.dot(prompt_acts, d_fac[1].T, preferred_element_type=jnp.float32) / math.sqrt(D)).astype(jnp.bfloat16)
        gate = base_gate.astype(jnp.float32) + perturb_gain * jnp.dot(proj_gate, f_fac[0], preferred_element_type=jnp.float32)
        up = base_up.astype(jnp.float32) + perturb_gain * jnp.dot(proj_up, f_fac[1], preferred_element_type=jnp.float32)
        hidden_state = (jax.nn.silu(gate) * up).astype(jnp.bfloat16)
        blocks = hidden_state.reshape(PROMPT, N_TENSOR, shard).astype(jnp.float32)
        partial_value = jnp.einsum('ptf,tfd->tpd', blocks, down_blocks, precision=lax.Precision.HIGHEST)
        summed = lax.optimization_barrier(jnp.sum(partial_value.astype(jnp.bfloat16).astype(jnp.float32), axis=0))
        proj_down = (jnp.dot(hidden_state, f_fac[2].T, preferred_element_type=jnp.float32) / math.sqrt(FFW)).astype(jnp.bfloat16)
        down_noise_delta = perturb_gain * jnp.dot(proj_down, d_fac[2], preferred_element_type=jnp.float32)
        return (summed + down_noise_delta).astype(jnp.bfloat16)
    outputs = lax.map(member_out, (down_factor_rows, f_rows))
    mean = jnp.sum(fitness) / POP
    spread = jnp.sum((fitness - mean) ** 2) / POP
    score = (fitness - mean) / jnp.sqrt(spread + 1.0)
    weighted = (down_factor_rows.astype(jnp.float32) * score[:, None, None, None]).astype(jnp.bfloat16)
    scale = 1.0 / math.sqrt(POP * RANK)
    w_gate = weighted[:, 0].reshape(POP * RANK, D)
    w_up = weighted[:, 1].reshape(POP * RANK, D)
    w_down = weighted[:, 2].reshape(POP * RANK, D)
    f_gate = f_rows[:, 0].reshape(POP * RANK, FFW)
    f_up = f_rows[:, 1].reshape(POP * RANK, FFW)
    down_factor_columns = f_rows[:, 2].reshape(POP * RANK, FFW)
    delta_gate = (jnp.dot(w_gate.T, f_gate, preferred_element_type=jnp.float32) * scale).astype(jnp.bfloat16)
    delta_up = (jnp.dot(w_up.T, f_up, preferred_element_type=jnp.float32) * scale).astype(jnp.bfloat16)
    delta_down = (jnp.dot(down_factor_columns.T, w_down, preferred_element_type=jnp.float32) * scale).astype(jnp.bfloat16)
    return (outputs, delta_gate, delta_up, delta_down)
```

```python
import functools
import math

import jax
import jax.numpy as jnp
from jax import lax
from jax.experimental import pallas as pl
from jax.experimental.pallas import tpu as pltpu
from jax.sharding import Mesh
from jax.sharding import PartitionSpec as P

D = 5120
FFW = 13824
FB = 864
FP = 896
AX = ("x", "yh", "c", "z", "yl")
MEMBER = ("x", "yh", "c")
TENSOR = ("z", "yl")
MESH = pl.DeviceIdType.MESH
BF = jnp.bfloat16
F32 = jnp.float32


def rcopy(src, dst, ss, rs, dev):
    return pltpu.make_async_remote_copy(
        src_ref=src, dst_ref=dst, send_sem=ss, recv_sem=rs, device_id=dev, device_id_type=MESH
    )


def at(x, yh, c, z, yl):
    return {"x": x, "yh": yh, "c": c, "z": z, "yl": yl}


def k1(
    dt_ref, base_ref, f_ref, pt_ref, a2_ref, out_ref,
    dbuf, hbuf, pd, snd, rcv, fin, fsnd, ft,
    ys, yr, yloc, xs_s, xs_r, ds_s, ds_r, rs_s, rs_r, fs_s, fs_r,
):
    x, yh, c, z, yl = [lax.axis_index(a) for a in AX]
    sgn = 1 - 2 * c
    xn, xp = lax.rem(x + sgn + 4, 4), lax.rem(x - sgn + 4, 4)
    zn, zp = lax.rem(z + sgn + 8, 8), lax.rem(z - sgn + 8, 8)
    ypeers = [at(x, h, yl, z, c) for h in range(2)]
    me_y = [(h == yh) & (c == yl) for h in range(2)]
    partner = at(x, yh, 1 - c, z, yl)
    ypart = at(x, 1 - yh, c, z, yl)

    barrier = pltpu.get_barrier_semaphore()
    others = [partner, ypart, at(xn, yh, c, z, yl), at(xp, yh, c, z, yl), at(x, yh, c, zn, yl), at(x, yh, c, zp, yl)]
    for o in others:
        pl.semaphore_signal(barrier, inc=1, device_id=o, device_id_type=MESH)
    for h in range(2):
        @pl.when(jnp.logical_not(me_y[h]))
        def _():
            pl.semaphore_signal(barrier, inc=1, device_id=ypeers[h], device_id_type=MESH)
    @pl.when(c == yl)
    def _():
        pl.semaphore_wait(barrier, 7)
    @pl.when(c != yl)
    def _():
        pl.semaphore_wait(barrier, 8)

    for h in range(2):
        @pl.when(jnp.logical_not(me_y[h]))
        def _():
            rcopy(dt_ref.at[h], dbuf.at[yl, 2 * x + yh], ys.at[h], yr.at[yh], ypeers[h]).start()
        @pl.when(me_y[h])
        def _():
            pltpu.make_async_copy(dt_ref.at[h], dbuf.at[yl, 2 * x + yh], yloc).start()

    def wait_y():
        for h in range(2):
            @pl.when(jnp.logical_not(me_y[h]))
            def _():
                rcopy(dt_ref.at[h], dbuf.at[c, 2 * x + h], ys.at[h], yr.at[h], ypeers[h]).wait_recv()
            @pl.when(me_y[h])
            def _():
                pltpu.make_async_copy(dt_ref.at[h], dbuf.at[yl, 2 * x + yh], yloc).wait()

    def blk(core, xi):
        return dbuf.at[core, pl.ds(2 * xi, 2)]

    def xfwd(s):
        xi = lax.rem(x - sgn * s + 8, 4)
        rcopy(blk(c, xi), blk(c, xi), xs_s.at[s], xs_r.at[s], at(xn, yh, c, z, yl)).start()

    def dfwd(s):
        xi = lax.rem(x - sgn * s + 8, 4)
        rcopy(blk(c, xi), blk(c, xi), ds_s.at[s], ds_r.at[s], partner).start()

    def wait_x(s):
        xi = lax.rem(x - sgn * (s + 1) + 8, 4)
        rcopy(blk(c, xi), blk(c, xi), xs_s.at[s], xs_r.at[s], at(xn, yh, c, z, yl)).wait_recv()

    def wait_d(s):
        xi = lax.rem(x + sgn * s + 8, 4)
        rcopy(blk(1 - c, xi), blk(1 - c, xi), ds_s.at[s], ds_r.at[s], partner).wait_recv()

    for g in range(2):
        for t in range(2):
            for k in range(2):
                ft[g, t, k] = f_ref[g, t, k].T

    wait_y()
    xfwd(0)
    dfwd(0)

    rowm = lax.broadcasted_iota(jnp.int32, (32, 256), 0) // 4
    lanem = lax.broadcasted_iota(jnp.int32, (32, 256), 1) // 128

    def hidden(i):
        g, cc = i // 4, lax.rem(i, 4)
        live = rowm == 2 * cc + lanem
        pm = [
            jnp.where(live, jnp.concatenate([pt_ref[g, k]] * 2, axis=1).astype(F32), 0.0).astype(BF)
            for k in range(2)
        ]
        for t in range(2):
            def rows(rb, _):
                r = pl.ds(pl.multiple_of(rb * 64, 64), 64)
                b = [base_ref[t, k, r].astype(F32) for k in range(2)]
                gu = [
                    jnp.concatenate([b[k], b[k]], axis=1)
                    + jnp.dot(ft[g, t, k, r], pm[k], preferred_element_type=F32)
                    for k in range(2)
                ]
                hbuf[i, t, r] = (gu[0] / (1.0 + jnp.exp(-gu[0])) * gu[1]).astype(BF)
                return 0
            lax.fori_loop(0, 14, rows, 0)
        q = jnp.dot(f_ref[g, 0, 2], hbuf[i, 0], preferred_element_type=F32)
        q += jnp.dot(f_ref[g, 1, 2], hbuf[i, 1], preferred_element_type=F32)
        pd[i] = jnp.where(live, q * (0.5 / math.sqrt(FFW)), 0.0).astype(BF)

    def hloop(lo, hi):
        def body(i, _):
            hidden(i)
            return 0
        lax.fori_loop(lo, hi, body, 0)

    hloop(0, 3)
    wait_x(0)
    xfwd(1)
    dfwd(1)
    hloop(3, 6)
    wait_x(1)
    xfwd(2)
    dfwd(2)
    hloop(6, 8)
    wait_x(2)
    dfwd(3)
    for s in range(4):
        wait_d(s)

    def part(d, i):
        g = i // 4
        p = jnp.dot(dbuf[0, d], hbuf[i, 0], preferred_element_type=F32)
        p += jnp.dot(dbuf[1, d], hbuf[i, 1], preferred_element_type=F32)
        p += jnp.dot(a2_ref[g, d], pd[i], preferred_element_type=F32)
        return p

    def chunk(j):
        return lax.rem(j + 4 * (1 - yh), 8)

    znd = at(x, yh, c, zn, yl)
    d0 = lax.rem(z - sgn + 8, 8)

    def first(j, _):
        i = chunk(j)
        snd[i] = part(d0, i).astype(BF)
        rcopy(snd.at[i], rcv.at[0, i], rs_s.at[0, i], rs_r.at[0, i], znd).start()
        return 0

    lax.fori_loop(0, 8, first, 0)

    def middle(n, _):
        s, j = n // 8 + 1, lax.rem(n, 8)
        i = chunk(j)
        d = lax.rem(z - sgn * (1 + s) + 16, 8)
        p = part(d, i)
        rcopy(snd.at[i], rcv.at[s - 1, i], rs_s.at[s - 1, i], rs_r.at[s - 1, i], znd).wait_recv()
        rcv[s - 1, i] = (p + rcv[s - 1, i].astype(F32)).astype(BF)
        rcopy(rcv.at[s - 1, i], rcv.at[s, i], rs_s.at[s, i], rs_r.at[s, i], znd).start()
        return 0

    lax.fori_loop(0, 48, middle, 0)

    def last(j):
        i = chunk(j)
        p = part(z, i)
        rcopy(snd.at[i], rcv.at[6, i], rs_s.at[6, i], rs_r.at[6, i], znd).wait_recv()
        return (p + rcv[6, i].astype(F32)).astype(BF)

    def last_far(j, _):
        fsnd[j] = last(j)
        rcopy(fsnd.at[j], fin.at[yh, j], fs_s.at[j], fs_r.at[j], ypart).start()
        return 0

    lax.fori_loop(0, 4, last_far, 0)

    def last_near(j, _):
        fin[yh, j] = last(j + 4)
        return 0

    lax.fori_loop(0, 4, last_near, 0)

    def finish(j, _):
        rcopy(fsnd.at[j], fin.at[1 - yh, j], fs_s.at[j], fs_r.at[j], ypart).wait()
        w = jnp.concatenate([fin[0, j], fin[1, j]], axis=0).astype(F32)
        for m in range(2):
            out_ref[2 * j + m] = w[:, 128 * m : 128 * (m + 1)].T.astype(BF)
        return 0

    lax.fori_loop(0, 4, finish, 0)

    for h in range(2):
        @pl.when(jnp.logical_not(me_y[h]))
        def _():
            rcopy(dt_ref.at[h], dbuf.at[yl, 2 * x + yh], ys.at[h], yr.at[yh], ypeers[h]).wait_send()
    for s in range(3):
        rcopy(blk(c, 0), blk(c, 0), xs_s.at[s], xs_r.at[s], at(xn, yh, c, z, yl)).wait_send()
    for s in range(4):
        rcopy(blk(c, 0), blk(c, 0), ds_s.at[s], ds_r.at[s], partner).wait_send()

    def drain(n, _):
        s, i = n // 8, lax.rem(n, 8)
        rcopy(snd.at[i], rcv.at[s, i], rs_s.at[s, i], rs_r.at[s, i], znd).wait_send()
        return 0

    lax.fori_loop(0, 56, drain, 0)


def call_k1(dt, base, f, pt, a2):
    v = pl.BlockSpec(memory_space=pltpu.VMEM)
    dma = pltpu.SemaphoreType.DMA
    return pl.pallas_call(
        k1,
        out_shape=jax.ShapeDtypeStruct((8, 128, 320), BF),
        in_specs=[pl.BlockSpec(memory_space=pl.ANY), v, v, v, v],
        out_specs=v,
        scratch_shapes=[
            pltpu.VMEM((2, 8, 160, FP), BF),
            pltpu.VMEM((8, 2, FP, 256), BF),
            pltpu.VMEM((8, 32, 256), BF),
            pltpu.VMEM((8, 160, 256), BF),
            pltpu.VMEM((7, 8, 160, 256), BF),
            pltpu.VMEM((2, 4, 160, 256), BF),
            pltpu.VMEM((4, 160, 256), BF),
            pltpu.VMEM((2, 2, 2, FP, 32), BF),
            dma((2,)), dma((2,)), dma(()), dma((3,)), dma((3,)), dma((4,)), dma((4,)),
            dma((7, 8)), dma((7, 8)), dma((4,)), dma((4,)),
        ],
        compiler_params=pltpu.CompilerParams(
            collective_id=0, has_side_effects=True, vmem_limit_bytes=56 << 20
        ),
        name="k1",
    )(dt, base, f, pt, a2)


def shards(prompt_acts, gate_weight, up_weight, down_weight, d_table, f_table, seeds, fitness):
    yh, yl = lax.axis_index("yh"), lax.axis_index("yl")
    d_sel = jnp.take(d_table, seeds, axis=0, mode="clip")
    f_sel = jnp.take(f_table, seeds, axis=0, mode="clip")
    both = jnp.concatenate([gate_weight, up_weight], axis=1)
    base = lax.psum(jnp.dot(prompt_acts, both, preferred_element_type=F32), MEMBER).astype(BF)
    base = jnp.pad(base.reshape(128, 2, FB), ((0, 0), (0, 0), (0, FP - FB)))
    base = lax.all_gather(base.transpose(1, 2, 0), "yl")
    prompt_full = lax.all_gather(prompt_acts, MEMBER, axis=1, tiled=True)
    dk = d_sel.transpose(1, 0, 2, 3).reshape(3, 32, D)
    proj = jnp.einsum("pd,krd->krp", prompt_full, dk[:2], preferred_element_type=F32)
    pt = lax.all_gather((proj / math.sqrt(D)).astype(BF) * BF(0.5), "yh")
    fk = jnp.pad(f_sel.transpose(1, 0, 2, 3).reshape(3, 32, FB), ((0, 0), (0, 0), (0, FP - FB)))
    f = lax.all_gather(lax.all_gather(fk, "yl"), "yh")
    a2 = dk[2].reshape(32, 8, 2, 2, 160).transpose(2, 3, 1, 4, 0)
    a2 = lax.all_gather(lax.dynamic_index_in_dim(a2, yl, 0, False), "yh")
    a2 = lax.dynamic_index_in_dim(a2, yh, 1, False)
    dt = jnp.pad(down_weight.T.reshape(2, 160, FB), ((0, 0), (0, 0), (0, FP - FB)))
    outputs = call_k1(dt, base, f, pt, a2)
    f_all = lax.all_gather(fk[:, :, :FB], MEMBER).transpose(1, 0, 2, 3).reshape(3, 512, FB)
    d_all = lax.all_to_all(dk, MEMBER, 2, 0, tiled=True).reshape(16, 3, 32, 320).transpose(1, 0, 2, 3).reshape(3, 512, 320)
    fit = lax.all_gather(fitness, MEMBER, tiled=True)
    mean = jnp.sum(fit) / 128
    spread = jnp.sum((fit - mean) ** 2) / 128
    score = (fit - mean) / jnp.sqrt(spread + 1.0)
    w = (d_all.astype(F32) * jnp.repeat(score, 4)[None, :, None]).astype(BF)
    s = 1.0 / math.sqrt(512)
    dg = (jnp.einsum("ma,mb->ab", w[0], f_all[0], preferred_element_type=F32) * s).astype(BF)
    du = (jnp.einsum("ma,mb->ab", w[1], f_all[1], preferred_element_type=F32) * s).astype(BF)
    dd = (jnp.einsum("ma,mb->ab", f_all[2], w[2], preferred_element_type=F32) * s).astype(BF)
    return outputs, dg, du, dd


def solution(mesh):
    split = Mesh(mesh.devices.reshape(4, 2, 2, 8, 2), AX)
    placed = (
        P(None, MEMBER), P(MEMBER, TENSOR), P(MEMBER, TENSOR), P(TENSOR, MEMBER),
        P(MEMBER, None, None, None), P(MEMBER, None, None, TENSOR), P(MEMBER), P(MEMBER),
    )
    return jax.shard_map(
        shards, mesh=split, in_specs=placed,
        out_specs=(P(MEMBER, None, TENSOR), P(MEMBER, TENSOR), P(MEMBER, TENSOR), P(TENSOR, MEMBER)),
        check_vma=False,
    )
```

```python
import functools
import math

import jax
import jax.numpy as jnp
from jax import lax
from jax.experimental import pallas as pl
from jax.experimental.pallas import tpu as pltpu
from jax.sharding import Mesh
from jax.sharding import PartitionSpec as P

D = 5120
FFW = 13824
FB = 864
AX = ("x", "yh", "c", "z", "yl")
MEMBER = ("x", "yh", "c")
TENSOR = ("z", "yl")
MESH = pl.DeviceIdType.MESH
BF = jnp.bfloat16
F32 = jnp.float32


def rem(a, n):
    return lax.rem(a, n)


def at(x, yh, c, z, yl):
    return {"x": x, "yh": yh, "c": c, "z": z, "yl": yl}


def tn(a, b):
    return lax.dot_general(a, b, (((0,), (0,)), ((), ())), preferred_element_type=F32)


def nt(a, b):
    return lax.dot_general(a, b, (((1,), (1,)), ((), ())), preferred_element_type=F32)


def nn(a, b):
    return jnp.dot(a, b, preferred_element_type=F32)


def step_kernel(
    pt_hbm, gw_hbm, uw_hbm, dt_hbm, dtab_hbm, ftab_hbm, seeds, fit,
    out_ref, dg_ref, du_ref, dd_ref,
    pt_v, w_v, dtab, ftab, dk, fall, foth, dbuf, hbuf, snd, rcv, fin, fsnd, ft,
    bsend, brecv, bown, ps, rsb, basebuf, basef, psh, prb, pjs, pjb, ptt,
    pdc, pdb, dall, fitall, score, wt, a2t,
    in_s, bx_s, bx_r, r1_s, r1_r, ag_s, ag_r, bf_s, bf_r, pr_s, pr_r, pj_s, pj_r,
    ft_s, ft_r, ys, yr, yloc, xo_s, xf_s, x_r, ds_s, ds_r, rs_s, rs_r, fs_s, fs_r,
    pd_s, pd_r, f_s, f_r, ff_s, ff_r, d_s, d_r, q_s, q_r,
):
    x, yh, c, z, yl = [lax.axis_index(a) for a in AX]
    y = 2 * yh + yl
    p = 2 * x + yh
    me = at(x, yh, c, z, yl)
    partner = at(x, yh, 1 - c, z, yl)
    ypart = at(x, 1 - yh, c, z, yl)
    pending = []

    def rc(src, dst, ss, rs, dev):
        return pltpu.make_async_remote_copy(
            src_ref=src, dst_ref=dst, send_sem=ss, recv_sem=rs, device_id=dev, device_id_type=MESH
        )

    def send(src, dst, ss, rs, dev):
        d = rc(src, dst, ss, rs, dev)
        d.start()
        pending.append(d.wait_send)

    def recv(dst, rs):
        rc(dst, dst, rs, rs, partner).wait_recv()

    loads = [
        (gw_hbm, w_v.at[0]), (uw_hbm, w_v.at[1]), (pt_hbm, pt_v), (ftab_hbm, ftab), (dtab_hbm, dtab),
    ]
    loads = [pltpu.make_async_copy(a, b, in_s.at[i]) for i, (a, b) in enumerate(loads)]
    for l in loads:
        l.start()

    def plane(rel):
        ny = rem(y + rel % 4, 4)
        return at(rem(x + rel // 4, 4), ny // 2, c, z, rem(ny, 2))

    def mate(rel):
        q = rem(p + rel // 2, 8)
        return at(q // 2, rem(q, 2), rem(c + rel % 2, 2), z, yl)

    def column(rel):
        return at(x, rem(yh + rel // 8, 2), c, rem(z + rel % 8, 8), yl)

    ypeers = [at(x, h, yl, z, c) for h in range(2)]
    me_y = [(h == yh) & (c == yl) for h in range(2)]
    barrier = pltpu.get_barrier_semaphore()

    def greet(dev):
        pl.semaphore_signal(barrier, inc=1, device_id=dev, device_id_type=MESH)

    peers = [plane(r) for r in range(1, 16)] + [mate(r) for r in range(1, 16, 2)]
    peers += [column(r) for r in range(1, 16) if r != 8]
    for o in peers:
        greet(o)
    for h in range(2):
        @pl.when(c != yl)
        def _():
            greet(ypeers[h])

    for l in loads[:3]:
        l.wait()

    def partial_base(k):
        return tn(w_v[k], pt_v[...])

    bsend[pl.ds(0, FB)] = partial_base(1 - c).astype(BF)
    bsend[pl.ds(FB, 32)] = jnp.zeros((32, 128), BF)

    n_peers = len(peers)

    @pl.when(c == yl)
    def _():
        pl.semaphore_wait(barrier, n_peers)

    @pl.when(c != yl)
    def _():
        pl.semaphore_wait(barrier, n_peers + 2)

    send(bsend, brecv, bx_s, bx_r, partner)

    for h in range(2):
        @pl.when(jnp.logical_not(me_y[h]))
        def _():
            rc(dt_hbm.at[h], dbuf.at[yl, 2 * x + yh], ys.at[h], yr.at[yh], ypeers[h]).start()
        @pl.when(me_y[h])
        def _():
            pltpu.make_async_copy(dt_hbm.at[h], dbuf.at[yl, 2 * x + yh], yloc).start()

    def wait_y():
        for h in range(2):
            @pl.when(jnp.logical_not(me_y[h]))
            def _():
                rc(dt_hbm.at[h], dbuf.at[c, 2 * x + h], ys.at[h], yr.at[h], ypeers[h]).wait_recv()
                rc(dt_hbm.at[h], dbuf.at[c, 2 * x + h], ys.at[h], yr.at[h], ypeers[h]).wait_send()
            @pl.when(me_y[h])
            def _():
                pltpu.make_async_copy(dt_hbm.at[h], dbuf.at[yl, 2 * x + yh], yloc).wait()

    ptr = pt_v[...].astype(F32).T.astype(BF)
    psh[...] = jnp.zeros_like(psh)

    @pl.when(c == 0)
    def _():
        psh[:, 0:320] = ptr

    @pl.when(c == 1)
    def _():
        psh[:, 64:384] = ptr

    toks = pl.ds(pl.multiple_of(16 * z, 16), 16)
    for r in range(1, 16):
        send(psh.at[toks], prb.at[r], pr_s.at[r], pr_r.at[r], mate(r))

    bown[pl.ds(0, FB)] = partial_base(c)
    bown[pl.ds(FB, 32)] = jnp.zeros((32, 128), F32)
    recv(brecv, bx_r)
    for q in range(8):
        rows = pl.ds(112 * q, 112)
        ps[q] = (bown[rows] + brecv[rows].astype(F32)).astype(BF)
    for r in range(1, 8):
        q = rem(p + r, 8)
        send(ps.at[q], rsb.at[r], r1_s.at[r], r1_r.at[r], at(q // 2, rem(q, 2), c, z, yl))

    loads[3].wait()
    for k in range(3):
        for m in range(8):
            fall[k, c, p, pl.ds(4 * m, 4)] = ftab[seeds[m], k]
    fteam = [(1, 0), (0, 1), (1, 1)]
    for i, (dh, dl) in enumerate(fteam):
        dev = at(x, rem(yh + dh, 2), c, z, rem(yl + dl, 2))
        dst = fall.at[:, c, p] if dl == 0 else foth.at[yh]
        send(fall.at[:, c, p], dst, ft_s.at[i], ft_r.at[i], dev)

    loads[4].wait()
    for k in range(3):
        for m in range(8):
            dk[k, pl.ds(4 * m, 4)] = dtab[seeds[m], k]

    def proj_of(r, piece):
        q = rem(p - r // 2 + 8, 8)
        cc = rem(c + r % 2, 2)
        lanes = pl.ds(pl.multiple_of(640 * q + 256 * cc, 128), 384)
        return nt(piece, dk[0:2, :, lanes].reshape(64, 384))

    acc = proj_of(0, psh[toks])
    for r in range(1, 16):
        recv(prb.at[r], pr_r.at[r])
        acc += proj_of(r, prb[r])
    acc = (acc / math.sqrt(D)).astype(BF).astype(F32)
    kk = lax.broadcasted_iota(jnp.int32, (16, 64), 1) // 32
    acc = jnp.where(kk == 0, acc * 0.25, acc * 0.5)
    pjs[...] = jnp.zeros_like(pjs)
    pjs[:, 0:64] = acc.astype(BF)
    for r in range(1, 16):
        send(pjs, pjb.at[yh, toks], pj_s.at[r], pj_r.at[r], column(r))
    pjb[yh, toks] = pjs[...]

    s = bown[pl.ds(pl.multiple_of(112 * p, 16), 112)] + brecv[pl.ds(pl.multiple_of(112 * p, 16), 112)].astype(F32)
    for r in range(1, 8):
        recv(rsb.at[r], r1_r.at[r])
        s += rsb[r].astype(F32)

    def brows(q):
        return pl.ds(pl.multiple_of(112 * q, 16), 112)

    basebuf[yl, c, brows(p)] = s.astype(BF)
    for r in range(1, 16):
        send(basebuf.at[yl, c, brows(p)], basebuf.at[yl, c, brows(p)], ag_s.at[r], ag_r.at[r], plane(r))

    e, kz = rem(z, 2), z // 2

    def zblk(r, ab):
        x0 = rem(x - r + 4, 4)
        m = rem(x0 - kz + 4, 4)
        low = jnp.where(e == 0, jnp.where(m == 1, 0, 1), jnp.where(m == 3, 1, 0))
        return 2 * x0 + (low if ab == 0 else 1 - low)

    xnb = [at(rem(x + 1, 4), yh, c, z, yl), at(rem(x + 3, 4), yh, c, z, yl)]

    def dsend(r, ab):
        b = zblk(r, ab)
        send(dbuf.at[c, b], dbuf.at[c, b], ds_s.at[r, ab], ds_r.at[r, ab], partner)

    def own_x(ab):
        b = dbuf.at[c, zblk(0, ab)]
        send(b, b, xo_s.at[0, ab], x_r.at[1, ab], xnb[0])
        send(b, b, xo_s.at[1, ab], x_r.at[3, ab], xnb[1])
        dsend(0, ab)

    def take_x(r, ab):
        b = dbuf.at[c, zblk(r, ab)]
        recv(b, x_r.at[r, ab])
        if r != 2:
            fwd = c == (0 if r == 1 else 1)
            d = rc(b, b, xf_s.at[r, ab], x_r.at[2, ab], xnb[0 if r == 1 else 1])
            pl.when(fwd)(d.start)
            pending.append(lambda: pl.when(fwd)(d.wait_send))
        dsend(r, ab)

    def take_d(r, ab):
        recv(dbuf.at[1 - c, zblk(r, ab)], ds_r.at[r, ab])

    wait_y()
    own_x(0)

    for i, (dh, dl) in enumerate(fteam):
        if dl == 0:
            recv(fall.at[:, c, p + 1 - 2 * yh], ft_r.at[i])
        else:
            recv(foth.at[rem(yh + dh, 2)], ft_r.at[i])

    def fac(g, tau):
        return fall.at[:, c, 2 * x + g] if tau == 0 else foth.at[g]

    for g in range(2):
        for tau in range(2):
            for k in range(2):
                ft[g, tau, k] = fac(g, tau)[k].T
    for r in range(1, 16):
        hz, zz = rem(yh + r // 8, 2), rem(z - r % 8 + 8, 8)
        recv(pjb.at[hz, pl.ds(pl.multiple_of(16 * zz, 16), 16)], pj_r.at[r])
    for g in range(2):
        ptt[g] = pjb[g].astype(F32).T[0:64].reshape(2, 32, 128)

    for r in range(1, 16):
        xx, yy = rem(x - r // 4 + 4, 4), rem(y - r % 4 + 4, 4)
        piece = basebuf.at[rem(yy, 2), c, brows(2 * xx + yy // 2)]
        recv(piece, ag_r.at[r])
    send(basebuf.at[:, c], basebuf.at[:, c], bf_s, bf_r, partner)

    take_x(1, 0)
    take_x(3, 0)
    own_x(1)
    recv(basebuf.at[:, 1 - c], bf_r)
    for tau in range(2):
        t = rem(yl + tau, 2)
        for k in range(2):
            b = basebuf[t, k, pl.ds(0, FB)].astype(F32)
            basef[tau, k] = b * 0.5 if k == 0 else b
    take_x(2, 0)
    for r in range(4):
        take_d(r, 0)

    rowm = lax.broadcasted_iota(jnp.int32, (32, 256), 0) // 4
    lanem = lax.broadcasted_iota(jnp.int32, (32, 256), 1) // 128

    def hidden(i):
        g, cc = i // 4, rem(i, 4)
        live = rowm == 2 * cc + lanem
        pm = [
            jnp.where(live, jnp.concatenate([ptt[g, k]] * 2, axis=1), 0.0).astype(BF)
            for k in range(2)
        ]
        for tau in range(2):
            def rows(rb, _):
                r = pl.ds(pl.multiple_of(rb * 48, 16), 48)
                b = [basef[tau, k, r] for k in range(2)]
                gu = [
                    jnp.concatenate([b[k], b[k]], axis=1) + nn(ft[g, tau, k, r], pm[k])
                    for k in range(2)
                ]
                hbuf[i, tau, r] = ((gu[0] + gu[0] * jnp.tanh(gu[0])) * gu[1]).astype(BF)
                return 0
            lax.fori_loop(0, 18, rows, 0, unroll=3)

    def chunk(j):
        return rem(j + 4 * (1 - yh), 8)

    sgn = 1 - 2 * c
    zn = rem(z + sgn + 8, 8)
    znd = at(x, yh, c, zn, yl)

    def part(d, i):
        return nn(dbuf[yl, d], hbuf[i, 0]) + nn(dbuf[1 - yl, d], hbuf[i, 1])

    d0 = rem(z - sgn + 8, 8)

    def first(j, _):
        i = chunk(j)
        hidden(i)
        snd[i] = part(d0, i).astype(BF)
        rc(snd.at[i], rcv.at[0, i], rs_s.at[0, i], rs_r.at[0, i], znd).start()
        return 0

    lax.fori_loop(0, 8, first, 0)

    tot = jnp.zeros((32, 128), F32)
    for cc in range(4):
        i = 4 * yh + cc
        q = nn(fall[2, c, p], hbuf[i, 0]) + nn(foth[yh, 2], hbuf[i, 1])
        q = jnp.where(rowm == 2 * cc + lanem, q, 0.0)
        tot += q[:, :128] + q[:, 128:]
    pdc[...] = tot
    for r in range(1, 8):
        send(pdc, pdb.at[r], pd_s.at[r], pd_r.at[r], column(r))

    take_x(1, 1)
    take_x(3, 1)
    take_x(2, 1)
    for r in range(4):
        take_d(r, 1)

    for i in range(1, 8):
        q = rem(p + i, 8)
        far = q != (p + 1 - 2 * yh)
        d = rc(fall.at[:, c, p], fall.at[:, c, p], f_s.at[i], f_r.at[i], at(q // 2, rem(q, 2), c, z, yl))
        pl.when(far)(d.start)
        pending.append(functools.partial(pl.when(far), d.wait_send))
    for m in range(8):
        fitall[c, p, pl.ds(4 * m, 4)] = jnp.full((4, 128), fit[m], F32)

    def dlanes(q, cc):
        return pl.ds(pl.multiple_of(640 * q + 256 * cc, 128), 384)

    dall[:, c, p] = dk[:, :, dlanes(p, c)]
    for r in range(1, 16):
        q, cc = rem(p + r // 2, 8), rem(c + r % 2, 2)
        send(dk.at[:, :, dlanes(q, cc)], dall.at[:, c, p], d_s.at[r], d_r.at[r], mate(r))
        send(fitall.at[c, p], fitall.at[c, p], q_s.at[r], q_r.at[r], mate(r))

    def middle(n, _):
        s, j = n // 8 + 1, rem(n, 8)
        i = chunk(j)
        pp = part(rem(z - sgn * (1 + s) + 16, 8), i)
        recv(rcv.at[s - 1, i], rs_r.at[s - 1, i])
        rcv[s - 1, i] = (pp + rcv[s - 1, i].astype(F32)).astype(BF)
        rc(rcv.at[s - 1, i], rcv.at[s, i], rs_s.at[s, i], rs_r.at[s, i], znd).start()
        return 0

    lax.fori_loop(0, 32, middle, 0)

    for i in range(1, 8):
        q = rem(p - i + 8, 8)
        far = q != (p + 1 - 2 * yh)
        pl.when(far)(functools.partial(recv, fall.at[:, c, q], f_r.at[i]))
    send(fall.at[:, c], fall.at[:, c], ff_s, ff_r, partner)

    lax.fori_loop(32, 40, middle, 0)

    for r in range(1, 16):
        q, cc = rem(p - r // 2 + 8, 8), rem(c + r % 2, 2)
        recv(dall.at[:, cc, q], d_r.at[r])
        recv(fitall.at[cc, q], q_r.at[r])
    recv(fall.at[:, 1 - c], ff_r)
    fv = fitall[...].reshape(512, 128)
    mean = jnp.sum(fv, axis=0, keepdims=True) / 512
    spread = jnp.sum((fv - mean) ** 2, axis=0, keepdims=True) / 512
    score[...] = ((fv - mean) / jnp.sqrt(spread + 1.0)).reshape(2, 8, 32, 128)
    for k in range(3):
        def weigh(g, _):
            a, b = g // 8, rem(g, 8)
            sc = score[a, b]
            w = dall[k, a, b].astype(F32) * jnp.concatenate([sc] * 3, axis=1)
            dall[k, a, b] = w.astype(BF)
            return 0
        lax.fori_loop(0, 16, weigh, 0)
        wt[k] = dall[k].reshape(512, 384).T

    def deltas(k, ref):
        def rows(rb, _):
            r = pl.ds(pl.multiple_of(64 * c + 32 * rb, 16), 32)
            v = nn(wt[k, r], fall[k].reshape(512, FB)) * (1.0 / math.sqrt(512))
            ref[pl.ds(pl.multiple_of(32 * rb, 16), 32)] = v.astype(BF)
            return 0
        lax.fori_loop(0, 10, rows, 0)

    deltas(0, dg_ref)
    deltas(1, du_ref)
    deltas(2, dd_ref)

    lax.fori_loop(40, 48, middle, 0)

    tot = pdc[...]
    for r in range(1, 8):
        recv(pdb.at[r], pd_r.at[r])
        tot += pdb[r]
    tot = (tot / math.sqrt(FFW)).astype(BF).astype(F32) * 0.5
    pdc2 = tot
    a2t[...] = dk[2, :, pl.ds(pl.multiple_of(640 * z + 256 * yl, 128), 384)].T
    pdb[0] = pdc2

    def last(j):
        i = chunk(j)
        pp = part(z, i)
        recv(rcv.at[6, i], rs_r.at[6, i])
        return (pp + rcv[6, i].astype(F32)).astype(BF)

    def last_far(j, _):
        fsnd[j] = last(j)
        rc(fsnd.at[j], fin.at[yh, j], fs_s.at[j], fs_r.at[j], ypart).start()
        return 0

    lax.fori_loop(0, 4, last_far, 0)

    def last_near(j, _):
        fin[yh, j] = last(j + 4)
        return 0

    lax.fori_loop(0, 4, last_near, 0)

    def finish(j, _):
        rc(fsnd.at[j], fin.at[1 - yh, j], fs_s.at[j], fs_r.at[j], ypart).wait()
        live = rowm == 2 * j + lanem
        pm = jnp.where(live, jnp.concatenate([pdb[0]] * 2, axis=1), 0.0).astype(BF)
        for h in range(2):
            r = pl.ds(pl.multiple_of(64 * yl + 160 * h, 16), 160)
            w = (fin[h, j].astype(F32) + nn(a2t[r], pm)).astype(BF)
            for m in range(2):
                out_ref[2 * j + m, pl.ds(160 * h, 160)] = w[:, 128 * m : 128 * (m + 1)]
        return 0

    lax.fori_loop(0, 4, finish, 0)

    for w in pending:
        w()

    def drain(n, _):
        s, i = n // 8, rem(n, 8)
        rc(snd.at[i], rcv.at[s, i], rs_s.at[s, i], rs_r.at[s, i], znd).wait_send()
        return 0

    lax.fori_loop(0, 56, drain, 0)


def call_step(pt, gw, uw, dt, dtab, ftab, seeds, fit):
    v = pl.BlockSpec(memory_space=pltpu.VMEM)
    a = pl.BlockSpec(memory_space=pl.ANY)
    sm = pl.BlockSpec(memory_space=pltpu.SMEM)
    dma = pltpu.SemaphoreType.DMA
    vm = pltpu.VMEM
    return pl.pallas_call(
        step_kernel,
        out_shape=[
            jax.ShapeDtypeStruct((8, 320, 128), BF),
            jax.ShapeDtypeStruct((320, FB), BF),
            jax.ShapeDtypeStruct((320, FB), BF),
            jax.ShapeDtypeStruct((320, FB), BF),
        ],
        in_specs=[a, a, a, a, a, a, sm, sm],
        out_specs=[v, v, v, v],
        scratch_shapes=[
            vm((320, 128), BF), vm((2, 320, FB), BF), vm((16, 3, 4, D), BF), vm((16, 3, 4, FB), BF),
            vm((3, 32, D), BF), vm((3, 2, 8, 32, FB), BF), vm((2, 3, 32, FB), BF),
            vm((2, 8, 160, FB), BF), vm((8, 2, FB, 256), BF), vm((8, 160, 256), BF),
            vm((7, 8, 160, 256), BF), vm((2, 4, 160, 256), BF), vm((4, 160, 256), BF),
            vm((2, 2, 2, FB, 32), BF),
            vm((896, 128), BF), vm((896, 128), BF), vm((896, 128), F32), vm((8, 112, 128), BF),
            vm((8, 112, 128), BF), vm((2, 2, 896, 128), BF), vm((2, 2, FB, 128), F32),
            vm((128, 384), BF), vm((16, 16, 384), BF), vm((16, 128), BF), vm((2, 128, 128), BF),
            vm((2, 2, 32, 128), F32),
            vm((32, 128), F32), vm((8, 32, 128), F32), vm((3, 2, 8, 32, 384), BF),
            vm((2, 8, 32, 128), F32), vm((2, 8, 32, 128), F32), vm((3, 384, 512), BF), vm((384, 32), BF),
            dma((5,)), dma(()), dma(()), dma((8,)), dma((8,)), dma((16,)), dma((16,)), dma(()), dma(()),
            dma((16,)), dma((16,)), dma((16,)), dma((16,)),
            dma((3,)), dma((3,)), dma((2,)), dma((2,)), dma(()), dma((2, 2)), dma((4, 2)), dma((4, 2)),
            dma((4, 2)), dma((4, 2)), dma((7, 8)), dma((7, 8)), dma((4,)), dma((4,)),
            dma((8,)), dma((8,)), dma((8,)), dma((8,)), dma(()), dma(()), dma((16,)), dma((16,)),
            dma((16,)), dma((16,)),
        ],
        compiler_params=pltpu.CompilerParams(
            collective_id=0, has_side_effects=True, vmem_limit_bytes=60 << 20
        ),
        name="es_step",
    )(pt, gw, uw, dt, dtab, ftab, seeds, fit)


def shards(prompt_acts, gate_weight, up_weight, down_weight, d_table, f_table, seeds, fitness):
    out, dg, du, dd = call_step(
        prompt_acts.T, gate_weight, up_weight, down_weight.T.reshape(2, 160, FB), d_table, f_table,
        seeds, fitness,
    )
    return out.transpose(0, 2, 1), dg, du, dd.T


def solution(mesh):
    split = Mesh(mesh.devices.reshape(4, 2, 2, 8, 2), AX)
    placed = (
        P(None, MEMBER), P(MEMBER, TENSOR), P(MEMBER, TENSOR), P(TENSOR, MEMBER),
        P(MEMBER, None, None, None), P(MEMBER, None, None, TENSOR), P(MEMBER), P(MEMBER),
    )
    return jax.shard_map(
        shards, mesh=split, in_specs=placed,
        out_specs=(P(MEMBER, None, TENSOR), P(MEMBER, TENSOR), P(MEMBER, TENSOR), P(TENSOR, MEMBER)),
        check_vma=False,
    )
```

```python
import functools
import math

import jax
import jax.numpy as jnp
from jax import lax
from jax.experimental import pallas as pl
from jax.experimental.pallas import tpu as pltpu
from jax.sharding import Mesh
from jax.sharding import PartitionSpec as P

D = 5120
FFW = 13824
FB = 864
AX = ("x", "yh", "c", "z", "yl")
MEMBER = ("x", "yh", "c")
TENSOR = ("z", "yl")
MESH = pl.DeviceIdType.MESH
BF = jnp.bfloat16
F32 = jnp.float32
HR = 864
HU = 1
LEAD = 4
TB = 0
ORDER = (
    "y_first",
    "y_second",
    "base_half",
    "base_scatter",
    "prompt_out",
    "local_rows",
    "base_sum",
    "factors_far",
    "prompt_on",
    "factors_near",
    "x_first",
    "base_on",
    "project",
    "take_first",
    "x_second",
    "factors_far_in",
    "base_end",
    "project_in",
    "base_other",
    "hidden_ahead",
    "factors_near_in",
    "take_first_far",
)


def rem(a, n):
    return lax.rem(a, n)


def at(x, yh, c, z, yl):
    return {"x": x, "yh": yh, "c": c, "z": z, "yl": yl}


def tn(a, b):
    return lax.dot_general(a, b, (((0,), (0,)), ((), ())), preferred_element_type=F32)


def nt(a, b):
    return lax.dot_general(a, b, (((1,), (1,)), ((), ())), preferred_element_type=F32)


def nn(a, b):
    return jnp.dot(a, b, preferred_element_type=F32)


def step_kernel(
    pt_hbm, gw_hbm, uw_hbm, dt_hbm, dtab_hbm, ftab_hbm, seeds, fit,
    out_ref, del_ref,
    pt_v, w_v, dt_v, dtab, ftab, dk, fall, foth, dbuf, hbuf, snd, rcv, fin, fsnd,
    bsend, brecv, bown, ps, rsb, lhs, rhs, psh, prb, pjs, pjb, ptt,
    pdc, pdb, pdt, dall, fitall, score, wt, a2t, nbuf,
    in_s, bx_s, bx_r, r1_s, r1_r, ag_s, ag_r, ah_s, ah_r, bf_s, bf_r, pr_s, pr_r, pj_s, pj_r,
    ft_s, ft_r, ft2_s, ft2_r, ys, yr, yloc, xo_s, xf_s, x_r, ds_s, ds_r, rs_s, rs_r, fs_s, fs_r,
    pd_s, pd_r, f_s, f_r, ff_s, ff_r, d_s, d_r, q_s, q_r,
):
    x, yh, c, z, yl = [lax.axis_index(a) for a in AX]
    y = 2 * yh + yl
    p = 2 * x + yh
    me = at(x, yh, c, z, yl)
    partner = at(x, yh, 1 - c, z, yl)
    ypart = at(x, 1 - yh, c, z, yl)
    pending = []

    def rc(src, dst, ss, rs, dev):
        return pltpu.make_async_remote_copy(
            src_ref=src, dst_ref=dst, send_sem=ss, recv_sem=rs, device_id=dev, device_id_type=MESH
        )

    def send(src, dst, ss, rs, dev):
        d = rc(src, dst, ss, rs, dev)
        d.start()
        pending.append(d.wait_send)

    def recv(dst, rs):
        rc(dst, dst, rs, rs, partner).wait_recv()

    loads = [
        (gw_hbm, w_v.at[0]), (uw_hbm, w_v.at[1]), (pt_hbm, pt_v), (ftab_hbm, ftab), (dtab_hbm, dtab),
        (dt_hbm, dt_v),
    ]
    loads = [pltpu.make_async_copy(a, b, in_s.at[i]) for i, (a, b) in enumerate(loads)]
    for l in loads:
        l.start()

    def plane(rel):
        ny = rem(y + rel % 4, 4)
        return at(rem(x + rel // 4, 4), ny // 2, c, z, rem(ny, 2))

    def mate(rel):
        q = rem(p + rel // 2, 8)
        return at(q // 2, rem(q, 2), rem(c + rel % 2, 2), z, yl)

    def column(rel):
        return at(x, rem(yh + rel // 8, 2), c, rem(z + rel % 8, 8), yl)

    ypeers = [at(x, h, yl, z, c) for h in range(2)]
    me_y = [(h == yh) & (c == yl) for h in range(2)]
    barrier = pltpu.get_barrier_semaphore()

    def greet(dev):
        pl.semaphore_signal(barrier, inc=1, device_id=dev, device_id_type=MESH)

    peers = [plane(r) for r in range(1, 16)] + [mate(r) for r in range(1, 16, 2)]
    peers += [column(r) for r in range(1, 16) if r != 8]
    for o in peers:
        greet(o)
    for h in range(2):
        @pl.when(c != yl)
        def _():
            greet(ypeers[h])

    for l in loads[:3]:
        l.wait()

    def partial_base(k):
        return tn(w_v[k], pt_v[...])

    bsend[pl.ds(0, FB)] = partial_base(1 - c).astype(BF)
    bsend[pl.ds(FB, 32)] = jnp.zeros((32, 128), BF)
    loads[3].wait()
    for k in range(3):
        for m in range(8):
            fall[k, c, p, pl.ds(4 * m, 4)] = ftab[seeds[m], k]
    loads[5].wait()
    n_peers = len(peers)
    @pl.when(c == yl)
    def _():
        pl.semaphore_wait(barrier, n_peers)

    @pl.when(c != yl)
    def _():
        pl.semaphore_wait(barrier, n_peers + 2)

    e, kz = rem(z, 2), z // 2

    def low(x0):
        m = rem(x0 - kz + 4, 4)
        return jnp.where(e == 0, jnp.where(m == 1, 0, 1), jnp.where(m == 3, 1, 0))

    def zblk(r, ab):
        x0 = rem(x - r + 4, 4)
        return 2 * x0 + (low(x0) if ab == 0 else 1 - low(x0))

    own_a = low(x)

    def ysend(ab):
        mine = yh == (own_a if ab == 0 else 1 - own_a)
        for h in range(2):
            @pl.when(mine & jnp.logical_not(me_y[h]))
            def _():
                rc(dt_v.at[h], dbuf.at[yl, 2 * x + yh], ys.at[h], yr.at[yh], ypeers[h]).start()
            @pl.when(mine & me_y[h])
            def _():
                pltpu.make_async_copy(dt_hbm.at[h], dbuf.at[yl, 2 * x + yh], yloc).start()

    def wait_y(ab):
        w = own_a if ab == 0 else 1 - own_a
        here = (w == yh) & (c == yl)

        @pl.when(jnp.logical_not(here))
        def _():
            recv(dbuf.at[c, 2 * x + w], yr.at[w])

        @pl.when(here)
        def _():
            pltpu.make_async_copy(dt_hbm.at[0], dbuf.at[c, 2 * x + w], yloc).wait()

    def y_drain():
        for h in range(2):
            @pl.when(jnp.logical_not(me_y[h]))
            def _():
                rc(dt_v.at[h], dbuf.at[yl, 2 * x + yh], ys.at[h], yr.at[yh], ypeers[h]).wait_send()

    pending.append(y_drain)
    xnb = [at(rem(x + 1, 4), yh, c, z, yl), at(rem(x + 3, 4), yh, c, z, yl)]

    def dsend(r, ab):
        b = dbuf.at[c, zblk(r, ab)]
        d = rc(b, b, ds_s.at[r, ab], ds_r.at[r, ab], partner)
        pending.append(d.wait_send)
        return d

    def own_x(ab):
        b = dbuf.at[c, zblk(0, ab)]
        send(b, b, xo_s.at[0, ab], x_r.at[1, ab], xnb[0])
        send(b, b, xo_s.at[1, ab], x_r.at[3, ab], xnb[1])
        dsend(0, ab).start()

    def taker(r, ab):
        b = dbuf.at[c, zblk(r, ab)]
        d2 = dsend(r, ab)
        if r == 2:
            def run():
                recv(b, x_r.at[r, ab])
                d2.start()
            return run
        fwd = c == (0 if r == 1 else 1)
        d = rc(b, b, xf_s.at[r, ab], x_r.at[2, ab], xnb[0 if r == 1 else 1])
        pending.append(lambda: pl.when(fwd)(d.wait_send))

        def run():
            recv(b, x_r.at[r, ab])
            pl.when(fwd)(d.start)
            d2.start()

        return run

    take = {(r, ab): taker(r, ab) for r in (1, 3, 2) for ab in range(2)}

    def take_d(r, ab):
        recv(dbuf.at[1 - c, zblk(r, ab)], ds_r.at[r, ab])

    toks = pl.ds(pl.multiple_of(16 * z, 16), 16)
    own_row = 4 * yh + x
    def bpiece(t, k, first, rows):
        return lhs.at[t, k, pl.ds(pl.multiple_of(112 * first, 16), rows), pl.ds(0, 128)]

    along_x = [at(rem(x + r, 4), yh, c, z, yl) for r in range(4)]
    along_y = [at(x, rem(y + r, 4) // 2, c, z, rem(y + r, 2)) for r in range(4)]
    stage1, stage2, got1, got2 = [], [], [], []
    for r in range(1, 4):
        b = bpiece(yl, c, own_row, 112)
        stage1.append((rc(b, b, ag_s.at[r], ag_r.at[r], along_x[r]), rc(b, b, ag_s.at[r], ag_r.at[r], along_y[r])))
        xx, yy = rem(x - r + 4, 4), rem(y - r + 4, 4)
        got1.append((bpiece(yl, c, 4 * yh + xx, 112), bpiece(rem(yy, 2), c, 4 * (yy // 2) + x, 112)))
        b = bpiece(yl, c, 4 * yh, 448)
        far = []
        for n in range(4):
            f = bpiece(n // 2, c, 4 * (n % 2) + x, 112)
            far.append(rc(f, f, ah_s.at[r, n], ah_r.at[r, n], along_x[r]))
        stage2.append(([rc(b, b, ah_s.at[r, 0], ah_r.at[r, 0], along_y[r])], far))
        got2.append((
            [bpiece(rem(yy, 2), c, 4 * (yy // 2), 448)],
            [bpiece(n // 2, c, 4 * (n % 2) + xx, 112) for n in range(4)],
        ))

    def by_core(f):
        for core in range(2):
            @pl.when(c == core)
            def _():
                f(core)

    def ag_one(core):
        for d in stage1:
            d[core].start()

    def ag_two(core):
        for g, r in zip(got1, range(1, 4)):
            recv(g[core], ag_r.at[r])
        for ds in stage2:
            for d in ds[core]:
                d.start()

    def ag_end(core):
        for g, r in zip(got2, range(1, 4)):
            for n, b in enumerate(g[core]):
                recv(b, ah_r.at[r, n])

    def ag_drain(core):
        for d in stage1:
            d[core].wait_send()
        for ds in stage2:
            for d in ds[core]:
                d.wait_send()

    pending.append(lambda: by_core(ag_drain))
    fteam = [(1, 0), (1, 1), (0, 1)]

    def fdev(i):
        dh, dl = fteam[i]
        return at(x, rem(yh + dh, 2), c, z, rem(yl + dl, 2))

    def fdst(i, ks):
        return fall.at[ks, c, p] if fteam[i][1] == 0 else foth.at[yh, ks]

    def frcv(i, ks):
        dh, dl = fteam[i]
        return fall.at[ks, c, p + 1 - 2 * yh] if dl == 0 else foth.at[rem(yh + dh, 2), ks]

    gu, down = pl.ds(0, 2), pl.ds(2, 1)
    def factors_in(own, where):
        for i in where:
            recv(frcv(i, gu), ft_r.at[i])
        g = yh if own else 1 - yh
        for k in range(2):
            lanes = pl.ds(160 if own else 128, 32)
            lhs[yl, k, pl.ds(0, FB), lanes] = fall[k, c, 2 * x + g].T
            lhs[1 - yl, k, pl.ds(0, FB), lanes] = foth[g, k].T

    rowm = lax.broadcasted_iota(jnp.int32, (32, 256), 0) // 4
    lanem = lax.broadcasted_iota(jnp.int32, (32, 256), 1) // 128

    def hidden(i):
        g, cc = i // 4, rem(i, 4)
        live = rowm == 2 * cc + lanem
        for k in range(2):
            for gg in range(2):
                v = jnp.concatenate([ptt[yh if gg == 1 else 1 - yh, k]] * 2, axis=1)
                own = g == (yh if gg == 1 else 1 - yh)
                rhs[k, pl.ds(128 + 32 * gg, 32)] = jnp.where(live & own, v, 0.0).astype(BF)

        def rows(rb, _):
            r = pl.ds(pl.multiple_of(rb * HR, 16), HR)
            for t in range(2):
                ga = nn(lhs[t, 0, r], rhs[0])
                up = nn(lhs[t, 1, r], rhs[1])
                hbuf[i, t, r] = ((ga + ga * jnp.tanh(ga)) * up).astype(BF)
            return 0

        lax.fori_loop(0, FB // HR, rows, 0, unroll=HU)

    def chunk(j):
        return rem(j + 4 * (1 - yh), 8)

    sgn = 1 - 2 * c
    zn = rem(z + sgn + 8, 8)
    znd = at(x, yh, c, zn, yl)

    def part(d, i):
        return nn(dbuf[0, d], hbuf[i, 0]) + nn(dbuf[1, d], hbuf[i, 1])

    d0 = rem(z - sgn + 8, 8)

    def rsend(s, i, src):
        return rc(src, rcv.at[s, i], rs_s.at[s, i], rs_r.at[s, i], znd)


    def local_rows():
        loads[4].wait()
        for k in range(3):
            for m in range(8):
                dk[k, pl.ds(4 * m, 4)] = dtab[seeds[m], k]

        eye = lax.broadcasted_iota(jnp.int32, (128, 256), 0) == rem(lax.broadcasted_iota(jnp.int32, (128, 256), 1), 128)
        for k in range(2):
            rhs[k, 0:128] = jnp.where(eye, 1.0, 0.0).astype(BF)
            for t in range(2):
                lhs[t, k, :, pl.ds(128, 64)] = jnp.zeros((896, 64), BF)

    def base_half():
        send(bsend, brecv, bx_s, bx_r, partner)

    def base_scatter():
        bown[pl.ds(0, FB)] = partial_base(c)
        bown[pl.ds(FB, 32)] = jnp.zeros((32, 128), F32)
        recv(brecv, bx_r)
        for q in range(8):
            rows = pl.ds(112 * q, 112)
            ps[q] = (bown[rows] + brecv[rows].astype(F32)).astype(BF)
        for r in range(1, 8):
            q = rem(own_row + r, 8)
            send(ps.at[q], rsb.at[r], r1_s.at[r], r1_r.at[r], at(rem(q, 4), q // 4, c, z, yl))

    def base_sum():
        mid = pl.ds(pl.multiple_of(112 * own_row, 16), 112)
        s = bown[mid] + brecv[mid].astype(F32)
        for r in range(1, 8):
            recv(rsb.at[r], r1_r.at[r])
            s += rsb[r].astype(F32)
        s = jnp.where(c == 0, s * 0.5, s)
        bpiece(yl, c, own_row, 112)[...] = s.astype(BF)
        by_core(ag_one)

    def base_on():
        by_core(ag_two)

    def base_end():
        by_core(ag_end)
        send(lhs.at[:, c, :, pl.ds(0, 128)], lhs.at[:, c, :, pl.ds(0, 128)], bf_s, bf_r, partner)

    def base_other():
        recv(lhs.at[:, 1 - c, :, pl.ds(0, 128)], bf_r)

    def prompt_out():
        ptr = pt_v[...].astype(F32).T.astype(BF)
        psh[...] = jnp.zeros_like(psh)

        @pl.when(c == 0)
        def _():
            psh[:, 0:320] = ptr

        @pl.when(c == 1)
        def _():
            psh[:, 64:384] = ptr

        prb[c, p] = psh[toks]
        for r in range(1, 8):
            send(prb.at[c, p], prb.at[c, p], pr_s.at[r], pr_r.at[r], mate(2 * r))

    def prompt_on():
        for r in range(1, 8):
            recv(prb.at[c, rem(p - r + 8, 8)], pr_r.at[r])
        send(prb.at[c], prb.at[c], pr_s.at[0], pr_r.at[0], partner)

    def project():
        recv(prb.at[1 - c], pr_r.at[0])

        def proj_of(n, acc):
            cc, q = n // 8, rem(n, 8)
            lanes = pl.ds(pl.multiple_of(640 * q + 256 * cc, 128), 384)
            return acc + nt(prb[cc, q], dk[0:2, :, lanes].reshape(64, 384))

        acc = lax.fori_loop(0, 16, proj_of, jnp.zeros((16, 64), F32), unroll=4)
        acc = (acc / math.sqrt(D)).astype(BF).astype(F32)
        kk = lax.broadcasted_iota(jnp.int32, (16, 64), 1) // 32
        acc = jnp.where(kk == 0, acc * 0.25, acc * 0.5)
        pjs[...] = jnp.zeros_like(pjs)
        pjs[:, 0:64] = acc.astype(BF)
        pjb[yh, toks] = pjs[...]
        for r in range(1, 16):
            send(pjs, pjb.at[yh, toks], pj_s.at[r], pj_r.at[r], column(r))


    def project_in():
        for r in range(1, 16):
            hz, zz = rem(yh + r // 8, 2), rem(z - r % 8 + 8, 8)
            recv(pjb.at[hz, pl.ds(pl.multiple_of(16 * zz, 16), 16)], pj_r.at[r])
        for g in range(2):
            ptt[g] = pjb[g].astype(F32).T[0:64].reshape(2, 32, 128)

    def y_first():
        ysend(0)

    def y_second():
        ysend(1)

    def x_first():
        wait_y(0)
        own_x(0)

    def x_second():
        wait_y(1)
        own_x(1)

    def take_first():
        take[1, 0]()
        take[3, 0]()

    def take_second():
        take[1, 1]()
        take[3, 1]()

    def take_first_far():
        take[2, 0]()
        for r in range(4):
            take_d(r, 0)

    def take_second_far():
        take[2, 1]()
        for r in range(4):
            take_d(r, 1)

    def factors_far():
        for i in (0, 1):
            send(fall.at[gu, c, p], fdst(i, gu), ft_s.at[i], ft_r.at[i], fdev(i))

    def factors_near():
        send(fall.at[gu, c, p], fdst(2, gu), ft_s.at[2], ft_r.at[2], fdev(2))

    def factors_far_in():
        factors_in(False, (0, 1))
        send(fall.at[down, c, p], fdst(2, down), ft2_s.at[0], ft2_r.at[0], fdev(2))
        send(fall.at[down, c, p], fdst(0, down), ft2_s.at[1], ft2_r.at[1], fdev(0))

    def factors_near_in():
        factors_in(True, (2,))

    def hidden_ahead():
        def ahead(j, _):
            hidden(chunk(j))
            return 0

        lax.fori_loop(0, LEAD, ahead, 0)

    steps = dict(
        local_rows=local_rows,
        base_half=base_half, base_scatter=base_scatter, base_sum=base_sum, base_on=base_on, base_end=base_end,
        base_other=base_other, prompt_out=prompt_out, prompt_on=prompt_on, project=project,
        project_in=project_in, y_first=y_first, y_second=y_second, x_first=x_first, x_second=x_second,
        take_first=take_first, take_second=take_second, take_first_far=take_first_far,
        factors_far=factors_far, factors_near=factors_near, factors_far_in=factors_far_in,
        factors_near_in=factors_near_in, hidden_ahead=hidden_ahead,
    )
    for name in ORDER:
        steps[name]()

    def first(j, _):
        i = chunk(j)
        snd[i] = part(d0, i).astype(BF)
        rsend(0, i, snd.at[i]).start()

        @pl.when(j + LEAD < 8)
        def _():
            hidden(chunk(j + LEAD))

        if "take_second" not in ORDER:
            pl.when(j == TB)(take_second)

        return 0

    lax.fori_loop(0, 8, first, 0)

    for i in range(1, 8):
        q = rem(p + i, 8)
        far = q != (p + 1 - 2 * yh)
        d = rc(fall.at[:, c, p], fall.at[:, c, p], f_s.at[i], f_r.at[i], at(q // 2, rem(q, 2), c, z, yl))
        pl.when(far)(d.start)
        pending.append(functools.partial(pl.when(far), d.wait_send))
    for m in range(8):
        fitall[c, p, pl.ds(m, 1)] = jnp.full((1, 128), fit[m], F32)

    def dlanes(q, cc):
        return pl.ds(pl.multiple_of(640 * q + 256 * cc, 128), 384)

    dall[:, c, p] = dk[:, :, dlanes(p, c)]
    for r in range(1, 16):
        q, cc = rem(p + r // 2, 8), rem(c + r % 2, 2)
        send(dk.at[:, :, dlanes(q, cc)], dall.at[:, c, p], d_s.at[r], d_r.at[r], mate(r))
        send(fitall.at[c, p], fitall.at[c, p], q_s.at[r], q_r.at[r], mate(r))

    recv(frcv(2, down), ft2_r.at[0])
    tot = jnp.zeros((32, 128), F32)
    for cc in range(4):
        i = 4 * yh + cc
        q = nn(fall[2, c, p], hbuf[i, yl]) + nn(foth[yh, 2], hbuf[i, 1 - yl])
        q = jnp.where(rowm == 2 * cc + lanem, q, 0.0)
        tot += q[:, :128] + q[:, 128:]
    pdc[...] = tot.astype(BF)
    for r in range(1, 8):
        send(pdc, pdb.at[r], pd_s.at[r], pd_r.at[r], column(r))

    take_second_far()

    recv(frcv(0, down), ft2_r.at[1])
    fwd_f = rc(fall.at[:, c], fall.at[:, c], ff_s, ff_r, partner)
    pending.append(fwd_f.wait_send)

    def collect_f():
        for i in range(1, 8):
            q = rem(p - i + 8, 8)
            far = q != (p + 1 - 2 * yh)
            pl.when(far)(functools.partial(recv, fall.at[:, c, q], f_r.at[i]))
        fwd_f.start()

    def collect_d():
        for r in range(1, 16):
            q, cc = rem(p - r // 2 + 8, 8), rem(c + r % 2, 2)
            recv(dall.at[:, cc, q], d_r.at[r])
            recv(fitall.at[cc, q], q_r.at[r])
        fv = fitall[...].reshape(128, 128)
        mean = jnp.sum(fv, axis=0, keepdims=True) / 128
        spread = jnp.sum((fv - mean) ** 2, axis=0, keepdims=True) / 128
        sc = (fv - mean) / jnp.sqrt(spread + 1.0)
        for i in range(16):
            v = jnp.broadcast_to(sc[8 * i : 8 * i + 8].reshape(8, 1, 128), (8, 4, 128))
            score[i // 8, i % 8] = v.reshape(32, 128)

    def weigh(k):
        def one(g, _):
            a, b = g // 8, rem(g, 8)
            sc = score[a, b]
            w = dall[k, a, b].astype(F32) * jnp.concatenate([sc] * 3, axis=1)
            dall[k, a, b] = w.astype(BF)
            return 0
        lax.fori_loop(0, 16, one, 0)
        wt[k] = dall[k].reshape(512, 384).T

    def delta(k, half):
        r = pl.ds(pl.multiple_of(64 * c + 160 * half, 16), 160)
        v = nn(wt[k, r], fall[k].reshape(512, FB)) * (1.0 / math.sqrt(512))
        del_ref[k, pl.ds(pl.multiple_of(160 * half, 16), 160)] = v.astype(BF)

    def noise_in():
        tot = pdc[...].astype(F32)
        for r in range(1, 8):
            recv(pdb.at[r], pd_r.at[r])
            tot += pdb[r].astype(F32)
        pdt[...] = (tot / math.sqrt(FFW)).astype(BF).astype(F32) * 0.5
        a2t[...] = dk[2, :, pl.ds(pl.multiple_of(640 * z + 256 * yl, 128), 384)].T

    def noise(j):
        live = rowm == 2 * j + lanem
        pm = jnp.where(live, jnp.concatenate([pdt[...]] * 2, axis=1), 0.0).astype(BF)
        for h in range(2):
            nbuf[h, j] = nn(a2t[pl.ds(pl.multiple_of(64 * yl + 160 * h, 16), 160)], pm)

    def middle(n, _):
        s, j = n // 8 + 1, rem(n, 8)
        i = chunk(j)
        pp = part(rem(z - sgn * (1 + s) + 16, 8), i)
        recv(rcv.at[s - 1, i], rs_r.at[s - 1, i])
        rcv[s - 1, i] = (pp + rcv[s - 1, i].astype(F32)).astype(BF)
        rsend(s, i, rcv.at[s - 1, i]).start()
        rsend(s - 1, i, rcv.at[s, i]).wait_send()

        @pl.when((s == 2) & (j == 3))
        def _():
            noise_in()

        @pl.when((s == 3) & (j < 4))
        def _():
            noise(j)

        @pl.when((s == 5) & (j == 0))
        def _():
            collect_f()

        @pl.when((s == 6) & (j == 0))
        def _():
            collect_d()

        @pl.when((s == 6) & (j >= 1) & (j < 4))
        def _():
            weigh(j - 1)

        @pl.when((s == 6) & (j == 3))
        def _():
            recv(fall.at[:, 1 - c], ff_r)

        @pl.when((s == 6) & (j >= 4))
        def _():
            delta((j - 4) // 2, rem(j, 2))

        return 0

    lax.fori_loop(0, 48, middle, 0)

    def last(j):
        i = chunk(j)
        pp = part(z, i)
        recv(rcv.at[6, i], rs_r.at[6, i])
        return pp + rcv[6, i].astype(F32)

    def last_far(j, _):
        fsnd[j] = last(j).astype(BF)
        rc(fsnd.at[j], fin.at[j], fs_s.at[j], fs_r.at[j], ypart).start()

        @pl.when(j < 2)
        def _():
            delta(2, j)

        return 0

    lax.fori_loop(0, 4, last_far, 0)

    def put(j, h, w):
        for m in range(2):
            out_ref[2 * j + m, pl.ds(pl.multiple_of(160 * h, 16), 160)] = w[:, 128 * m : 128 * (m + 1)].astype(BF)

    def last_near(j, _):
        put(j, yh, last(j + 4) + nbuf[yh, j])
        return 0

    lax.fori_loop(0, 4, last_near, 0)

    def finish(j, _):
        rc(fsnd.at[j], fin.at[j], fs_s.at[j], fs_r.at[j], ypart).wait()
        put(j, 1 - yh, fin[j].astype(F32) + nbuf[1 - yh, j])
        return 0

    lax.fori_loop(0, 4, finish, 0)

    for w in pending:
        w()

    def drain(i, _):
        rsend(6, i, snd.at[i]).wait_send()
        return 0

    lax.fori_loop(0, 8, drain, 0)


def call_step(*arrays):
    arrays = [pltpu.with_memory_space_constraint(v, pltpu.HBM) for v in arrays]
    v = pl.BlockSpec(memory_space=pltpu.VMEM)
    a = pl.BlockSpec(memory_space=pltpu.HBM)
    sm = pl.BlockSpec(memory_space=pltpu.SMEM)
    dma = pltpu.SemaphoreType.DMA
    vm = pltpu.VMEM
    return pl.pallas_call(
        step_kernel,
        out_shape=[
            jax.ShapeDtypeStruct((8, 320, 128), BF),
            jax.ShapeDtypeStruct((3, 320, FB), BF),
        ],
        in_specs=[a, a, a, a, a, a, sm, sm],
        out_specs=[v, v],
        scratch_shapes=[
            vm((320, 128), BF), vm((2, 320, FB), BF), vm((2, 160, FB), BF), vm((16, 3, 4, D), BF), vm((16, 3, 4, FB), BF),
            vm((3, 32, D), BF), vm((3, 2, 8, 32, FB), BF), vm((2, 3, 32, FB), BF),
            vm((2, 8, 160, FB), BF), vm((8, 2, FB, 256), BF), vm((8, 160, 256), BF),
            vm((7, 8, 160, 256), BF), vm((4, 160, 256), BF), vm((4, 160, 256), BF),
            vm((896, 128), BF), vm((896, 128), BF), vm((896, 128), F32), vm((8, 112, 128), BF),
            vm((8, 112, 128), BF), vm((2, 2, 896, 192), BF), vm((2, 192, 256), BF),
            vm((128, 384), BF), vm((2, 8, 16, 384), BF), vm((16, 128), BF), vm((2, 128, 128), BF),
            vm((2, 2, 32, 128), F32),
            vm((32, 128), BF), vm((8, 32, 128), BF), vm((32, 128), F32), vm((3, 2, 8, 32, 384), BF),
            vm((2, 8, 8, 128), F32), vm((2, 8, 32, 128), F32), vm((3, 384, 512), BF), vm((384, 32), BF), vm((2, 4, 160, 256), F32),
            dma((6,)), dma(()), dma(()), dma((8,)), dma((8,)), dma((4,)), dma((4,)), dma((4, 4)), dma((4, 4)), dma(()), dma(()),
            dma((8,)), dma((8,)), dma((16,)), dma((16,)),
            dma((3,)), dma((3,)), dma((2,)), dma((2,)), dma((2,)), dma((2,)), dma(()), dma((2, 2)), dma((4, 2)), dma((4, 2)),
            dma((4, 2)), dma((4, 2)), dma((7, 8)), dma((7, 8)), dma((4,)), dma((4,)),
            dma((8,)), dma((8,)), dma((8,)), dma((8,)), dma(()), dma(()), dma((16,)), dma((16,)),
            dma((16,)), dma((16,)),
        ],
        compiler_params=pltpu.CompilerParams(
            collective_id=0, has_side_effects=True, vmem_limit_bytes=44 << 20
        ),
        name="es_step",
    )(*arrays)


EMIT_LIM = 4 << 20


def emit_kernel(out, deltas, o_hbm, g_hbm, u_hbm, d_hbm, sems):
    pairs = [(deltas.at[0], g_hbm), (deltas.at[1], u_hbm), (deltas.at[2], d_hbm), (out, o_hbm)]
    copies = [pltpu.make_async_copy(a, b, sems.at[i]) for i, (a, b) in enumerate(pairs)]
    for d in copies:
        d.start()
    for d in copies:
        d.wait()


def emit(out, deltas):
    v = pl.BlockSpec(memory_space=pltpu.VMEM)
    a = pl.BlockSpec(memory_space=pltpu.HBM)
    one = jax.ShapeDtypeStruct((320, FB), BF)
    return pl.pallas_call(
        emit_kernel,
        out_shape=[jax.ShapeDtypeStruct((8, 320, 128), BF), one, one, one],
        in_specs=[v, v],
        out_specs=[a, a, a, a],
        scratch_shapes=[pltpu.SemaphoreType.DMA((4,))],
        compiler_params=pltpu.CompilerParams(vmem_limit_bytes=EMIT_LIM),
        name="emit",
    )(out, deltas)


def shards(prompt_acts, gate_weight, up_weight, down_weight, d_table, f_table, seeds, fitness):
    out, deltas = call_step(
        prompt_acts.T, gate_weight, up_weight, down_weight.T.reshape(2, 160, FB), d_table, f_table,
        seeds, fitness,
    )
    out, dg, du, dd = emit(out, deltas)
    return out.transpose(0, 2, 1), dg, du, dd.T


def solution(mesh):
    split = Mesh(mesh.devices.reshape(4, 2, 2, 8, 2), AX)
    placed = (
        P(None, MEMBER), P(MEMBER, TENSOR), P(MEMBER, TENSOR), P(TENSOR, MEMBER),
        P(MEMBER, None, None, None), P(MEMBER, None, None, TENSOR), P(MEMBER), P(MEMBER),
    )
    return jax.shard_map(
        shards, mesh=split, in_specs=placed,
        out_specs=(P(MEMBER, None, TENSOR), P(MEMBER, TENSOR), P(MEMBER, TENSOR), P(TENSOR, MEMBER)),
        check_vma=False,
    )
```

```python
import functools
import math

import jax
import jax.numpy as jnp
from jax import lax
from jax.experimental import pallas as pl
from jax.experimental.pallas import tpu as pltpu
from jax.sharding import Mesh
from jax.sharding import PartitionSpec as P

D = 5120
FFW = 13824
FB = 864
AX = ("x", "yh", "c", "z", "yl")
MEMBER = ("x", "yh", "c")
TENSOR = ("z", "yl")
MESH = pl.DeviceIdType.MESH
BF = jnp.bfloat16
F32 = jnp.float32
HR = 864
HU = 1
LEAD = 3
TB = 0
TF = 6
CF = 32
CD = 40
DS = 1
ORDER = (
    "y_first",
    "y_first_b",
    "y_second",
    "base_half",
    "y_second_b",
    "base_scatter",
    "prompt_out",
    "base_mid",
    "x_first",
    "base_sum",
    "x_first_b",
    "local_rows",
    "factors_far",
    "factors_diag",
    "prompt_on",
    "take_first",
    "base_on",
    "project",
    "factors_near",
    "take_first_b",
    "project_in",
    "x_second",
    "x_second_b",
    "factors_far_in",
    "down_out",
    "base_end",
    "base_other",
    "take_first_far",
    "hidden_ahead",
    "factors_near_in",
    "take_second",
    "first_in",
)


def rem(a, n):
    return lax.rem(a, n)


def at(x, yh, c, z, yl):
    return {"x": x, "yh": yh, "c": c, "z": z, "yl": yl}


def tn(a, b):
    return lax.dot_general(a, b, (((0,), (0,)), ((), ())), preferred_element_type=F32)


def nt(a, b):
    return lax.dot_general(a, b, (((1,), (1,)), ((), ())), preferred_element_type=F32)


def nn(a, b):
    return jnp.dot(a, b, preferred_element_type=F32)


def step_kernel(
    pt_hbm, gw_hbm, uw_hbm, dt_hbm, dtab_hbm, ftab_hbm, seeds_hbm, fit_hbm,
    out_ref, del_ref,
    seeds, fit, pt_v, w_v, dt_v, dtab, ftab, dk, fall, foth, dbuf, hbuf, snd, rcv, fin, fsnd,
    bsend, brecv, bown, ps, rsb, rsend2, rrecv2, lhs, rhs, psh, prb, pjs, pjb, ptt,
    pdc, pdb, pdt, dall, fitall, score, wt, a2t, nbuf,
    in_s, bx_s, bx_r, r1_s, r1_r, ag_s, ag_r, ah_s, ah_r, bf_s, bf_r, pr_s, pr_r, pj_s, pj_r,
    ft_s, ft_r, ft2_s, ft2_r, ys, yr, yloc, xo_s, xf_s, x_r, ds_s, ds_r, rs_s, rs_r, fs_s, fs_r,
    pd_s, pd_r, f_s, f_r, ff_s, ff_r, d_s, d_r, q_s, q_r,
):
    x, yh, c, z, yl = [lax.axis_index(a) for a in AX]
    y = 2 * yh + yl
    p = 2 * x + yh
    me = at(x, yh, c, z, yl)
    partner = at(x, yh, 1 - c, z, yl)
    ypart = at(x, 1 - yh, c, z, yl)
    pending = []

    def rc(src, dst, ss, rs, dev):
        return pltpu.make_async_remote_copy(
            src_ref=src, dst_ref=dst, send_sem=ss, recv_sem=rs, device_id=dev, device_id_type=MESH
        )

    def send(src, dst, ss, rs, dev):
        d = rc(src, dst, ss, rs, dev)
        d.start()
        pending.append(d.wait_send)

    def recv(dst, rs):
        rc(dst, dst, rs, rs, partner).wait_recv()

    loads = [
        (gw_hbm, w_v.at[0]), (uw_hbm, w_v.at[1]), (pt_hbm, pt_v), (ftab_hbm, ftab), (dtab_hbm, dtab),
        (dt_hbm, dt_v), (seeds_hbm, seeds), (fit_hbm, fit),
    ]
    loads = [pltpu.make_async_copy(a, b, in_s.at[i]) for i, (a, b) in enumerate(loads)]
    for i in (5, 2, 0, 1, 6, 7, 3, 4):
        loads[i].start()

    def plane(rel):
        ny = rem(y + rel % 4, 4)
        return at(rem(x + rel // 4, 4), ny // 2, c, z, rem(ny, 2))

    def mate(rel):
        q = rem(p + rel // 2, 8)
        return at(q // 2, rem(q, 2), rem(c + rel % 2, 2), z, yl)

    def column(rel):
        return at(x, rem(yh + rel // 8, 2), c, rem(z + rel % 8, 8), yl)

    ypeers = [at(x, h, yl, z, c) for h in range(2)]
    me_y = [(h == yh) & (c == yl) for h in range(2)]
    barrier = pltpu.get_barrier_semaphore()

    def greet(dev):
        pl.semaphore_signal(barrier, inc=1, device_id=dev, device_id_type=MESH)

    peers = [plane(1), plane(3)] + [mate(r) for r in range(1, 16)]
    peers += [column(r) for r in range(1, 16) if r != 8]
    for o in peers:
        greet(o)
    @pl.when(c != yl)
    def _():
        for h in range(2):
            greet(ypeers[h])

    def partial_base(k):
        return tn(w_v[k], pt_v[...])

    loads[5].wait()
    n_peers = len(peers)
    @pl.when(c == yl)
    def _():
        pl.semaphore_wait(barrier, n_peers)

    @pl.when(c != yl)
    def _():
        pl.semaphore_wait(barrier, n_peers + 2)

    e, kz = rem(z, 2), z // 2

    def low(x0):
        m = rem(x0 - kz + 4, 4)
        return jnp.where(e == 0, jnp.where(m == 1, 0, 1), jnp.where(m == 3, 1, 0))

    def zblk(r, ab):
        x0 = rem(x - r + 4, 4)
        return 2 * x0 + (low(x0) if ab == 0 else 1 - low(x0))

    own_a = low(x)

    def half(b, part):
        return b.at[pl.ds(80 * part, 80)]

    def ycopy(h, part):
        dst = half(dbuf.at[yl, 2 * x + yh], part)
        return rc(half(dt_v.at[h], part), dst, ys.at[h, part], yr.at[yh, part], ypeers[h])

    def ylocal(h, part):
        return pltpu.make_async_copy(half(dt_hbm.at[h], part), half(dbuf.at[yl, 2 * x + yh], part), yloc.at[part])

    def ysend(ab, part):
        mine = yh == (own_a if ab == 0 else 1 - own_a)
        for h in range(2):
            @pl.when(mine & jnp.logical_not(me_y[h]))
            def _():
                ycopy(h, part).start()
            @pl.when(mine & me_y[h])
            def _():
                ylocal(h, part).start()

    def wait_y(ab, part):
        w = own_a if ab == 0 else 1 - own_a
        here = (w == yh) & (c == yl)

        @pl.when(jnp.logical_not(here))
        def _():
            recv(half(dbuf.at[c, 2 * x + w], part), yr.at[w, part])

        @pl.when(here)
        def _():
            ylocal(0, part).wait()

    def y_drain():
        for h in range(2):
            @pl.when(jnp.logical_not(me_y[h]))
            def _():
                for part in range(2):
                    ycopy(h, part).wait_send()

    pending.append(y_drain)
    xnb = [at(rem(x + 1, 4), yh, c, z, yl), at(rem(x + 3, 4), yh, c, z, yl)]

    def dsend(r, ab):
        b = dbuf.at[c, zblk(r, ab)]
        d = rc(b, b, ds_s.at[r, ab], ds_r.at[r, ab], partner)
        pending.append(d.wait_send)
        return d

    def own_x(ab, part):
        b = dbuf.at[c, zblk(0, ab)]
        if part == 1:
            dsend(0, ab).start()
        b = half(b, part)
        send(b, b, xo_s.at[0, ab, part], x_r.at[1, ab, part], xnb[0])
        send(b, b, xo_s.at[1, ab, part], x_r.at[3, ab, part], xnb[1])

    def taker(r, ab):
        b = dbuf.at[c, zblk(r, ab)]
        d2 = dsend(r, ab)
        fwd = c == (0 if r == 1 else 1)
        hops = []
        for part in range(2 if r != 2 else 0):
            h = half(b, part)
            d = rc(h, h, xf_s.at[r, ab, part], x_r.at[2, ab, part], xnb[0 if r == 1 else 1])
            hops.append(d)
            pending.append(functools.partial(pl.when(fwd), d.wait_send))

        def run(part):
            recv(half(b, part), x_r.at[r, ab, part])
            if r != 2:
                pl.when(fwd)(hops[part].start)
            if part == 1:
                d2.start()

        return run

    take = {(r, ab): taker(r, ab) for r in (1, 3, 2) for ab in range(2)}

    def take_d(r, ab):
        recv(dbuf.at[1 - c, zblk(r, ab)], ds_r.at[r, ab])

    toks = pl.ds(pl.multiple_of(16 * z, 16), 16)
    own_row = 4 * yh + x
    def bpiece(t, k, first, rows):
        return lhs.at[t, k, pl.ds(pl.multiple_of(112 * first, 16), rows), pl.ds(0, 128)]

    along_x = [at(rem(x + r, 4), yh, c, z, yl) for r in range(4)]
    along_y = [at(x, rem(y + r, 4) // 2, c, z, rem(y + r, 2)) for r in range(4)]
    stage1, stage2, got1, got2 = [], [], [], []
    for r in range(1, 4):
        b = bpiece(yl, c, own_row, 112)
        stage1.append((rc(b, b, ag_s.at[r], ag_r.at[r], along_x[r]), rc(b, b, ag_s.at[r], ag_r.at[r], along_y[r])))
        xx, yy = rem(x - r + 4, 4), rem(y - r + 4, 4)
        got1.append((bpiece(yl, c, 4 * yh + xx, 112), bpiece(rem(yy, 2), c, 4 * (yy // 2) + x, 112)))
        b = bpiece(yl, c, 4 * yh, 448)
        far = []
        for n in range(4):
            f = bpiece(n // 2, c, 4 * (n % 2) + x, 112)
            far.append(rc(f, f, ah_s.at[r, n], ah_r.at[r, n], along_x[r]))
        stage2.append(([rc(b, b, ah_s.at[r, 0], ah_r.at[r, 0], along_y[r])], far))
        got2.append((
            [bpiece(rem(yy, 2), c, 4 * (yy // 2), 448)],
            [bpiece(n // 2, c, 4 * (n % 2) + xx, 112) for n in range(4)],
        ))

    def by_core(f):
        for core in range(2):
            @pl.when(c == core)
            def _():
                f(core)

    def ag_one(core):
        for d in stage1:
            d[core].start()

    def ag_two(core):
        for g, r in zip(got1, range(1, 4)):
            recv(g[core], ag_r.at[r])
        for ds in stage2:
            for d in ds[core]:
                d.start()

    def ag_end(core):
        for g, r in zip(got2, range(1, 4)):
            for n, b in enumerate(g[core]):
                recv(b, ah_r.at[r, n])

    def ag_drain(core):
        for d in stage1:
            d[core].wait_send()
        for ds in stage2:
            for d in ds[core]:
                d.wait_send()

    pending.append(lambda: by_core(ag_drain))
    fteam = [(1, 0), (1, 1), (0, 1)]

    def fdev(i):
        dh, dl = fteam[i]
        return at(x, rem(yh + dh, 2), c, z, rem(yl + dl, 2))

    def fdst(i, ks):
        return fall.at[ks, c, p] if fteam[i][1] == 0 else foth.at[yh, ks]

    def frcv(i, ks):
        dh, dl = fteam[i]
        return fall.at[ks, c, p + 1 - 2 * yh] if dl == 0 else foth.at[rem(yh + dh, 2), ks]

    gu, down = pl.ds(0, 2), pl.ds(2, 1)
    def factors_in(own, where):
        for i in where:
            recv(frcv(i, gu), ft_r.at[i])
        g = yh if own else 1 - yh
        for k in range(2):
            lanes = pl.ds(160 if own else 128, 32)
            lhs[yl, k, pl.ds(0, FB), lanes] = fall[k, c, 2 * x + g].T
            lhs[1 - yl, k, pl.ds(0, FB), lanes] = foth[g, k].T

    rowm = lax.broadcasted_iota(jnp.int32, (32, 256), 0) // 4
    lanem = lax.broadcasted_iota(jnp.int32, (32, 256), 1) // 128

    def hidden(i):
        g, cc = i // 4, rem(i, 4)
        live = rowm == 2 * cc + lanem
        for k in range(2):
            for gg in range(2):
                v = jnp.concatenate([ptt[yh if gg == 1 else 1 - yh, k]] * 2, axis=1)
                own = g == (yh if gg == 1 else 1 - yh)
                rhs[k, pl.ds(128 + 32 * gg, 32)] = jnp.where(live & own, v, 0.0).astype(BF)

        def rows(rb, _):
            r = pl.ds(pl.multiple_of(rb * HR, 16), HR)
            for t in range(2):
                ga = nn(lhs[t, 0, r], rhs[0])
                up = nn(lhs[t, 1, r], rhs[1])
                hbuf[i, t, r] = ((ga + ga * jnp.tanh(ga)) * up).astype(BF)
            return 0

        lax.fori_loop(0, FB // HR, rows, 0, unroll=HU)

    def chunk(j):
        return rem(j + 4 * (1 - yh), 8)

    sgn = 1 - 2 * c
    zn = rem(z + sgn + 8, 8)
    znd = at(x, yh, c, zn, yl)

    def part(d, i):
        return nn(dbuf[0, d], hbuf[i, 0]) + nn(dbuf[1, d], hbuf[i, 1])

    d0 = rem(z - sgn + 8, 8)

    def rsend(s, i, src):
        return rc(src, rcv.at[s, i], rs_s.at[s, i], rs_r.at[s, i], znd)


    def local_rows():
        for i in (6, 7, 3):
            loads[i].wait()
        for k in range(3):
            for m in range(8):
                fall[k, c, p, pl.ds(4 * m, 4)] = ftab[seeds[m], k]
        loads[4].wait()
        for k in range(3):
            for m in range(8):
                dk[k, pl.ds(4 * m, 4)] = dtab[seeds[m], k]

        eye = lax.broadcasted_iota(jnp.int32, (128, 256), 0) == rem(lax.broadcasted_iota(jnp.int32, (128, 256), 1), 128)
        for k in range(2):
            rhs[k, 0:128] = jnp.where(eye, 1.0, 0.0).astype(BF)
            for t in range(2):
                lhs[t, k, :, pl.ds(128, 64)] = jnp.zeros((896, 64), BF)

    def base_half():
        for i in range(3):
            loads[i].wait()
        bsend[pl.ds(0, FB)] = partial_base(1 - c).astype(BF)
        bsend[pl.ds(FB, 32)] = jnp.zeros((32, 128), BF)
        send(bsend, brecv, bx_s, bx_r, partner)

    def base_scatter():
        bown[pl.ds(0, FB)] = partial_base(c)
        bown[pl.ds(FB, 32)] = jnp.zeros((32, 128), F32)
        recv(brecv, bx_r)
        for q in range(8):
            rows = pl.ds(112 * q, 112)
            ps[q // 4, q % 4] = (bown[rows] + brecv[rows].astype(F32)).astype(BF)
        for r in range(1, 4):
            xx = rem(x + r, 4)
            send(ps.at[:, xx], rsb.at[r], r1_s.at[r], r1_r.at[r], at(xx, yh, c, z, yl))

    def own_sum(h):
        mid = pl.ds(pl.multiple_of(112 * (4 * h + x), 16), 112)
        s = bown[mid] + brecv[mid].astype(F32)
        for r in range(1, 4):
            s += rsb[r, h].astype(F32)
        return s

    def base_mid():
        for r in range(1, 4):
            recv(rsb.at[r], r1_r.at[r])
        rsend2[...] = own_sum(1 - yh).astype(BF)
        send(rsend2, rrecv2, r1_s.at[0], r1_r.at[0], ypart)

    def base_sum():
        recv(rrecv2, r1_r.at[0])
        s = own_sum(yh) + rrecv2[...].astype(F32)
        s = jnp.where(c == 0, s * 0.5, s)
        bpiece(yl, c, own_row, 112)[...] = s.astype(BF)
        by_core(ag_one)

    def base_on():
        by_core(ag_two)

    def base_end():
        by_core(ag_end)
        send(lhs.at[:, c, :, pl.ds(0, 128)], lhs.at[:, c, :, pl.ds(0, 128)], bf_s, bf_r, partner)

    def base_other():
        recv(lhs.at[:, 1 - c, :, pl.ds(0, 128)], bf_r)

    def prompt_out():
        ptr = pt_v[...].astype(F32).T.astype(BF)
        psh[...] = jnp.zeros_like(psh)

        @pl.when(c == 0)
        def _():
            psh[:, 0:320] = ptr

        @pl.when(c == 1)
        def _():
            psh[:, 64:384] = ptr

        prb[c, p] = psh[toks]
        for r in range(1, 8):
            send(prb.at[c, p], prb.at[c, p], pr_s.at[r], pr_r.at[r], mate(2 * r))

    def prompt_on():
        for r in range(1, 8):
            recv(prb.at[c, rem(p - r + 8, 8)], pr_r.at[r])
        send(prb.at[c], prb.at[c], pr_s.at[0], pr_r.at[0], partner)

    def project():
        recv(prb.at[1 - c], pr_r.at[0])

        def proj_of(n, acc):
            cc, q = n // 8, rem(n, 8)
            lanes = pl.ds(pl.multiple_of(640 * q + 256 * cc, 128), 384)
            return acc + nt(prb[cc, q], dk[0:2, :, lanes].reshape(64, 384))

        acc = lax.fori_loop(0, 16, proj_of, jnp.zeros((16, 64), F32), unroll=4)
        acc = (acc / math.sqrt(D)).astype(BF).astype(F32)
        kk = lax.broadcasted_iota(jnp.int32, (16, 64), 1) // 32
        acc = jnp.where(kk == 0, acc * 0.25, acc * 0.5)
        pjs[...] = jnp.zeros_like(pjs)
        pjs[:, 0:64] = acc.astype(BF)
        pjb[yh, toks] = pjs[...]
        for r in range(1, 16):
            send(pjs, pjb.at[yh, toks], pj_s.at[r], pj_r.at[r], column(r))


    def project_in():
        for r in range(1, 16):
            hz, zz = rem(yh + r // 8, 2), rem(z - r % 8 + 8, 8)
            recv(pjb.at[hz, pl.ds(pl.multiple_of(16 * zz, 16), 16)], pj_r.at[r])
        for g in range(2):
            ptt[g] = pjb[g].astype(F32).T[0:64].reshape(2, 32, 128)

    def y_first():
        ysend(0, 0)

    def y_first_b():
        ysend(0, 1)

    def y_second():
        ysend(1, 0)

    def y_second_b():
        ysend(1, 1)

    def x_first():
        wait_y(0, 0)
        own_x(0, 0)

    def x_first_b():
        wait_y(0, 1)
        own_x(0, 1)

    def x_second():
        wait_y(1, 0)
        own_x(1, 0)

    def x_second_b():
        wait_y(1, 1)
        own_x(1, 1)

    def down_out():
        send(fall.at[down, c, p], fdst(2, down), ft2_s.at[0], ft2_r.at[0], fdev(2))
        send(fall.at[down, c, p], fdst(0, down), ft2_s.at[1], ft2_r.at[1], fdev(0))

    def take_first():
        take[1, 0](0)
        take[3, 0](0)

    def take_first_b():
        take[1, 0](1)
        take[3, 0](1)

    def take_second():
        take[1, 1](0)
        take[3, 1](0)

    def take_second_b():
        take[1, 1](1)
        take[3, 1](1)

    def take_first_far():
        for part in range(2):
            take[2, 0](part)

    def first_in():
        for r in range(4):
            take_d(r, 0)

    def take_second_far():
        for part in range(2):
            take[2, 1](part)

    def second_in():
        for r in range(4):
            take_d(r, 1)

    def factors_far():
        send(fall.at[gu, c, p], fdst(0, gu), ft_s.at[0], ft_r.at[0], fdev(0))

    def factors_diag():
        send(fall.at[gu, c, p], fdst(1, gu), ft_s.at[1], ft_r.at[1], fdev(1))

    def factors_near():
        send(fall.at[gu, c, p], fdst(2, gu), ft_s.at[2], ft_r.at[2], fdev(2))

    def factors_far_in():
        factors_in(False, (0, 1))

    def factors_near_in():
        factors_in(True, (2,))

    def hidden_ahead():
        def ahead(j, _):
            hidden(chunk(j))
            return 0

        lax.fori_loop(0, LEAD, ahead, 0)

    steps = dict(
        local_rows=local_rows, down_out=down_out,
        base_half=base_half, base_scatter=base_scatter, base_mid=base_mid, base_sum=base_sum, base_on=base_on, base_end=base_end,
        base_other=base_other, prompt_out=prompt_out, prompt_on=prompt_on, project=project,
        project_in=project_in, y_first=y_first, y_second=y_second, y_first_b=y_first_b, y_second_b=y_second_b, x_first=x_first, x_second=x_second, x_first_b=x_first_b, x_second_b=x_second_b,
        take_first=take_first, take_first_b=take_first_b, take_second_b=take_second_b, take_second=take_second, take_first_far=take_first_far, first_in=first_in,
        factors_far=factors_far, factors_diag=factors_diag, factors_near=factors_near, factors_far_in=factors_far_in,
        factors_near_in=factors_near_in, hidden_ahead=hidden_ahead,
    )
    for name in ORDER:
        steps[name]()

    def first(j, _):
        i = chunk(j)
        snd[i] = part(d0, i).astype(BF)
        rsend(0, i, snd.at[i]).start()

        @pl.when(j + LEAD < 8)
        def _():
            hidden(chunk(j + LEAD))

        if "take_second" not in ORDER:
            pl.when(j == TB)(take_second)
        if "take_second_b" not in ORDER:
            pl.when(j == TB)(take_second_b)
        pl.when(j == TF)(take_second_far)

        return 0

    lax.fori_loop(0, 8, first, 0)

    for i in range(1, 8):
        q = rem(p + i, 8)
        far = q != (p + 1 - 2 * yh)
        d = rc(fall.at[:, c, p], fall.at[:, c, p], f_s.at[i], f_r.at[i], at(q // 2, rem(q, 2), c, z, yl))
        pl.when(far)(d.start)
        pending.append(functools.partial(pl.when(far), d.wait_send))
    for m in range(8):
        fitall[c, p, pl.ds(m, 1)] = jnp.full((1, 128), fit[m], F32)

    def dlanes(q, cc):
        return pl.ds(pl.multiple_of(640 * q + 256 * cc, 128), 384)

    dall[:, c, p] = dk[:, :, dlanes(p, c)]
    for r in range(1, 16):
        q, cc = rem(p + r // 2, 8), rem(c + r % 2, 2)
        send(dk.at[:, :, dlanes(q, cc)], dall.at[:, c, p], d_s.at[r], d_r.at[r], mate(r))
        send(fitall.at[c, p], fitall.at[c, p], q_s.at[r], q_r.at[r], mate(r))

    second_in()

    recv(frcv(0, down), ft2_r.at[1])
    fwd_f = rc(fall.at[:, c], fall.at[:, c], ff_s, ff_r, partner)
    pending.append(fwd_f.wait_send)

    def collect_f():
        for i in range(1, 8):
            q = rem(p - i + 8, 8)
            far = q != (p + 1 - 2 * yh)
            pl.when(far)(functools.partial(recv, fall.at[:, c, q], f_r.at[i]))
        fwd_f.start()

    def collect_d():
        for r in range(1, 16):
            q, cc = rem(p - r // 2 + 8, 8), rem(c + r % 2, 2)
            recv(dall.at[:, cc, q], d_r.at[r])
            recv(fitall.at[cc, q], q_r.at[r])
        fv = fitall[...].reshape(128, 128)
        mean = jnp.sum(fv, axis=0, keepdims=True) / 128
        spread = jnp.sum((fv - mean) ** 2, axis=0, keepdims=True) / 128
        sc = (fv - mean) / jnp.sqrt(spread + 1.0)
        for i in range(16):
            v = jnp.broadcast_to(sc[8 * i : 8 * i + 8].reshape(8, 1, 128), (8, 4, 128))
            score[i // 8, i % 8] = v.reshape(32, 128)

    def weigh(k):
        def one(g, _):
            a, b = g // 8, rem(g, 8)
            sc = score[a, b]
            w = dall[k, a, b].astype(F32) * jnp.concatenate([sc] * 3, axis=1)
            dall[k, a, b] = w.astype(BF)
            return 0
        lax.fori_loop(0, 16, one, 0)
        wt[k] = dall[k].reshape(512, 384).T

    def delta(k, half):
        r = pl.ds(pl.multiple_of(64 * c + 160 * half, 16), 160)
        v = nn(wt[k, r], fall[k].reshape(512, FB)) * (1.0 / math.sqrt(512))
        del_ref[k, pl.ds(pl.multiple_of(160 * half, 16), 160)] = v.astype(BF)

    pd_out = [rc(pdc, pdb.at[r], pd_s.at[r], pd_r.at[r], column(r)) for r in range(1, 8)]
    pending.extend(d.wait_send for d in pd_out)

    def down_sums():
        recv(frcv(2, down), ft2_r.at[0])
        tot = jnp.zeros((32, 128), F32)
        for cc in range(4):
            i = 4 * yh + cc
            q = nn(fall[2, c, p], hbuf[i, yl]) + nn(foth[yh, 2], hbuf[i, 1 - yl])
            q = jnp.where(rowm == 2 * cc + lanem, q, 0.0)
            tot += q[:, :128] + q[:, 128:]
        pdc[...] = tot.astype(BF)
        for d in pd_out:
            d.start()


    def noise_in():
        tot = pdc[...].astype(F32)
        for r in range(1, 8):
            recv(pdb.at[r], pd_r.at[r])
            tot += pdb[r].astype(F32)
        pdt[...] = (tot / math.sqrt(FFW)).astype(BF).astype(F32) * 0.5
        a2t[...] = dk[2, :, pl.ds(pl.multiple_of(640 * z + 256 * yl, 128), 384)].T

    def noise(j):
        live = rowm == 2 * j + lanem
        pm = jnp.where(live, jnp.concatenate([pdt[...]] * 2, axis=1), 0.0).astype(BF)
        for h in range(2):
            nbuf[h, j] = nn(a2t[pl.ds(pl.multiple_of(64 * yl + 160 * h, 16), 160)], pm)

    down_sums()

    def middle(n, _):
        s, j = n // 8 + 1, rem(n, 8)
        i = chunk(j)
        pp = part(rem(z - sgn * (1 + s) + 16, 8), i)
        recv(rcv.at[s - 1, i], rs_r.at[s - 1, i])
        rcv[s - 1, i] = (pp + rcv[s - 1, i].astype(F32)).astype(BF)
        rsend(s, i, rcv.at[s - 1, i]).start()
        rsend(s - 1, i, rcv.at[s, i]).wait_send()

        @pl.when((s == 4) & (j == 3))
        def _():
            noise_in()

        @pl.when((s == 5) & (j >= 2) & (j < 6))
        def _():
            noise(j - 2)

        @pl.when(n == CF)
        def _():
            collect_f()

        m = n - CD

        @pl.when(m == 0)
        def _():
            collect_d()

        @pl.when((m >= 1) & (m < 4))
        def _():
            weigh(m - 1)

        @pl.when(m == 3)
        def _():
            recv(fall.at[:, 1 - c], ff_r)

        @pl.when((m >= 4) & (m < 4 + 6 * DS) & (rem(m, DS) == 0))
        def _():
            q = (m - 4) // DS
            delta(q // 2, rem(q, 2))

        return 0

    lax.fori_loop(0, 48, middle, 0)

    def last(j):
        i = chunk(j)
        pp = part(z, i)
        recv(rcv.at[6, i], rs_r.at[6, i])
        return pp + rcv[6, i].astype(F32)

    def last_far(j, _):
        fsnd[j] = last(j).astype(BF)
        rc(fsnd.at[j], fin.at[j], fs_s.at[j], fs_r.at[j], ypart).start()

        if 48 - CD - 4 < 6 * DS:
            @pl.when(j < 2)
            def _():
                delta(2, j)

        return 0

    lax.fori_loop(0, 4, last_far, 0)

    def put(j, h, w):
        for m in range(2):
            out_ref[2 * j + m, pl.ds(pl.multiple_of(160 * h, 16), 160)] = w[:, 128 * m : 128 * (m + 1)].astype(BF)

    def last_near(j, _):
        put(j, yh, last(j + 4) + nbuf[yh, j])
        return 0

    lax.fori_loop(0, 4, last_near, 0)

    def finish(j, _):
        rc(fsnd.at[j], fin.at[j], fs_s.at[j], fs_r.at[j], ypart).wait()
        put(j, 1 - yh, fin[j].astype(F32) + nbuf[1 - yh, j])
        return 0

    lax.fori_loop(0, 4, finish, 0)

    for w in pending:
        w()

    def drain(i, _):
        rsend(6, i, snd.at[i]).wait_send()
        return 0

    lax.fori_loop(0, 8, drain, 0)


def call_step(*arrays):
    arrays = [pltpu.with_memory_space_constraint(v, pltpu.HBM) for v in arrays]
    v = pl.BlockSpec(memory_space=pltpu.VMEM)
    a = pl.BlockSpec(memory_space=pltpu.HBM)
    dma = pltpu.SemaphoreType.DMA
    vm = pltpu.VMEM
    return pl.pallas_call(
        step_kernel,
        out_shape=[
            jax.ShapeDtypeStruct((8, 320, 128), BF),
            jax.ShapeDtypeStruct((3, 320, FB), BF),
        ],
        in_specs=[a] * 8,
        out_specs=[v, v],
        scratch_shapes=[
            pltpu.SMEM((8,), jnp.int32), pltpu.SMEM((8,), F32),
            vm((320, 128), BF), vm((2, 320, FB), BF), vm((2, 160, FB), BF), vm((16, 3, 4, D), BF), vm((16, 3, 4, FB), BF),
            vm((3, 32, D), BF), vm((3, 2, 8, 32, FB), BF), vm((2, 3, 32, FB), BF),
            vm((2, 8, 160, FB), BF), vm((8, 2, FB, 256), BF), vm((8, 160, 256), BF),
            vm((7, 8, 160, 256), BF), vm((4, 160, 256), BF), vm((4, 160, 256), BF),
            vm((896, 128), BF), vm((896, 128), BF), vm((896, 128), F32), vm((2, 4, 112, 128), BF),
            vm((4, 2, 112, 128), BF), vm((112, 128), BF), vm((112, 128), BF), vm((2, 2, 896, 192), BF), vm((2, 192, 256), BF),
            vm((128, 384), BF), vm((2, 8, 16, 384), BF), vm((16, 128), BF), vm((2, 128, 128), BF),
            vm((2, 2, 32, 128), F32),
            vm((32, 128), BF), vm((8, 32, 128), BF), vm((32, 128), F32), vm((3, 2, 8, 32, 384), BF),
            vm((2, 8, 8, 128), F32), vm((2, 8, 32, 128), F32), vm((3, 384, 512), BF), vm((384, 32), BF), vm((2, 4, 160, 256), F32),
            dma((8,)), dma(()), dma(()), dma((8,)), dma((8,)), dma((4,)), dma((4,)), dma((4, 4)), dma((4, 4)), dma(()), dma(()),
            dma((8,)), dma((8,)), dma((16,)), dma((16,)),
            dma((3,)), dma((3,)), dma((2,)), dma((2,)), dma((2, 2)), dma((2, 2)), dma((2,)), dma((2, 2, 2)), dma((4, 2, 2)), dma((4, 2, 2)),
            dma((4, 2)), dma((4, 2)), dma((7, 8)), dma((7, 8)), dma((4,)), dma((4,)),
            dma((8,)), dma((8,)), dma((8,)), dma((8,)), dma(()), dma(()), dma((16,)), dma((16,)),
            dma((16,)), dma((16,)),
        ],
        compiler_params=pltpu.CompilerParams(
            collective_id=0, has_side_effects=True, vmem_limit_bytes=44 << 20
        ),
        name="es_step",
    )(*arrays)


EMIT_LIM = 4 << 20


def emit_kernel(out, deltas, o_hbm, g_hbm, u_hbm, d_hbm, sems):
    pairs = [(deltas.at[0], g_hbm), (deltas.at[1], u_hbm), (deltas.at[2], d_hbm), (out, o_hbm)]
    copies = [pltpu.make_async_copy(a, b, sems.at[i]) for i, (a, b) in enumerate(pairs)]
    for d in copies:
        d.start()
    for d in copies:
        d.wait()


def emit(out, deltas):
    v = pl.BlockSpec(memory_space=pltpu.VMEM)
    a = pl.BlockSpec(memory_space=pltpu.HBM)
    one = jax.ShapeDtypeStruct((320, FB), BF)
    return pl.pallas_call(
        emit_kernel,
        out_shape=[jax.ShapeDtypeStruct((8, 320, 128), BF), one, one, one],
        in_specs=[v, v],
        out_specs=[a, a, a, a],
        scratch_shapes=[pltpu.SemaphoreType.DMA((4,))],
        compiler_params=pltpu.CompilerParams(vmem_limit_bytes=EMIT_LIM),
        name="emit",
    )(out, deltas)


def shards(prompt_acts, gate_weight, up_weight, down_weight, d_table, f_table, seeds, fitness):
    out, deltas = call_step(
        prompt_acts.T, gate_weight, up_weight, down_weight.T.reshape(2, 160, FB), d_table, f_table,
        seeds, fitness,
    )
    out, dg, du, dd = emit(out, deltas)
    return out.transpose(0, 2, 1), dg, du, dd.T


def solution(mesh):
    split = Mesh(mesh.devices.reshape(4, 2, 2, 8, 2), AX)
    placed = (
        P(None, MEMBER), P(MEMBER, TENSOR), P(MEMBER, TENSOR), P(TENSOR, MEMBER),
        P(MEMBER, None, None, None), P(MEMBER, None, None, TENSOR), P(MEMBER), P(MEMBER),
    )
    return jax.shard_map(
        shards, mesh=split, in_specs=placed,
        out_specs=(P(MEMBER, None, TENSOR), P(MEMBER, TENSOR), P(MEMBER, TENSOR), P(TENSOR, MEMBER)),
        check_vma=False,
    )
```

```python
import functools
import math

import jax
import jax.numpy as jnp
from jax import lax
from jax.experimental import pallas as pl
from jax.experimental.pallas import tpu as pltpu
from jax.sharding import Mesh
from jax.sharding import PartitionSpec as P

D = 5120
FFW = 13824
FB = 864
AX = ("x", "yh", "c", "z", "yl")
MEMBER = ("x", "yh", "c")
TENSOR = ("z", "yl")
MESH = pl.DeviceIdType.MESH
BF = jnp.bfloat16
F32 = jnp.float32
HR = 864
HU = 1
LEAD = 1
TB = 0
TB2 = 2
TF = 7
FX = 17
PN = 6
NI = 20
CF = 35
DX = 33
CD = 38
DS = 1
ORDER = (
    "y_first",
    "y_first_b",
    "y_second",
    "base_half",
    "y_second_b",
    "base_scatter",
    "prompt_out",
    "base_mid",
    "x_first",
    "base_sum",
    "x_first_b",
    "local_rows",
    "factors_far",
    "factors_diag",
    "prompt_on",
    "take_first",
    "base_on",
    "project",
    "factors_near",
    "take_first_b",
    "x_second",
    "factors_near_in",
    "x_second_b",
    "factors_far_in",
    "base_end",
    "take_first_far",
    "project_in",
    "base_other",
    "down_out",
    "hidden_ahead",
    "first_in",
)


def rem(a, n):
    return lax.rem(a, n)


def at(x, yh, c, z, yl):
    return {"x": x, "yh": yh, "c": c, "z": z, "yl": yl}


def tn(a, b):
    return lax.dot_general(a, b, (((0,), (0,)), ((), ())), preferred_element_type=F32)


def nt(a, b):
    return lax.dot_general(a, b, (((1,), (1,)), ((), ())), preferred_element_type=F32)


def nn(a, b):
    return jnp.dot(a, b, preferred_element_type=F32)


def step_kernel(
    pt_hbm, gw_hbm, uw_hbm, dt_hbm, dtab_hbm, ftab_hbm, seeds_hbm, fit_hbm,
    out_ref, del_ref,
    seeds, fit, pt_v, w_v, dt_v, dtab, ftab, dk, fall, foth, dbuf, hbuf, snd, rcv, fin, fsnd,
    bsend, brecv, bown, ps, rsb, rsend2, rrecv2, lhs, rhs, psh, prb, pjs, pjb, ptt,
    pdc, pdb, pdt, dall, fitall, score, wt, a2t, nbuf, wbuf,
    in_s, bx_s, bx_r, r1_s, r1_r, ag_s, ag_r, ah_s, ah_r, bf_s, bf_r, pr_s, pr_r, pj_s, pj_r,
    ft_s, ft_r, ft2_s, ft2_r, ys, yr, yloc, xo_s, xf_s, x_r, ds_s, ds_r, rs_s, rs_r, fs_s, fs_r,
    pd_s, pd_r, f_s, f_r, ff_s, ff_r, d_s, d_r, q_s, q_r,
):
    x, yh, c, z, yl = [lax.axis_index(a) for a in AX]
    y = 2 * yh + yl
    p = 2 * x + yh
    me = at(x, yh, c, z, yl)
    partner = at(x, yh, 1 - c, z, yl)
    ypart = at(x, 1 - yh, c, z, yl)
    pending = []

    def rc(src, dst, ss, rs, dev):
        return pltpu.make_async_remote_copy(
            src_ref=src, dst_ref=dst, send_sem=ss, recv_sem=rs, device_id=dev, device_id_type=MESH
        )

    def send(src, dst, ss, rs, dev):
        d = rc(src, dst, ss, rs, dev)
        d.start()
        pending.append(d.wait_send)

    def recv(dst, rs):
        rc(dst, dst, rs, rs, partner).wait_recv()

    loads = [
        (gw_hbm, w_v.at[0]), (uw_hbm, w_v.at[1]), (pt_hbm, pt_v), (ftab_hbm, ftab), (dtab_hbm, dtab),
        (dt_hbm, dt_v), (seeds_hbm, seeds), (fit_hbm, fit),
    ]
    loads = [pltpu.make_async_copy(a, b, in_s.at[i]) for i, (a, b) in enumerate(loads)]
    for i in (5, 2, 0, 1, 6, 7, 3, 4):
        loads[i].start()

    def plane(rel):
        ny = rem(y + rel % 4, 4)
        return at(rem(x + rel // 4, 4), ny // 2, c, z, rem(ny, 2))

    def mate(rel):
        q = rem(p + rel // 2, 8)
        return at(q // 2, rem(q, 2), rem(c + rel % 2, 2), z, yl)

    def column(rel):
        return at(x, rem(yh + rel // 8, 2), c, rem(z + rel % 8, 8), yl)

    ypeers = [at(x, h, yl, z, c) for h in range(2)]
    me_y = [(h == yh) & (c == yl) for h in range(2)]
    barrier = pltpu.get_barrier_semaphore()

    def greet(dev):
        pl.semaphore_signal(barrier, inc=1, device_id=dev, device_id_type=MESH)

    peers = [plane(1), plane(3)] + [mate(r) for r in range(1, 16)]
    peers += [column(r) for r in range(1, 16) if r != 8]
    for o in peers:
        greet(o)
    @pl.when(c != yl)
    def _():
        for h in range(2):
            greet(ypeers[h])

    def partial_base(k):
        return tn(w_v[k], pt_v[...])

    for i in (0, 1, 2, 5):
        loads[i].wait()
    bsend[pl.ds(0, FB)] = partial_base(1 - c).astype(BF)
    bsend[pl.ds(FB, 32)] = jnp.zeros((32, 128), BF)
    n_peers = len(peers)
    @pl.when(c == yl)
    def _():
        pl.semaphore_wait(barrier, n_peers)

    @pl.when(c != yl)
    def _():
        pl.semaphore_wait(barrier, n_peers + 2)

    e, kz = rem(z, 2), z // 2

    def low(x0):
        m = rem(x0 - kz + 4, 4)
        return jnp.where(e == 0, jnp.where(m == 1, 0, 1), jnp.where(m == 3, 1, 0))

    def zblk(r, ab):
        x0 = rem(x - r + 4, 4)
        return 2 * x0 + (low(x0) if ab == 0 else 1 - low(x0))

    own_a = low(x)

    def half(b, part):
        return b.at[pl.ds(80 * part, 80)]

    def ycopy(h, part):
        dst = half(dbuf.at[yl, 2 * x + yh], part)
        return rc(half(dt_v.at[h], part), dst, ys.at[h, part], yr.at[yh, part], ypeers[h])

    def ylocal(h, part):
        return pltpu.make_async_copy(half(dt_hbm.at[h], part), half(dbuf.at[yl, 2 * x + yh], part), yloc.at[part])

    def ysend(ab, part):
        mine = yh == (own_a if ab == 0 else 1 - own_a)
        for h in range(2):
            @pl.when(mine & jnp.logical_not(me_y[h]))
            def _():
                ycopy(h, part).start()
            @pl.when(mine & me_y[h])
            def _():
                ylocal(h, part).start()

    def wait_y(ab, part):
        w = own_a if ab == 0 else 1 - own_a
        here = (w == yh) & (c == yl)

        @pl.when(jnp.logical_not(here))
        def _():
            recv(half(dbuf.at[c, 2 * x + w], part), yr.at[w, part])

        @pl.when(here)
        def _():
            ylocal(0, part).wait()

    def y_drain():
        for h in range(2):
            @pl.when(jnp.logical_not(me_y[h]))
            def _():
                for part in range(2):
                    ycopy(h, part).wait_send()

    pending.append(y_drain)
    xnb = [at(rem(x + 1, 4), yh, c, z, yl), at(rem(x + 3, 4), yh, c, z, yl)]

    def dsend(r, ab, part):
        b = half(dbuf.at[c, zblk(r, ab)], part)
        d = rc(b, b, ds_s.at[r, ab, part], ds_r.at[r, ab, part], partner)
        pending.append(d.wait_send)
        return d

    def own_x(ab, part):
        b = dbuf.at[c, zblk(0, ab)]
        dsend(0, ab, part).start()
        b = half(b, part)
        send(b, b, xo_s.at[0, ab, part], x_r.at[1, ab, part], xnb[0])
        send(b, b, xo_s.at[1, ab, part], x_r.at[3, ab, part], xnb[1])

    def taker(r, ab):
        b = dbuf.at[c, zblk(r, ab)]
        d2 = [dsend(r, ab, part) for part in range(2)]
        fwd = c == (0 if r == 1 else 1)
        hops = []
        for part in range(2 if r != 2 else 0):
            h = half(b, part)
            d = rc(h, h, xf_s.at[r, ab, part], x_r.at[2, ab, part], xnb[0 if r == 1 else 1])
            hops.append(d)
            pending.append(functools.partial(pl.when(fwd), d.wait_send))

        def run(part):
            recv(half(b, part), x_r.at[r, ab, part])
            if r != 2:
                pl.when(fwd)(hops[part].start)
            d2[part].start()

        return run

    take = {(r, ab): taker(r, ab) for r in (1, 3, 2) for ab in range(2)}

    def take_d(r, ab):
        for part in range(2):
            recv(half(dbuf.at[1 - c, zblk(r, ab)], part), ds_r.at[r, ab, part])

    toks = pl.ds(pl.multiple_of(16 * z, 16), 16)
    own_row = 4 * yh + x
    def bpiece(t, k, first, rows):
        return lhs.at[t, k, pl.ds(pl.multiple_of(112 * first, 16), rows), pl.ds(0, 128)]

    along_x = [at(rem(x + r, 4), yh, c, z, yl) for r in range(4)]
    along_y = [at(x, rem(y + r, 4) // 2, c, z, rem(y + r, 2)) for r in range(4)]
    stage1, stage2, got1, got2 = [], [], [], []
    for r in range(1, 4):
        b = bpiece(yl, c, own_row, 112)
        stage1.append((rc(b, b, ag_s.at[r], ag_r.at[r], along_x[r]), rc(b, b, ag_s.at[r], ag_r.at[r], along_y[r])))
        xx, yy = rem(x - r + 4, 4), rem(y - r + 4, 4)
        got1.append((bpiece(yl, c, 4 * yh + xx, 112), bpiece(rem(yy, 2), c, 4 * (yy // 2) + x, 112)))
        b = bpiece(yl, c, 4 * yh, 448)
        far = []
        for n in range(4):
            f = bpiece(n // 2, c, 4 * (n % 2) + x, 112)
            far.append(rc(f, f, ah_s.at[r, n], ah_r.at[r, n], along_x[r]))
        stage2.append(([rc(b, b, ah_s.at[r, 0], ah_r.at[r, 0], along_y[r])], far))
        got2.append((
            [bpiece(rem(yy, 2), c, 4 * (yy // 2), 448)],
            [bpiece(n // 2, c, 4 * (n % 2) + xx, 112) for n in range(4)],
        ))

    def by_core(f):
        for core in range(2):
            @pl.when(c == core)
            def _():
                f(core)

    def ag_one(core):
        for d in stage1:
            d[core].start()

    def ag_two(core):
        for g, r in zip(got1, range(1, 4)):
            recv(g[core], ag_r.at[r])
        for ds in stage2:
            for d in ds[core]:
                d.start()

    def ag_end(core):
        for g, r in zip(got2, range(1, 4)):
            for n, b in enumerate(g[core]):
                recv(b, ah_r.at[r, n])

    def ag_drain(core):
        for d in stage1:
            d[core].wait_send()
        for ds in stage2:
            for d in ds[core]:
                d.wait_send()

    pending.append(lambda: by_core(ag_drain))
    fteam = [(1, 0), (1, 1), (0, 1)]

    def fdev(i):
        dh, dl = fteam[i]
        return at(x, rem(yh + dh, 2), c, z, rem(yl + dl, 2))

    def fdst(i, ks):
        return fall.at[ks, c, p] if fteam[i][1] == 0 else foth.at[yh, ks]

    def frcv(i, ks):
        dh, dl = fteam[i]
        return fall.at[ks, c, p + 1 - 2 * yh] if dl == 0 else foth.at[rem(yh + dh, 2), ks]

    gu, down = pl.ds(0, 2), pl.ds(2, 1)
    def factors_in(own, where):
        for i in where:
            recv(frcv(i, gu), ft_r.at[i])
        g = yh if own else 1 - yh
        for k in range(2):
            lanes = pl.ds(160 if own else 128, 32)
            lhs[yl, k, pl.ds(0, FB), lanes] = fall[k, c, 2 * x + g].T
            lhs[1 - yl, k, pl.ds(0, FB), lanes] = foth[g, k].T

    rowm = lax.broadcasted_iota(jnp.int32, (32, 256), 0) // 4
    lanem = lax.broadcasted_iota(jnp.int32, (32, 256), 1) // 128

    def hidden_rows():
        for i in range(8):
            g, cc = i // 4, i % 4
            for k in range(2):
                for gg in range(2):
                    of = yh if gg == 1 else 1 - yh
                    v = jnp.concatenate([ptt[of, k]] * 2, axis=1)
                    live = (rowm == 2 * cc + lanem) & (g == of)
                    rhs[i, k, pl.ds(128 + 32 * gg, 32)] = jnp.where(live, v, 0.0).astype(BF)

    def hidden(i):
        def rows(rb, _):
            r = pl.ds(pl.multiple_of(rb * HR, 16), HR)
            for t in range(2):
                ga = nn(lhs[t, 0, r], rhs[i, 0])
                up = nn(lhs[t, 1, r], rhs[i, 1])
                hbuf[i, t, r] = ((ga + ga * jnp.tanh(ga)) * up).astype(BF)
            return 0

        lax.fori_loop(0, FB // HR, rows, 0, unroll=HU)

    def chunk(j):
        return rem(j + 4 * (1 - yh), 8)

    sgn = 1 - 2 * c
    zn = rem(z + sgn + 8, 8)
    znd = at(x, yh, c, zn, yl)

    def part(d, i):
        return nn(dbuf[0, d], hbuf[i, 0]) + nn(dbuf[1, d], hbuf[i, 1])

    d0 = rem(z - sgn + 8, 8)

    def rsend(s, i, src):
        return rc(src, rcv.at[s, i], rs_s.at[s, i], rs_r.at[s, i], znd)


    def local_rows():
        for i in (6, 7, 3):
            loads[i].wait()
        for k in range(3):
            for m in range(8):
                fall[k, c, p, pl.ds(4 * m, 4)] = ftab[seeds[m], k]
        loads[4].wait()
        for k in range(3):
            for m in range(8):
                dk[k, pl.ds(4 * m, 4)] = dtab[seeds[m], k]

        eye = lax.broadcasted_iota(jnp.int32, (128, 256), 0) == rem(lax.broadcasted_iota(jnp.int32, (128, 256), 1), 128)
        for k in range(2):
            for i in range(8):
                rhs[i, k, 0:128] = jnp.where(eye, 1.0, 0.0).astype(BF)
            for t in range(2):
                lhs[t, k, :, pl.ds(128, 64)] = jnp.zeros((896, 64), BF)

    def base_half():
        send(bsend, brecv, bx_s, bx_r, partner)

    def base_scatter():
        bown[pl.ds(0, FB)] = partial_base(c)
        bown[pl.ds(FB, 32)] = jnp.zeros((32, 128), F32)
        recv(brecv, bx_r)
        for q in range(8):
            rows = pl.ds(112 * q, 112)
            ps[q // 4, q % 4] = (bown[rows] + brecv[rows].astype(F32)).astype(BF)
        for r in range(1, 4):
            xx = rem(x + r, 4)
            send(ps.at[:, xx], rsb.at[r], r1_s.at[r], r1_r.at[r], at(xx, yh, c, z, yl))

    def own_sum(h):
        mid = pl.ds(pl.multiple_of(112 * (4 * h + x), 16), 112)
        s = bown[mid] + brecv[mid].astype(F32)
        for r in range(1, 4):
            s += rsb[r, h].astype(F32)
        return s

    def base_mid():
        for r in range(1, 4):
            recv(rsb.at[r], r1_r.at[r])
        rsend2[...] = own_sum(1 - yh).astype(BF)
        send(rsend2, rrecv2, r1_s.at[0], r1_r.at[0], ypart)

    def base_sum():
        recv(rrecv2, r1_r.at[0])
        s = own_sum(yh) + rrecv2[...].astype(F32)
        s = jnp.where(c == 0, s * 0.5, s)
        bpiece(yl, c, own_row, 112)[...] = s.astype(BF)
        by_core(ag_one)

    def base_on():
        by_core(ag_two)

    def base_end():
        by_core(ag_end)
        send(lhs.at[:, c, :, pl.ds(0, 128)], lhs.at[:, c, :, pl.ds(0, 128)], bf_s, bf_r, partner)

    def base_other():
        recv(lhs.at[:, 1 - c, :, pl.ds(0, 128)], bf_r)

    def prompt_out():
        ptr = pt_v[...].astype(F32).T.astype(BF)
        psh[...] = jnp.zeros_like(psh)

        @pl.when(c == 0)
        def _():
            psh[:, 0:320] = ptr

        @pl.when(c == 1)
        def _():
            psh[:, 64:384] = ptr

        prb[c, p] = psh[toks]
        for r in range(1, 8):
            send(prb.at[c, p], prb.at[c, p], pr_s.at[r], pr_r.at[r], mate(2 * r))

    def prompt_on():
        for r in range(1, 8):
            recv(prb.at[c, rem(p - r + 8, 8)], pr_r.at[r])
        send(prb.at[c], prb.at[c], pr_s.at[0], pr_r.at[0], partner)

    def project():
        recv(prb.at[1 - c], pr_r.at[0])

        def proj_of(n, acc):
            cc, q = n // 8, rem(n, 8)
            lanes = pl.ds(pl.multiple_of(640 * q + 256 * cc, 128), 384)
            return acc + nt(prb[cc, q], dk[0:2, :, lanes].reshape(64, 384))

        acc = lax.fori_loop(0, 16, proj_of, jnp.zeros((16, 64), F32), unroll=4)
        acc = (acc / math.sqrt(D)).astype(BF).astype(F32)
        kk = lax.broadcasted_iota(jnp.int32, (16, 64), 1) // 32
        acc = jnp.where(kk == 0, acc * 0.25, acc * 0.5)
        pjs[...] = jnp.zeros_like(pjs)
        pjs[:, 0:64] = acc.astype(BF)
        pjb[yh, toks] = pjs[...]
        for r in range(1, 16):
            send(pjs, pjb.at[yh, toks], pj_s.at[r], pj_r.at[r], column(r))


    def project_in():
        for r in range(1, 16):
            hz, zz = rem(yh + r // 8, 2), rem(z - r % 8 + 8, 8)
            recv(pjb.at[hz, pl.ds(pl.multiple_of(16 * zz, 16), 16)], pj_r.at[r])
        for g in range(2):
            ptt[g] = pjb[g].astype(F32).T[0:64].reshape(2, 32, 128)
        hidden_rows()

    def y_first():
        ysend(0, 0)

    def y_first_b():
        ysend(0, 1)

    def y_second():
        ysend(1, 0)

    def y_second_b():
        ysend(1, 1)

    def x_first():
        wait_y(0, 0)
        own_x(0, 0)

    def x_first_b():
        wait_y(0, 1)
        own_x(0, 1)

    def x_second():
        wait_y(1, 0)
        own_x(1, 0)

    def x_second_b():
        wait_y(1, 1)
        own_x(1, 1)

    def down_out():
        send(fall.at[down, c, p], fdst(2, down), ft2_s.at[0], ft2_r.at[0], fdev(2))
        send(fall.at[down, c, p], fdst(0, down), ft2_s.at[1], ft2_r.at[1], fdev(0))

    def take_first():
        take[1, 0](0)
        take[3, 0](0)

    def take_first_b():
        take[1, 0](1)
        take[3, 0](1)

    def take_second():
        take[1, 1](0)
        take[3, 1](0)

    def take_second_b():
        take[1, 1](1)
        take[3, 1](1)

    def take_first_far():
        for part in range(2):
            take[2, 0](part)

    def first_in():
        for r in range(4):
            take_d(r, 0)

    def take_second_far():
        for part in range(2):
            take[2, 1](part)

    def second_in():
        for r in range(4):
            take_d(r, 1)

    def factors_far():
        send(fall.at[gu, c, p], fdst(0, gu), ft_s.at[0], ft_r.at[0], fdev(0))

    def factors_diag():
        send(fall.at[gu, c, p], fdst(1, gu), ft_s.at[1], ft_r.at[1], fdev(1))

    def factors_near():
        send(fall.at[gu, c, p], fdst(2, gu), ft_s.at[2], ft_r.at[2], fdev(2))

    def factors_far_in():
        factors_in(False, (0, 1))

    def factors_near_in():
        factors_in(True, (2,))

    def hidden_ahead():
        def ahead(j, _):
            hidden(chunk(j))
            return 0

        lax.fori_loop(0, LEAD, ahead, 0)

    steps = dict(
        local_rows=local_rows, down_out=down_out,
        base_half=base_half, base_scatter=base_scatter, base_mid=base_mid, base_sum=base_sum, base_on=base_on, base_end=base_end,
        base_other=base_other, prompt_out=prompt_out, prompt_on=prompt_on, project=project,
        project_in=project_in, y_first=y_first, y_second=y_second, y_first_b=y_first_b, y_second_b=y_second_b, x_first=x_first, x_second=x_second, x_first_b=x_first_b, x_second_b=x_second_b,
        take_first=take_first, take_first_b=take_first_b, take_second_b=take_second_b, take_second=take_second, take_first_far=take_first_far, first_in=first_in,
        factors_far=factors_far, factors_diag=factors_diag, factors_near=factors_near, factors_far_in=factors_far_in,
        factors_near_in=factors_near_in, hidden_ahead=hidden_ahead,
    )
    for name in ORDER:
        steps[name]()

    def step_zero(j):
        i = chunk(j)
        snd[i] = part(d0, i).astype(BF)
        rsend(0, i, snd.at[i]).start()

    def first(j, _):
        i = chunk(j)
        p0 = part(d0, i).astype(BF)
        hidden(chunk(j + 1))
        snd[i] = p0
        rsend(0, i, snd.at[i]).start()
        pl.when(j == TB)(take_second)
        pl.when(j == TB2)(take_second_b)
        return 0

    lax.fori_loop(0, 7, first, 0)
    step_zero(7)
    take_second_far()

    recv(frcv(0, down), ft2_r.at[1])

    def fpiece(i, other):
        return fall.at[:, c, 2 * rem(x - i + 4, 4) + (1 - yh if other else yh)]

    f_out, f_on = [], []
    for i in range(1, 4):
        f_out.append([rc(fpiece(0, h), fpiece(0, h), f_s.at[4 * h + i], f_r.at[4 * h + i], along_x[i]) for h in range(2)])
        f_on.append(rc(fpiece(i, 0), fpiece(i, 0), f_s.at[4 + i], f_r.at[4 + i], ypart))

    def factors_out(core):
        for d in f_out:
            for h in range(1 + core):
                d[h].start()

    def factors_drain(core):
        for d in f_out:
            for h in range(1 + core):
                d[h].wait_send()
        if core == 0:
            for d in f_on:
                d.wait_send()

    by_core(factors_out)
    pending.append(lambda: by_core(factors_drain))
    for m in range(8):
        fitall[c, p, pl.ds(m, 1)] = jnp.full((1, 128), fit[m], F32)

    def dlanes(q):
        return pl.ds(pl.multiple_of(640 * q, 128), 640)

    dall[:, c, p] = dk[:, :, dlanes(p)]
    for r in range(1, 8):
        q = rem(p + r, 8)
        send(dk.at[:, :, dlanes(q)], dall.at[:, c, p], d_s.at[r], d_r.at[r], mate(2 * r))
        send(fitall.at[c, p], fitall.at[c, p], q_s.at[r], q_r.at[r], mate(2 * r))

    second_in()

    fwd_f = rc(fall.at[:, c], fall.at[:, c], ff_s, ff_r, partner)
    pending.append(fwd_f.wait_send)

    def factors_on():
        @pl.when(c == 0)
        def _():
            for i in range(1, 4):
                recv(fpiece(i, 0), f_r.at[i])
            for d in f_on:
                d.start()

    def collect_f():
        @pl.when(c == 1)
        def _():
            for i in range(1, 4):
                recv(fpiece(i, 0), f_r.at[i])

        for i in range(1, 4):
            recv(fpiece(i, 1), f_r.at[4 + i])
        fwd_f.start()

    d_on = rc(dall.at[:, c], dall.at[:, c], d_s.at[0], d_r.at[0], partner)
    q_on = rc(fitall.at[c], fitall.at[c], q_s.at[0], q_r.at[0], partner)
    pending.extend([d_on.wait_send, q_on.wait_send])

    def factors_d_on():
        for r in range(1, 8):
            q = rem(p - r + 8, 8)
            recv(dall.at[:, c, q], d_r.at[r])
            recv(fitall.at[c, q], q_r.at[r])
        d_on.start()
        q_on.start()

    def collect_d():
        recv(dall.at[:, 1 - c], d_r.at[0])
        recv(fitall.at[1 - c], q_r.at[0])
        fv = fitall[...].reshape(128, 128)
        mean = jnp.sum(fv, axis=0, keepdims=True) / 128
        spread = jnp.sum((fv - mean) ** 2, axis=0, keepdims=True) / 128
        sc = (fv - mean) / jnp.sqrt(spread + 1.0)
        for i in range(16):
            v = jnp.broadcast_to(sc[8 * i : 8 * i + 8].reshape(8, 1, 128), (8, 4, 128))
            score[i // 8, i % 8] = v.reshape(32, 128)

    def weigh(k):
        def one(g, _):
            a, b = g // 8, rem(g, 8)
            sc = score[a, b]
            own = pl.ds(pl.multiple_of(256 * c, 128), 384)
            w = dall[k, a, b, :, own].astype(F32) * jnp.concatenate([sc] * 3, axis=1)
            wbuf[g] = w.astype(BF)
            return 0
        lax.fori_loop(0, 16, one, 0)
        wt[k] = wbuf[...].reshape(512, 384).T

    def delta(k, half):
        r = pl.ds(pl.multiple_of(64 * c + 160 * half, 16), 160)
        v = nn(wt[k, r], fall[k].reshape(512, FB)) * (1.0 / math.sqrt(512))
        del_ref[k, pl.ds(pl.multiple_of(160 * half, 16), 160)] = v.astype(BF)

    pd_out = [rc(pdc, pdb.at[r], pd_s.at[r], pd_r.at[r], column(r)) for r in range(1, 8)]
    pending.extend(d.wait_send for d in pd_out)

    def down_sums():
        recv(frcv(2, down), ft2_r.at[0])
        tot = jnp.zeros((32, 128), F32)
        for cc in range(4):
            i = 4 * yh + cc
            q = nn(fall[2, c, p], hbuf[i, yl]) + nn(foth[yh, 2], hbuf[i, 1 - yl])
            q = jnp.where(rowm == 2 * cc + lanem, q, 0.0)
            tot += q[:, :128] + q[:, 128:]
        pdc[...] = tot.astype(BF)
        for d in pd_out:
            d.start()


    def noise_in():
        tot = pdc[...].astype(F32)
        for r in range(1, 8):
            recv(pdb.at[r], pd_r.at[r])
            tot += pdb[r].astype(F32)
        pdt[...] = (tot / math.sqrt(FFW)).astype(BF).astype(F32) * 0.5
        a2t[...] = dk[2, :, pl.ds(pl.multiple_of(640 * z + 256 * yl, 128), 384)].T

    def noise(j):
        live = rowm == 2 * j + lanem
        pm = jnp.where(live, jnp.concatenate([pdt[...]] * 2, axis=1), 0.0).astype(BF)
        for h in range(2):
            nbuf[h, j] = nn(a2t[pl.ds(pl.multiple_of(64 * yl + 160 * h, 16), 160)], pm)

    def place(n):
        m = n - 12
        late = jnp.where(rem(m + 16, 8) >= 4, 1, 0)
        s = jnp.where(n < 8, 1, jnp.where(n < 12, 2, jnp.where(n < 44, 3 + m // 8 - late, 6)))
        j = jnp.where(n < 8, n, jnp.where(n < 12, n - 8, jnp.where(n < 44, rem(m + 16, 8), n - 40)))
        return s, j

    def middle(n, _):
        s, j = place(n)
        i = chunk(j)
        pp = part(rem(z - sgn * (1 + s) + 16, 8), i)
        recv(rcv.at[s - 1, i], rs_r.at[s - 1, i])
        rcv[s - 1, i] = (pp + rcv[s - 1, i].astype(F32)).astype(BF)
        rsend(s, i, rcv.at[s - 1, i]).start()
        rsend(s - 1, i, rcv.at[s, i]).wait_send()

        @pl.when(n == PN)
        def _():
            down_sums()

        @pl.when(n == NI)
        def _():
            noise_in()

        @pl.when((n > NI) & (n <= NI + 4))
        def _():
            noise(n - NI - 1)

        @pl.when(n == FX)
        def _():
            factors_on()

        @pl.when(n == CF)
        def _():
            collect_f()

        @pl.when(n == DX)
        def _():
            factors_d_on()

        m = n - CD

        @pl.when(m == 0)
        def _():
            collect_d()

        @pl.when((m >= 1) & (m < 4))
        def _():
            weigh(m - 1)

        @pl.when(m == 3)
        def _():
            recv(fall.at[:, 1 - c], ff_r)

        @pl.when((m >= 4) & (m < 4 + 6 * DS) & (rem(m, DS) == 0))
        def _():
            q = (m - 4) // DS
            delta(q // 2, rem(q, 2))

        return 0

    lax.fori_loop(0, 44, middle, 0)

    def last(j):
        i = chunk(j)
        pp = part(z, i)
        recv(rcv.at[6, i], rs_r.at[6, i])
        return pp + rcv[6, i].astype(F32)

    def last_far(j, _):
        fsnd[j] = last(j).astype(BF)
        rc(fsnd.at[j], fin.at[j], fs_s.at[j], fs_r.at[j], ypart).start()

        return 0

    lax.fori_loop(0, 4, last_far, 0)
    lax.fori_loop(44, 48, middle, 0)

    def put(j, h, w):
        for m in range(2):
            out_ref[2 * j + m, pl.ds(pl.multiple_of(160 * h, 16), 160)] = w[:, 128 * m : 128 * (m + 1)].astype(BF)

    def last_near(j, _):
        put(j, yh, last(j + 4) + nbuf[yh, j])
        return 0

    lax.fori_loop(0, 4, last_near, 0)

    def finish(j, _):
        rc(fsnd.at[j], fin.at[j], fs_s.at[j], fs_r.at[j], ypart).wait()
        put(j, 1 - yh, fin[j].astype(F32) + nbuf[1 - yh, j])
        return 0

    lax.fori_loop(0, 4, finish, 0)

    for w in pending:
        w()

    def drain(i, _):
        rsend(6, i, snd.at[i]).wait_send()
        return 0

    lax.fori_loop(0, 8, drain, 0)


def call_step(*arrays):
    arrays = [pltpu.with_memory_space_constraint(v, pltpu.HBM) for v in arrays]
    v = pl.BlockSpec(memory_space=pltpu.VMEM)
    a = pl.BlockSpec(memory_space=pltpu.HBM)
    dma = pltpu.SemaphoreType.DMA
    vm = pltpu.VMEM
    return pl.pallas_call(
        step_kernel,
        out_shape=[
            jax.ShapeDtypeStruct((8, 320, 128), BF),
            jax.ShapeDtypeStruct((3, 320, FB), BF),
        ],
        in_specs=[a] * 8,
        out_specs=[v, v],
        scratch_shapes=[
            pltpu.SMEM((8,), jnp.int32), pltpu.SMEM((8,), F32),
            vm((320, 128), BF), vm((2, 320, FB), BF), vm((2, 160, FB), BF), vm((16, 3, 4, D), BF), vm((16, 3, 4, FB), BF),
            vm((3, 32, D), BF), vm((3, 2, 8, 32, FB), BF), vm((2, 3, 32, FB), BF),
            vm((2, 8, 160, FB), BF), vm((8, 2, FB, 256), BF), vm((8, 160, 256), BF),
            vm((7, 8, 160, 256), BF), vm((4, 160, 256), BF), vm((4, 160, 256), BF),
            vm((896, 128), BF), vm((896, 128), BF), vm((896, 128), F32), vm((2, 4, 112, 128), BF),
            vm((4, 2, 112, 128), BF), vm((112, 128), BF), vm((112, 128), BF), vm((2, 2, 896, 192), BF), vm((8, 2, 192, 256), BF),
            vm((128, 384), BF), vm((2, 8, 16, 384), BF), vm((16, 128), BF), vm((2, 128, 128), BF),
            vm((2, 2, 32, 128), F32),
            vm((32, 128), BF), vm((8, 32, 128), BF), vm((32, 128), F32), vm((3, 2, 8, 32, 640), BF),
            vm((2, 8, 8, 128), F32), vm((2, 8, 32, 128), F32), vm((3, 384, 512), BF), vm((384, 32), BF), vm((2, 4, 160, 256), F32), vm((16, 32, 384), BF),
            dma((8,)), dma(()), dma(()), dma((8,)), dma((8,)), dma((4,)), dma((4,)), dma((4, 4)), dma((4, 4)), dma(()), dma(()),
            dma((8,)), dma((8,)), dma((16,)), dma((16,)),
            dma((3,)), dma((3,)), dma((2,)), dma((2,)), dma((2, 2)), dma((2, 2)), dma((2,)), dma((2, 2, 2)), dma((4, 2, 2)), dma((4, 2, 2)),
            dma((4, 2, 2)), dma((4, 2, 2)), dma((7, 8)), dma((7, 8)), dma((4,)), dma((4,)),
            dma((8,)), dma((8,)), dma((8,)), dma((8,)), dma(()), dma(()), dma((16,)), dma((16,)),
            dma((16,)), dma((16,)),
        ],
        compiler_params=pltpu.CompilerParams(
            collective_id=0, has_side_effects=True, vmem_limit_bytes=44 << 20
        ),
        name="es_step",
    )(*arrays)


EMIT_LIM = 4 << 20


def emit_kernel(out, deltas, o_hbm, g_hbm, u_hbm, d_hbm, sems):
    pairs = [(deltas.at[0], g_hbm), (deltas.at[1], u_hbm), (deltas.at[2], d_hbm), (out, o_hbm)]
    copies = [pltpu.make_async_copy(a, b, sems.at[i]) for i, (a, b) in enumerate(pairs)]
    for d in copies:
        d.start()
    for d in copies:
        d.wait()


def emit(out, deltas):
    v = pl.BlockSpec(memory_space=pltpu.VMEM)
    a = pl.BlockSpec(memory_space=pltpu.HBM)
    one = jax.ShapeDtypeStruct((320, FB), BF)
    return pl.pallas_call(
        emit_kernel,
        out_shape=[jax.ShapeDtypeStruct((8, 320, 128), BF), one, one, one],
        in_specs=[v, v],
        out_specs=[a, a, a, a],
        scratch_shapes=[pltpu.SemaphoreType.DMA((4,))],
        compiler_params=pltpu.CompilerParams(vmem_limit_bytes=EMIT_LIM),
        name="emit",
    )(out, deltas)


def shards(prompt_acts, gate_weight, up_weight, down_weight, d_table, f_table, seeds, fitness):
    out, deltas = call_step(
        prompt_acts.T, gate_weight, up_weight, down_weight.T.reshape(2, 160, FB), d_table, f_table,
        seeds, fitness,
    )
    out, dg, du, dd = emit(out, deltas)
    return out.transpose(0, 2, 1), dg, du, dd.T


def solution(mesh):
    split = Mesh(mesh.devices.reshape(4, 2, 2, 8, 2), AX)
    placed = (
        P(None, MEMBER), P(MEMBER, TENSOR), P(MEMBER, TENSOR), P(TENSOR, MEMBER),
        P(MEMBER, None, None, None), P(MEMBER, None, None, TENSOR), P(MEMBER), P(MEMBER),
    )
    return jax.shard_map(
        shards, mesh=split, in_specs=placed,
        out_specs=(P(MEMBER, None, TENSOR), P(MEMBER, TENSOR), P(MEMBER, TENSOR), P(TENSOR, MEMBER)),
        check_vma=False,
    )
```

```python
import functools
import math

import jax
import jax.numpy as jnp
from jax import lax
from jax.experimental import pallas as pl
from jax.experimental.pallas import tpu as pltpu
from jax.sharding import Mesh
from jax.sharding import PartitionSpec as P

D = 5120
FFW = 13824
FB = 864
AX = ("x", "yh", "c", "z", "yl")
MEMBER = ("x", "yh", "c")
TENSOR = ("z", "yl")
MESH = pl.DeviceIdType.MESH
BF = jnp.bfloat16
F32 = jnp.float32
HR = 864
HU = 1
LEAD = 1
TB = 0
TB2 = 2
TF = 5
TF2 = 6
FX = 17
PN = 4
NI = 30
CF = 35
DX = 33
CD = 38
DS = 1
ORDER = (
    "y_first",
    "y_first_b",
    "y_second",
    "base_half",
    "y_second_b",
    "base_scatter",
    "prompt_out",
    "base_mid",
    "x_first",
    "base_sum",
    "x_first_b",
    "local_rows",
    "factors_far",
    "factors_diag",
    "prompt_on",
    "take_first",
    "base_on",
    "project",
    "factors_near",
    "take_first_b",
    "x_second",
    "factors_near_in",
    "x_second_b",
    "factors_far_in",
    "base_end",
    "take_first_far",
    "project_in",
    "base_other",
    "down_out",
    "hidden_ahead",
    "first_in",
)


def rem(a, n):
    return lax.rem(a, n)


def at(x, yh, c, z, yl):
    return {"x": x, "yh": yh, "c": c, "z": z, "yl": yl}


def tn(a, b):
    return lax.dot_general(a, b, (((0,), (0,)), ((), ())), preferred_element_type=F32)


def nt(a, b):
    return lax.dot_general(a, b, (((1,), (1,)), ((), ())), preferred_element_type=F32)


def nn(a, b):
    return jnp.dot(a, b, preferred_element_type=F32)


def step_kernel(
    pt_hbm, gw_hbm, uw_hbm, dt_hbm, dtab_hbm, ftab_hbm, seeds_hbm, fit_hbm,
    out_ref, del_ref,
    seeds, fit, pt_v, w_v, dt_v, dtab, ftab, dk, fall, foth, dbuf, hbuf, snd, rcv, fin, fsnd,
    bsend, brecv, bown, ps, rsb, rsend2, rrecv2, lhs, rhs, psh, prb, pjs, pjb, ptt,
    pdc, pdb, pdt, dall, fitall, score, wt, a2t, nbuf, wbuf,
    in_s, bx_s, bx_r, r1_s, r1_r, ag_s, ag_r, ah_s, ah_r, bf_s, bf_r, pr_s, pr_r, pj_s, pj_r,
    ft_s, ft_r, ft2_s, ft2_r, ys, yr, yloc, xo_s, xf_s, x_r, ds_s, ds_r, rs_s, rs_r, fs_s, fs_r,
    pd_s, pd_r, f_s, f_r, ff_s, ff_r, d_s, d_r, q_s, q_r,
):
    x, yh, c, z, yl = [lax.axis_index(a) for a in AX]
    y = 2 * yh + yl
    p = 2 * x + yh
    me = at(x, yh, c, z, yl)
    partner = at(x, yh, 1 - c, z, yl)
    ypart = at(x, 1 - yh, c, z, yl)
    pending = []

    def rc(src, dst, ss, rs, dev):
        return pltpu.make_async_remote_copy(
            src_ref=src, dst_ref=dst, send_sem=ss, recv_sem=rs, device_id=dev, device_id_type=MESH
        )

    def send(src, dst, ss, rs, dev):
        d = rc(src, dst, ss, rs, dev)
        d.start()
        pending.append(d.wait_send)

    def recv(dst, rs):
        rc(dst, dst, rs, rs, partner).wait_recv()

    loads = [
        (gw_hbm, w_v.at[0]), (uw_hbm, w_v.at[1]), (pt_hbm, pt_v), (ftab_hbm, ftab), (dtab_hbm, dtab),
        (dt_hbm, dt_v), (seeds_hbm, seeds), (fit_hbm, fit),
    ]
    loads = [pltpu.make_async_copy(a, b, in_s.at[i]) for i, (a, b) in enumerate(loads)]
    for i in (5, 2, 0, 1, 6, 7, 3, 4):
        loads[i].start()

    def plane(rel):
        ny = rem(y + rel % 4, 4)
        return at(rem(x + rel // 4, 4), ny // 2, c, z, rem(ny, 2))

    def mate(rel):
        q = rem(p + rel // 2, 8)
        return at(q // 2, rem(q, 2), rem(c + rel % 2, 2), z, yl)

    def column(rel):
        return at(x, rem(yh + rel // 8, 2), c, rem(z + rel % 8, 8), yl)

    ypeers = [at(x, h, yl, z, c) for h in range(2)]
    me_y = [(h == yh) & (c == yl) for h in range(2)]
    barrier = pltpu.get_barrier_semaphore()

    def greet(dev):
        pl.semaphore_signal(barrier, inc=1, device_id=dev, device_id_type=MESH)

    peers = [plane(1), plane(3)] + [mate(r) for r in range(1, 16)]
    peers += [column(r) for r in range(1, 16) if r != 8]
    for o in peers:
        greet(o)
    @pl.when(c != yl)
    def _():
        for h in range(2):
            greet(ypeers[h])

    def partial_base(k):
        return tn(w_v[k], pt_v[...])

    for i in (0, 1, 2, 5):
        loads[i].wait()
    bsend[pl.ds(0, FB)] = partial_base(1 - c).astype(BF)
    bsend[pl.ds(FB, 32)] = jnp.zeros((32, 128), BF)
    n_peers = len(peers)
    @pl.when(c == yl)
    def _():
        pl.semaphore_wait(barrier, n_peers)

    @pl.when(c != yl)
    def _():
        pl.semaphore_wait(barrier, n_peers + 2)

    e, kz = rem(z, 2), z // 2

    def low(x0):
        m = rem(x0 - kz + 4, 4)
        return jnp.where(e == 0, jnp.where(m == 1, 0, 1), jnp.where(m == 3, 1, 0))

    def zblk(r, ab):
        x0 = rem(x - r + 4, 4)
        return 2 * x0 + (low(x0) if ab == 0 else 1 - low(x0))

    own_a = low(x)

    def half(b, part):
        return b.at[pl.ds(80 * part, 80)]

    def ycopy(h, part):
        dst = half(dbuf.at[yl, 2 * x + yh], part)
        return rc(half(dt_v.at[h], part), dst, ys.at[h, part], yr.at[yh, part], ypeers[h])

    def ylocal(h, part):
        return pltpu.make_async_copy(half(dt_hbm.at[h], part), half(dbuf.at[yl, 2 * x + yh], part), yloc.at[part])

    def ysend(ab, part):
        mine = yh == (own_a if ab == 0 else 1 - own_a)
        for h in range(2):
            @pl.when(mine & jnp.logical_not(me_y[h]))
            def _():
                ycopy(h, part).start()
            @pl.when(mine & me_y[h])
            def _():
                ylocal(h, part).start()

    def wait_y(ab, part):
        w = own_a if ab == 0 else 1 - own_a
        here = (w == yh) & (c == yl)

        @pl.when(jnp.logical_not(here))
        def _():
            recv(half(dbuf.at[c, 2 * x + w], part), yr.at[w, part])

        @pl.when(here)
        def _():
            ylocal(0, part).wait()

    def y_drain():
        for h in range(2):
            @pl.when(jnp.logical_not(me_y[h]))
            def _():
                for part in range(2):
                    ycopy(h, part).wait_send()

    pending.append(y_drain)
    xnb = [at(rem(x + 1, 4), yh, c, z, yl), at(rem(x + 3, 4), yh, c, z, yl)]

    def dsend(r, ab, part):
        b = half(dbuf.at[c, zblk(r, ab)], part)
        d = rc(b, b, ds_s.at[r, ab, part], ds_r.at[r, ab, part], partner)
        pending.append(d.wait_send)
        return d

    def own_x(ab, part):
        b = dbuf.at[c, zblk(0, ab)]
        dsend(0, ab, part).start()
        b = half(b, part)
        send(b, b, xo_s.at[0, ab, part], x_r.at[1, ab, part], xnb[0])
        send(b, b, xo_s.at[1, ab, part], x_r.at[3, ab, part], xnb[1])

    def taker(r, ab):
        b = dbuf.at[c, zblk(r, ab)]
        d2 = [dsend(r, ab, part) for part in range(2)]
        fwd = c == (0 if r == 1 else 1)
        hops = []
        for part in range(2 if r != 2 else 0):
            h = half(b, part)
            d = rc(h, h, xf_s.at[r, ab, part], x_r.at[2, ab, part], xnb[0 if r == 1 else 1])
            hops.append(d)
            pending.append(functools.partial(pl.when(fwd), d.wait_send))

        def run(part):
            recv(half(b, part), x_r.at[r, ab, part])
            if r != 2:
                pl.when(fwd)(hops[part].start)
            d2[part].start()

        return run

    take = {(r, ab): taker(r, ab) for r in (1, 3, 2) for ab in range(2)}

    def take_d(r, ab):
        for part in range(2):
            recv(half(dbuf.at[1 - c, zblk(r, ab)], part), ds_r.at[r, ab, part])

    toks = pl.ds(pl.multiple_of(16 * z, 16), 16)
    own_row = 4 * yh + x
    def bpiece(t, k, first, rows):
        return lhs.at[t, k, pl.ds(pl.multiple_of(112 * first, 16), rows), pl.ds(0, 128)]

    along_x = [at(rem(x + r, 4), yh, c, z, yl) for r in range(4)]
    along_y = [at(x, rem(y + r, 4) // 2, c, z, rem(y + r, 2)) for r in range(4)]
    stage1, stage2, got1, got2 = [], [], [], []
    for r in range(1, 4):
        b = bpiece(yl, c, own_row, 112)
        stage1.append((rc(b, b, ag_s.at[r], ag_r.at[r], along_x[r]), rc(b, b, ag_s.at[r], ag_r.at[r], along_y[r])))
        xx, yy = rem(x - r + 4, 4), rem(y - r + 4, 4)
        got1.append((bpiece(yl, c, 4 * yh + xx, 112), bpiece(rem(yy, 2), c, 4 * (yy // 2) + x, 112)))
        b = bpiece(yl, c, 4 * yh, 448)
        far = []
        for n in range(4):
            f = bpiece(n // 2, c, 4 * (n % 2) + x, 112)
            far.append(rc(f, f, ah_s.at[r, n], ah_r.at[r, n], along_x[r]))
        stage2.append(([rc(b, b, ah_s.at[r, 0], ah_r.at[r, 0], along_y[r])], far))
        got2.append((
            [bpiece(rem(yy, 2), c, 4 * (yy // 2), 448)],
            [bpiece(n // 2, c, 4 * (n % 2) + xx, 112) for n in range(4)],
        ))

    def by_core(f):
        for core in range(2):
            @pl.when(c == core)
            def _():
                f(core)

    def ag_one(core):
        for d in stage1:
            d[core].start()

    def ag_two(core):
        for g, r in zip(got1, range(1, 4)):
            recv(g[core], ag_r.at[r])
        for ds in stage2:
            for d in ds[core]:
                d.start()

    def ag_end(core):
        for g, r in zip(got2, range(1, 4)):
            for n, b in enumerate(g[core]):
                recv(b, ah_r.at[r, n])

    def ag_drain(core):
        for d in stage1:
            d[core].wait_send()
        for ds in stage2:
            for d in ds[core]:
                d.wait_send()

    pending.append(lambda: by_core(ag_drain))
    fteam = [(1, 0), (1, 1), (0, 1)]

    def fdev(i):
        dh, dl = fteam[i]
        return at(x, rem(yh + dh, 2), c, z, rem(yl + dl, 2))

    def fdst(i, ks):
        return fall.at[ks, c, p] if fteam[i][1] == 0 else foth.at[yh, ks]

    def frcv(i, ks):
        dh, dl = fteam[i]
        return fall.at[ks, c, p + 1 - 2 * yh] if dl == 0 else foth.at[rem(yh + dh, 2), ks]

    gu, down = pl.ds(0, 2), pl.ds(2, 1)
    def factors_in(own, where):
        for i in where:
            recv(frcv(i, gu), ft_r.at[i])
        g = yh if own else 1 - yh
        for k in range(2):
            lanes = pl.ds(160 if own else 128, 32)
            lhs[yl, k, pl.ds(0, FB), lanes] = fall[k, c, 2 * x + g].T
            lhs[1 - yl, k, pl.ds(0, FB), lanes] = foth[g, k].T

    rowm = lax.broadcasted_iota(jnp.int32, (32, 256), 0) // 4
    lanem = lax.broadcasted_iota(jnp.int32, (32, 256), 1) // 128

    def hidden_rows():
        for i in range(8):
            g, cc = i // 4, i % 4
            for k in range(2):
                for gg in range(2):
                    of = yh if gg == 1 else 1 - yh
                    v = jnp.concatenate([ptt[of, k]] * 2, axis=1)
                    live = (rowm == 2 * cc + lanem) & (g == of)
                    rhs[i, k, pl.ds(128 + 32 * gg, 32)] = jnp.where(live, v, 0.0).astype(BF)

    def hidden(i):
        def rows(rb, _):
            r = pl.ds(pl.multiple_of(rb * HR, 16), HR)
            for t in range(2):
                ga = nn(lhs[t, 0, r], rhs[i, 0])
                up = nn(lhs[t, 1, r], rhs[i, 1])
                hbuf[i, t, r] = ((ga + ga * jnp.tanh(ga)) * up).astype(BF)
            return 0

        lax.fori_loop(0, FB // HR, rows, 0, unroll=HU)

    def chunk(j):
        return rem(j + 4 * (1 - yh), 8)

    sgn = 1 - 2 * c
    zn = rem(z + sgn + 8, 8)
    znd = at(x, yh, c, zn, yl)

    def part(d, i):
        return nn(dbuf[0, d], hbuf[i, 0]) + nn(dbuf[1, d], hbuf[i, 1])

    d0 = rem(z - sgn + 8, 8)

    def rsend(s, i, src):
        return rc(src, rcv.at[s, i], rs_s.at[s, i], rs_r.at[s, i], znd)


    def local_rows():
        for i in (6, 7, 3):
            loads[i].wait()
        for k in range(3):
            for m in range(8):
                fall[k, c, p, pl.ds(4 * m, 4)] = ftab[seeds[m], k]
        loads[4].wait()
        for k in range(3):
            for m in range(8):
                dk[k, pl.ds(4 * m, 4)] = dtab[seeds[m], k]

        eye = lax.broadcasted_iota(jnp.int32, (128, 256), 0) == rem(lax.broadcasted_iota(jnp.int32, (128, 256), 1), 128)
        for k in range(2):
            for i in range(8):
                rhs[i, k, 0:128] = jnp.where(eye, 1.0, 0.0).astype(BF)
            for t in range(2):
                lhs[t, k, :, pl.ds(128, 64)] = jnp.zeros((896, 64), BF)

    def base_half():
        send(bsend, brecv, bx_s, bx_r, partner)

    def base_scatter():
        bown[pl.ds(0, FB)] = partial_base(c)
        bown[pl.ds(FB, 32)] = jnp.zeros((32, 128), F32)
        recv(brecv, bx_r)
        for q in range(8):
            rows = pl.ds(112 * q, 112)
            ps[q // 4, q % 4] = (bown[rows] + brecv[rows].astype(F32)).astype(BF)
        for r in range(1, 4):
            xx = rem(x + r, 4)
            send(ps.at[:, xx], rsb.at[r], r1_s.at[r], r1_r.at[r], at(xx, yh, c, z, yl))

    def own_sum(h):
        mid = pl.ds(pl.multiple_of(112 * (4 * h + x), 16), 112)
        s = bown[mid] + brecv[mid].astype(F32)
        for r in range(1, 4):
            s += rsb[r, h].astype(F32)
        return s

    def base_mid():
        for r in range(1, 4):
            recv(rsb.at[r], r1_r.at[r])
        rsend2[...] = own_sum(1 - yh).astype(BF)
        send(rsend2, rrecv2, r1_s.at[0], r1_r.at[0], ypart)

    def base_sum():
        recv(rrecv2, r1_r.at[0])
        s = own_sum(yh) + rrecv2[...].astype(F32)
        s = jnp.where(c == 0, s * 0.5, s)
        bpiece(yl, c, own_row, 112)[...] = s.astype(BF)
        by_core(ag_one)

    def base_on():
        by_core(ag_two)

    def base_end():
        by_core(ag_end)
        send(lhs.at[:, c, :, pl.ds(0, 128)], lhs.at[:, c, :, pl.ds(0, 128)], bf_s, bf_r, partner)

    def base_other():
        recv(lhs.at[:, 1 - c, :, pl.ds(0, 128)], bf_r)

    def prompt_out():
        ptr = pt_v[...].astype(F32).T.astype(BF)
        psh[...] = jnp.zeros_like(psh)

        @pl.when(c == 0)
        def _():
            psh[:, 0:320] = ptr

        @pl.when(c == 1)
        def _():
            psh[:, 64:384] = ptr

        prb[c, p] = psh[toks]
        for r in range(1, 8):
            send(prb.at[c, p], prb.at[c, p], pr_s.at[r], pr_r.at[r], mate(2 * r))

    def prompt_on():
        for r in range(1, 8):
            recv(prb.at[c, rem(p - r + 8, 8)], pr_r.at[r])
        send(prb.at[c], prb.at[c], pr_s.at[0], pr_r.at[0], partner)

    def project():
        recv(prb.at[1 - c], pr_r.at[0])

        def proj_of(n, acc):
            cc, q = n // 8, rem(n, 8)
            lanes = pl.ds(pl.multiple_of(640 * q + 256 * cc, 128), 384)
            return acc + nt(prb[cc, q], dk[0:2, :, lanes].reshape(64, 384))

        acc = lax.fori_loop(0, 16, proj_of, jnp.zeros((16, 64), F32), unroll=4)
        acc = (acc / math.sqrt(D)).astype(BF).astype(F32)
        kk = lax.broadcasted_iota(jnp.int32, (16, 64), 1) // 32
        acc = jnp.where(kk == 0, acc * 0.25, acc * 0.5)
        pjs[...] = jnp.zeros_like(pjs)
        pjs[:, 0:64] = acc.astype(BF)
        pjb[yh, toks] = pjs[...]
        for r in range(1, 16):
            send(pjs, pjb.at[yh, toks], pj_s.at[r], pj_r.at[r], column(r))


    def project_in():
        for r in range(1, 16):
            hz, zz = rem(yh + r // 8, 2), rem(z - r % 8 + 8, 8)
            recv(pjb.at[hz, pl.ds(pl.multiple_of(16 * zz, 16), 16)], pj_r.at[r])
        for g in range(2):
            ptt[g] = pjb[g].astype(F32).T[0:64].reshape(2, 32, 128)
        hidden_rows()

    def y_first():
        ysend(0, 0)

    def y_first_b():
        ysend(0, 1)

    def y_second():
        ysend(1, 0)

    def y_second_b():
        ysend(1, 1)

    def x_first():
        wait_y(0, 0)
        own_x(0, 0)

    def x_first_b():
        wait_y(0, 1)
        own_x(0, 1)

    def x_second():
        wait_y(1, 0)
        own_x(1, 0)

    def x_second_b():
        wait_y(1, 1)
        own_x(1, 1)

    def down_out():
        send(fall.at[down, c, p], fdst(2, down), ft2_s.at[0], ft2_r.at[0], fdev(2))
        send(fall.at[down, c, p], fdst(0, down), ft2_s.at[1], ft2_r.at[1], fdev(0))

    def take_first():
        take[1, 0](0)
        take[3, 0](0)

    def take_first_b():
        take[1, 0](1)
        take[3, 0](1)

    def take_second():
        take[1, 1](0)
        take[3, 1](0)

    def take_second_b():
        take[1, 1](1)
        take[3, 1](1)

    def take_first_far():
        for part in range(2):
            take[2, 0](part)

    def first_in():
        for r in range(4):
            take_d(r, 0)

    def take_second_far():
        take[2, 1](0)

    def take_second_far_b():
        take[2, 1](1)

    def second_in():
        for r in range(4):
            take_d(r, 1)

    def factors_far():
        send(fall.at[gu, c, p], fdst(0, gu), ft_s.at[0], ft_r.at[0], fdev(0))

    def factors_diag():
        send(fall.at[gu, c, p], fdst(1, gu), ft_s.at[1], ft_r.at[1], fdev(1))

    def factors_near():
        send(fall.at[gu, c, p], fdst(2, gu), ft_s.at[2], ft_r.at[2], fdev(2))

    def factors_far_in():
        factors_in(False, (0, 1))

    def factors_near_in():
        factors_in(True, (2,))

    def hidden_ahead():
        def ahead(j, _):
            hidden(chunk(j))
            return 0

        lax.fori_loop(0, LEAD, ahead, 0)

    steps = dict(
        local_rows=local_rows, down_out=down_out,
        base_half=base_half, base_scatter=base_scatter, base_mid=base_mid, base_sum=base_sum, base_on=base_on, base_end=base_end,
        base_other=base_other, prompt_out=prompt_out, prompt_on=prompt_on, project=project,
        project_in=project_in, y_first=y_first, y_second=y_second, y_first_b=y_first_b, y_second_b=y_second_b, x_first=x_first, x_second=x_second, x_first_b=x_first_b, x_second_b=x_second_b,
        take_first=take_first, take_first_b=take_first_b, take_second_b=take_second_b, take_second=take_second, take_first_far=take_first_far, first_in=first_in,
        factors_far=factors_far, factors_diag=factors_diag, factors_near=factors_near, factors_far_in=factors_far_in,
        factors_near_in=factors_near_in, hidden_ahead=hidden_ahead,
    )
    for name in ORDER:
        steps[name]()

    def step_zero(j):
        i = chunk(j)
        snd[i] = part(d0, i).astype(BF)
        rsend(0, i, snd.at[i]).start()

    def first(j, _):
        i = chunk(j)
        p0 = part(d0, i).astype(BF)
        hidden(chunk(j + 1))
        snd[i] = p0
        rsend(0, i, snd.at[i]).start()
        pl.when(j == TB)(take_second)
        pl.when(j == TB2)(take_second_b)
        if TF <= 6:
            pl.when(j == TF)(take_second_far)
        if TF2 <= 6:
            pl.when(j == TF2)(take_second_far_b)
        return 0

    lax.fori_loop(0, 7, first, 0)
    if TF > 6:
        take_second_far()
    step_zero(7)
    if TF2 > 6:
        take_second_far_b()

    recv(frcv(0, down), ft2_r.at[1])

    def fpiece(i, other):
        return fall.at[:, c, 2 * rem(x - i + 4, 4) + (1 - yh if other else yh)]

    f_out, f_on = [], []
    for i in range(1, 4):
        f_out.append([rc(fpiece(0, h), fpiece(0, h), f_s.at[4 * h + i], f_r.at[4 * h + i], along_x[i]) for h in range(2)])
        f_on.append(rc(fpiece(i, 0), fpiece(i, 0), f_s.at[4 + i], f_r.at[4 + i], ypart))

    def factors_out(core):
        for d in f_out:
            for h in range(1 + core):
                d[h].start()

    def factors_drain(core):
        for d in f_out:
            for h in range(1 + core):
                d[h].wait_send()
        if core == 0:
            for d in f_on:
                d.wait_send()

    by_core(factors_out)
    pending.append(lambda: by_core(factors_drain))
    for m in range(8):
        fitall[c, p, pl.ds(m, 1)] = jnp.full((1, 128), fit[m], F32)

    def dlanes(q):
        return pl.ds(pl.multiple_of(640 * q, 128), 640)

    dall[:, c, p] = dk[:, :, dlanes(p)]
    for r in range(1, 8):
        q = rem(p + r, 8)
        send(dk.at[:, :, dlanes(q)], dall.at[:, c, p], d_s.at[r], d_r.at[r], mate(2 * r))
        send(fitall.at[c, p], fitall.at[c, p], q_s.at[r], q_r.at[r], mate(2 * r))

    second_in()

    fwd_f = rc(fall.at[:, c], fall.at[:, c], ff_s, ff_r, partner)
    pending.append(fwd_f.wait_send)

    def factors_on():
        @pl.when(c == 0)
        def _():
            for i in range(1, 4):
                recv(fpiece(i, 0), f_r.at[i])
            for d in f_on:
                d.start()

    def collect_f():
        @pl.when(c == 1)
        def _():
            for i in range(1, 4):
                recv(fpiece(i, 0), f_r.at[i])

        for i in range(1, 4):
            recv(fpiece(i, 1), f_r.at[4 + i])
        fwd_f.start()

    d_on = rc(dall.at[:, c], dall.at[:, c], d_s.at[0], d_r.at[0], partner)
    q_on = rc(fitall.at[c], fitall.at[c], q_s.at[0], q_r.at[0], partner)
    pending.extend([d_on.wait_send, q_on.wait_send])

    def factors_d_on():
        for r in range(1, 8):
            q = rem(p - r + 8, 8)
            recv(dall.at[:, c, q], d_r.at[r])
            recv(fitall.at[c, q], q_r.at[r])
        d_on.start()
        q_on.start()

    def collect_d():
        recv(dall.at[:, 1 - c], d_r.at[0])
        recv(fitall.at[1 - c], q_r.at[0])
        fv = fitall[...].reshape(128, 128)
        mean = jnp.sum(fv, axis=0, keepdims=True) / 128
        spread = jnp.sum((fv - mean) ** 2, axis=0, keepdims=True) / 128
        sc = (fv - mean) / jnp.sqrt(spread + 1.0)
        for i in range(16):
            v = jnp.broadcast_to(sc[8 * i : 8 * i + 8].reshape(8, 1, 128), (8, 4, 128))
            score[i // 8, i % 8] = v.reshape(32, 128)

    def weigh(k):
        def one(g, _):
            a, b = g // 8, rem(g, 8)
            sc = score[a, b]
            own = pl.ds(pl.multiple_of(256 * c, 128), 384)
            w = dall[k, a, b, :, own].astype(F32) * jnp.concatenate([sc] * 3, axis=1)
            wbuf[g] = w.astype(BF)
            return 0
        lax.fori_loop(0, 16, one, 0)
        wt[k] = wbuf[...].reshape(512, 384).T

    def delta(k, half):
        r = pl.ds(pl.multiple_of(64 * c + 160 * half, 16), 160)
        v = nn(wt[k, r], fall[k].reshape(512, FB)) * (1.0 / math.sqrt(512))
        del_ref[k, pl.ds(pl.multiple_of(160 * half, 16), 160)] = v.astype(BF)

    flips = [z + 1 - 2 * rem(z, 2), z + 2 - 4 * rem(z // 2, 2), z + 4 - 8 * (z // 4)]
    pd_out = [rc(pdc.at[k], pdb.at[k], pd_s.at[k], pd_r.at[k], at(x, yh, c, f, yl)) for k, f in enumerate(flips)]
    pending.extend(d.wait_send for d in pd_out)

    def down_sum(k):
        recv(pdb.at[k], pd_r.at[k])
        tot = pdc[k].astype(F32) + pdb[k].astype(F32)
        pdc[k + 1] = tot.astype(BF)
        pd_out[k + 1].start()

    def down_sums():
        recv(frcv(2, down), ft2_r.at[0])
        tot = jnp.zeros((32, 128), F32)
        for cc in range(4):
            i = 4 * yh + cc
            q = nn(fall[2, c, p], hbuf[i, yl]) + nn(foth[yh, 2], hbuf[i, 1 - yl])
            q = jnp.where(rowm == 2 * cc + lanem, q, 0.0)
            tot += q[:, :128] + q[:, 128:]
        pdc[0] = tot.astype(BF)
        pd_out[0].start()


    def noise_in():
        recv(pdb.at[2], pd_r.at[2])
        tot = pdc[2].astype(F32) + pdb[2].astype(F32)
        pdt[...] = (tot / math.sqrt(FFW)).astype(BF).astype(F32) * 0.5
        a2t[...] = dk[2, :, pl.ds(pl.multiple_of(640 * z + 256 * yl, 128), 384)].T

    def noise(j):
        live = rowm == 2 * j + lanem
        pm = jnp.where(live, jnp.concatenate([pdt[...]] * 2, axis=1), 0.0).astype(BF)
        for h in range(2):
            nbuf[h, j] = nn(a2t[pl.ds(pl.multiple_of(64 * yl + 160 * h, 16), 160)], pm)

    def place(n):
        m = n - 12
        late = jnp.where(rem(m + 16, 8) >= 4, 1, 0)
        s = jnp.where(n < 8, 1, jnp.where(n < 12, 2, jnp.where(n < 44, 3 + m // 8 - late, 6)))
        j = jnp.where(n < 8, n, jnp.where(n < 12, n - 8, jnp.where(n < 44, rem(m + 16, 8), n - 40)))
        return s, j

    def middle(n, _):
        s, j = place(n)
        i = chunk(j)
        pp = part(rem(z - sgn * (1 + s) + 16, 8), i)
        recv(rcv.at[s - 1, i], rs_r.at[s - 1, i])
        rcv[s - 1, i] = (pp + rcv[s - 1, i].astype(F32)).astype(BF)
        rsend(s, i, rcv.at[s - 1, i]).start()
        rsend(s - 1, i, rcv.at[s, i]).wait_send()

        @pl.when(n == PN)
        def _():
            down_sums()

        for k in range(2):
            pl.when(n == PN + 8 * (k + 1))(functools.partial(down_sum, k))

        @pl.when(n == NI)
        def _():
            noise_in()

        @pl.when((n > NI) & (n <= NI + 4))
        def _():
            noise(n - NI - 1)

        @pl.when(n == FX)
        def _():
            factors_on()

        @pl.when(n == CF)
        def _():
            collect_f()

        @pl.when(n == DX)
        def _():
            factors_d_on()

        m = n - CD

        @pl.when(m == 0)
        def _():
            collect_d()

        @pl.when((m >= 1) & (m < 4))
        def _():
            weigh(m - 1)

        @pl.when(m == 3)
        def _():
            recv(fall.at[:, 1 - c], ff_r)

        @pl.when((m >= 4) & (m < 4 + 6 * DS) & (rem(m, DS) == 0))
        def _():
            q = (m - 4) // DS
            delta(q // 2, rem(q, 2))

        return 0

    lax.fori_loop(0, 44, middle, 0)

    def last(j):
        i = chunk(j)
        pp = part(z, i)
        recv(rcv.at[6, i], rs_r.at[6, i])
        return pp + rcv[6, i].astype(F32)

    def last_far(j, _):
        fsnd[j] = last(j).astype(BF)
        rc(fsnd.at[j], fin.at[j], fs_s.at[j], fs_r.at[j], ypart).start()

        return 0

    lax.fori_loop(0, 4, last_far, 0)
    lax.fori_loop(44, 48, middle, 0)

    def put(j, h, w):
        for m in range(2):
            out_ref[2 * j + m, pl.ds(pl.multiple_of(160 * h, 16), 160)] = w[:, 128 * m : 128 * (m + 1)].astype(BF)

    def last_near(j, _):
        put(j, yh, last(j + 4) + nbuf[yh, j])
        return 0

    lax.fori_loop(0, 4, last_near, 0)

    def finish(j, _):
        rc(fsnd.at[j], fin.at[j], fs_s.at[j], fs_r.at[j], ypart).wait()
        put(j, 1 - yh, fin[j].astype(F32) + nbuf[1 - yh, j])
        return 0

    lax.fori_loop(0, 4, finish, 0)

    for w in pending:
        w()

    def drain(i, _):
        rsend(6, i, snd.at[i]).wait_send()
        return 0

    lax.fori_loop(0, 8, drain, 0)


def call_step(*arrays):
    arrays = [pltpu.with_memory_space_constraint(v, pltpu.HBM) for v in arrays]
    v = pl.BlockSpec(memory_space=pltpu.VMEM)
    a = pl.BlockSpec(memory_space=pltpu.HBM)
    dma = pltpu.SemaphoreType.DMA
    vm = pltpu.VMEM
    return pl.pallas_call(
        step_kernel,
        out_shape=[
            jax.ShapeDtypeStruct((8, 320, 128), BF),
            jax.ShapeDtypeStruct((3, 320, FB), BF),
        ],
        in_specs=[a] * 8,
        out_specs=[v, v],
        scratch_shapes=[
            pltpu.SMEM((8,), jnp.int32), pltpu.SMEM((8,), F32),
            vm((320, 128), BF), vm((2, 320, FB), BF), vm((2, 160, FB), BF), vm((16, 3, 4, D), BF), vm((16, 3, 4, FB), BF),
            vm((3, 32, D), BF), vm((3, 2, 8, 32, FB), BF), vm((2, 3, 32, FB), BF),
            vm((2, 8, 160, FB), BF), vm((8, 2, FB, 256), BF), vm((8, 160, 256), BF),
            vm((7, 8, 160, 256), BF), vm((4, 160, 256), BF), vm((4, 160, 256), BF),
            vm((896, 128), BF), vm((896, 128), BF), vm((896, 128), F32), vm((2, 4, 112, 128), BF),
            vm((4, 2, 112, 128), BF), vm((112, 128), BF), vm((112, 128), BF), vm((2, 2, 896, 192), BF), vm((8, 2, 192, 256), BF),
            vm((128, 384), BF), vm((2, 8, 16, 384), BF), vm((16, 128), BF), vm((2, 128, 128), BF),
            vm((2, 2, 32, 128), F32),
            vm((3, 32, 128), BF), vm((3, 32, 128), BF), vm((32, 128), F32), vm((3, 2, 8, 32, 640), BF),
            vm((2, 8, 8, 128), F32), vm((2, 8, 32, 128), F32), vm((3, 384, 512), BF), vm((384, 32), BF), vm((2, 4, 160, 256), F32), vm((16, 32, 384), BF),
            dma((8,)), dma(()), dma(()), dma((8,)), dma((8,)), dma((4,)), dma((4,)), dma((4, 4)), dma((4, 4)), dma(()), dma(()),
            dma((8,)), dma((8,)), dma((16,)), dma((16,)),
            dma((3,)), dma((3,)), dma((2,)), dma((2,)), dma((2, 2)), dma((2, 2)), dma((2,)), dma((2, 2, 2)), dma((4, 2, 2)), dma((4, 2, 2)),
            dma((4, 2, 2)), dma((4, 2, 2)), dma((7, 8)), dma((7, 8)), dma((4,)), dma((4,)),
            dma((8,)), dma((8,)), dma((8,)), dma((8,)), dma(()), dma(()), dma((16,)), dma((16,)),
            dma((16,)), dma((16,)),
        ],
        compiler_params=pltpu.CompilerParams(
            collective_id=0, has_side_effects=True, vmem_limit_bytes=44 << 20
        ),
        name="es_step",
    )(*arrays)


EMIT_LIM = 4 << 20


def emit_kernel(out, deltas, o_hbm, g_hbm, u_hbm, d_hbm, sems):
    pairs = [(deltas.at[0], g_hbm), (deltas.at[1], u_hbm), (deltas.at[2], d_hbm), (out, o_hbm)]
    copies = [pltpu.make_async_copy(a, b, sems.at[i]) for i, (a, b) in enumerate(pairs)]
    for d in copies:
        d.start()
    for d in copies:
        d.wait()


def emit(out, deltas):
    v = pl.BlockSpec(memory_space=pltpu.VMEM)
    a = pl.BlockSpec(memory_space=pltpu.HBM)
    one = jax.ShapeDtypeStruct((320, FB), BF)
    return pl.pallas_call(
        emit_kernel,
        out_shape=[jax.ShapeDtypeStruct((8, 320, 128), BF), one, one, one],
        in_specs=[v, v],
        out_specs=[a, a, a, a],
        scratch_shapes=[pltpu.SemaphoreType.DMA((4,))],
        compiler_params=pltpu.CompilerParams(vmem_limit_bytes=EMIT_LIM),
        name="emit",
    )(out, deltas)


def shards(prompt_acts, gate_weight, up_weight, down_weight, d_table, f_table, seeds, fitness):
    out, deltas = call_step(
        prompt_acts.T, gate_weight, up_weight, down_weight.T.reshape(2, 160, FB), d_table, f_table,
        seeds, fitness,
    )
    out, dg, du, dd = emit(out, deltas)
    return out.transpose(0, 2, 1), dg, du, dd.T


def solution(mesh):
    split = Mesh(mesh.devices.reshape(4, 2, 2, 8, 2), AX)
    placed = (
        P(None, MEMBER), P(MEMBER, TENSOR), P(MEMBER, TENSOR), P(TENSOR, MEMBER),
        P(MEMBER, None, None, None), P(MEMBER, None, None, TENSOR), P(MEMBER), P(MEMBER),
    )
    return jax.shard_map(
        shards, mesh=split, in_specs=placed,
        out_specs=(P(MEMBER, None, TENSOR), P(MEMBER, TENSOR), P(MEMBER, TENSOR), P(TENSOR, MEMBER)),
        check_vma=False,
    )
```

```python
import functools
import math

import jax
import jax.numpy as jnp
from jax import lax
from jax.experimental import pallas as pl
from jax.experimental.pallas import tpu as pltpu
from jax.sharding import Mesh
from jax.sharding import PartitionSpec as P

D = 5120
FFW = 13824
FB = 864
AX = ("x", "yh", "c", "z", "yl")
MEMBER = ("x", "yh", "c")
TENSOR = ("z", "yl")
MESH = pl.DeviceIdType.MESH
BF = jnp.bfloat16
F32 = jnp.float32
HR = 864
HU = 1
LEAD = 1
TB = 0
TB2 = 2
TF = 5
TF2 = 6
FX = 17
PN = 4
NI = 32
CF = 35
DX = 33
CD = 38
DS = 1
ORDER = (
    "y_second",
    "y_first",
    "y_first_b",
    "base_half",
    "y_second_b",
    "base_scatter",
    "prompt_out",
    "base_mid",
    "x_first",
    "base_sum",
    "x_first_b",
    "local_rows",
    "factors_far",
    "factors_diag",
    "prompt_on",
    "take_first",
    "base_on",
    "factors_near",
    "take_first_b",
    "x_second",
    "project",
    "factors_near_in",
    "x_second_b",
    "factors_far_in",
    "base_end",
    "take_first_far",
    "project_in",
    "base_other",
    "down_out",
    "hidden_ahead",
    "first_in",
)


def rem(a, n):
    return lax.rem(a, n)


def at(x, yh, c, z, yl):
    return {"x": x, "yh": yh, "c": c, "z": z, "yl": yl}


def tn(a, b):
    return lax.dot_general(a, b, (((0,), (0,)), ((), ())), preferred_element_type=F32)


def nt(a, b):
    return lax.dot_general(a, b, (((1,), (1,)), ((), ())), preferred_element_type=F32)


def nn(a, b):
    return jnp.dot(a, b, preferred_element_type=F32)


def step_kernel(
    pt_hbm, gw_hbm, uw_hbm, dt_hbm, dtab_hbm, ftab_hbm, seeds_hbm, fit_hbm,
    out_ref, del_ref,
    seeds, fit, pt_v, w_v, dt_v, dtab, ftab, dk, fall, foth, dbuf, hbuf, snd, rcv, fin, fsnd,
    bsend, brecv, bown, ps, rsb, rsend2, rrecv2, lhs, rhs, psh, prb, pjs, pjb, ptt,
    pdc, pdb, pdt, dall, fitall, score, wt, a2t, nbuf, wbuf,
    in_s, bx_s, bx_r, r1_s, r1_r, ag_s, ag_r, ah_s, ah_r, bf_s, bf_r, pr_s, pr_r, pj_s, pj_r,
    ft_s, ft_r, ft2_s, ft2_r, ys, yr, yloc, xo_s, xf_s, x_r, ds_s, ds_r, rs_s, rs_r, fs_s, fs_r,
    pd_s, pd_r, f_s, f_r, ff_s, ff_r, d_s, d_r, q_s, q_r,
):
    x, yh, c, z, yl = [lax.axis_index(a) for a in AX]
    y = 2 * yh + yl
    p = 2 * x + yh
    me = at(x, yh, c, z, yl)
    partner = at(x, yh, 1 - c, z, yl)
    ypart = at(x, 1 - yh, c, z, yl)
    pending = []

    def rc(src, dst, ss, rs, dev):
        return pltpu.make_async_remote_copy(
            src_ref=src, dst_ref=dst, send_sem=ss, recv_sem=rs, device_id=dev, device_id_type=MESH
        )

    def send(src, dst, ss, rs, dev):
        d = rc(src, dst, ss, rs, dev)
        d.start()
        pending.append(d.wait_send)

    def recv(dst, rs):
        rc(dst, dst, rs, rs, partner).wait_recv()

    loads = [
        (gw_hbm, w_v.at[0]), (uw_hbm, w_v.at[1]), (pt_hbm, pt_v), (ftab_hbm, ftab), (dtab_hbm, dtab),
        (dt_hbm, dt_v), (seeds_hbm, seeds), (fit_hbm, fit),
    ]
    loads = [pltpu.make_async_copy(a, b, in_s.at[i]) for i, (a, b) in enumerate(loads)]
    for i in (5, 2, 0, 1, 6, 7, 3, 4):
        loads[i].start()

    def plane(rel):
        ny = rem(y + rel % 4, 4)
        return at(rem(x + rel // 4, 4), ny // 2, c, z, rem(ny, 2))

    def mate(rel):
        q = rem(p + rel // 2, 8)
        return at(q // 2, rem(q, 2), rem(c + rel % 2, 2), z, yl)

    def column(rel):
        return at(x, rem(yh + rel // 8, 2), c, rem(z + rel % 8, 8), yl)

    ypeers = [at(x, h, yl, z, c) for h in range(2)]
    me_y = [(h == yh) & (c == yl) for h in range(2)]
    barrier = pltpu.get_barrier_semaphore()

    def greet(dev):
        pl.semaphore_signal(barrier, inc=1, device_id=dev, device_id_type=MESH)

    peers = [plane(1), plane(3)] + [mate(r) for r in range(1, 16)]
    peers += [column(r) for r in range(1, 16) if r != 8]
    for o in peers:
        greet(o)
    @pl.when(c != yl)
    def _():
        for h in range(2):
            greet(ypeers[h])

    def partial_base(k):
        return tn(w_v[k], pt_v[...])

    for i in (0, 1, 2, 5):
        loads[i].wait()
    bsend[pl.ds(0, FB)] = partial_base(1 - c).astype(BF)
    bsend[pl.ds(FB, 32)] = jnp.zeros((32, 128), BF)
    n_peers = len(peers)
    @pl.when(c == yl)
    def _():
        pl.semaphore_wait(barrier, n_peers)

    @pl.when(c != yl)
    def _():
        pl.semaphore_wait(barrier, n_peers + 2)

    e, kz = rem(z, 2), z // 2

    def low(x0):
        m = rem(x0 - kz + 4, 4)
        return jnp.where(e == 0, jnp.where(m == 1, 0, 1), jnp.where(m == 3, 1, 0))

    def zblk(r, ab):
        x0 = rem(x - r + 4, 4)
        return 2 * x0 + (low(x0) if ab == 0 else 1 - low(x0))

    own_a = low(x)

    def half(b, part):
        return b.at[pl.ds(80 * part, 80)]

    def ycopy(h, part):
        dst = half(dbuf.at[yl, 2 * x + yh], part)
        return rc(half(dt_v.at[h], part), dst, ys.at[h, part], yr.at[yh, part], ypeers[h])

    def ylocal(h, part):
        return pltpu.make_async_copy(half(dt_hbm.at[h], part), half(dbuf.at[yl, 2 * x + yh], part), yloc.at[part])

    def ysend(ab, part):
        mine = yh == (own_a if ab == 0 else 1 - own_a)
        for h in range(2):
            @pl.when(mine & jnp.logical_not(me_y[h]))
            def _():
                ycopy(h, part).start()
            @pl.when(mine & me_y[h])
            def _():
                ylocal(h, part).start()

    def wait_y(ab, part):
        w = own_a if ab == 0 else 1 - own_a
        here = (w == yh) & (c == yl)

        @pl.when(jnp.logical_not(here))
        def _():
            recv(half(dbuf.at[c, 2 * x + w], part), yr.at[w, part])

        @pl.when(here)
        def _():
            ylocal(0, part).wait()

    def y_drain():
        for h in range(2):
            @pl.when(jnp.logical_not(me_y[h]))
            def _():
                for part in range(2):
                    ycopy(h, part).wait_send()

    pending.append(y_drain)
    xnb = [at(rem(x + 1, 4), yh, c, z, yl), at(rem(x + 3, 4), yh, c, z, yl)]

    def dsend(r, ab, part):
        b = half(dbuf.at[c, zblk(r, ab)], part)
        d = rc(b, b, ds_s.at[r, ab, part], ds_r.at[r, ab, part], partner)
        pending.append(d.wait_send)
        return d

    def own_x(ab, part):
        b = dbuf.at[c, zblk(0, ab)]
        dsend(0, ab, part).start()
        b = half(b, part)
        send(b, b, xo_s.at[0, ab, part], x_r.at[1, ab, part], xnb[0])
        send(b, b, xo_s.at[1, ab, part], x_r.at[3, ab, part], xnb[1])

    def taker(r, ab):
        b = dbuf.at[c, zblk(r, ab)]
        d2 = [dsend(r, ab, part) for part in range(2)]
        fwd = c == (0 if r == 1 else 1)
        hops = []
        for part in range(2 if r != 2 else 0):
            h = half(b, part)
            d = rc(h, h, xf_s.at[r, ab, part], x_r.at[2, ab, part], xnb[0 if r == 1 else 1])
            hops.append(d)
            pending.append(functools.partial(pl.when(fwd), d.wait_send))

        def run(part):
            recv(half(b, part), x_r.at[r, ab, part])
            if r != 2:
                pl.when(fwd)(hops[part].start)
            d2[part].start()

        return run

    take = {(r, ab): taker(r, ab) for r in (1, 3, 2) for ab in range(2)}

    def take_d(r, ab):
        for part in range(2):
            recv(half(dbuf.at[1 - c, zblk(r, ab)], part), ds_r.at[r, ab, part])

    toks = pl.ds(pl.multiple_of(16 * z, 16), 16)
    own_row = 4 * yh + x
    def bpiece(t, k, first, rows):
        return lhs.at[t, k, pl.ds(pl.multiple_of(112 * first, 16), rows), pl.ds(0, 128)]

    along_x = [at(rem(x + r, 4), yh, c, z, yl) for r in range(4)]
    along_y = [at(x, rem(y + r, 4) // 2, c, z, rem(y + r, 2)) for r in range(4)]
    stage1, stage2, got1, got2 = [], [], [], []
    for r in range(1, 4):
        b = bpiece(yl, c, own_row, 112)
        stage1.append((rc(b, b, ag_s.at[r], ag_r.at[r], along_x[r]), rc(b, b, ag_s.at[r], ag_r.at[r], along_y[r])))
        xx, yy = rem(x - r + 4, 4), rem(y - r + 4, 4)
        got1.append((bpiece(yl, c, 4 * yh + xx, 112), bpiece(rem(yy, 2), c, 4 * (yy // 2) + x, 112)))
        b = bpiece(yl, c, 4 * yh, 448)
        far = []
        for n in range(4):
            f = bpiece(n // 2, c, 4 * (n % 2) + x, 112)
            far.append(rc(f, f, ah_s.at[r, n], ah_r.at[r, n], along_x[r]))
        stage2.append(([rc(b, b, ah_s.at[r, 0], ah_r.at[r, 0], along_y[r])], far))
        got2.append((
            [bpiece(rem(yy, 2), c, 4 * (yy // 2), 448)],
            [bpiece(n // 2, c, 4 * (n % 2) + xx, 112) for n in range(4)],
        ))

    def by_core(f):
        for core in range(2):
            @pl.when(c == core)
            def _():
                f(core)

    def ag_one(core):
        for d in stage1:
            d[core].start()

    def ag_two(core):
        for g, r in zip(got1, range(1, 4)):
            recv(g[core], ag_r.at[r])
        for ds in stage2:
            for d in ds[core]:
                d.start()

    def ag_end(core):
        for g, r in zip(got2, range(1, 4)):
            for n, b in enumerate(g[core]):
                recv(b, ah_r.at[r, n])

    def ag_drain(core):
        for d in stage1:
            d[core].wait_send()
        for ds in stage2:
            for d in ds[core]:
                d.wait_send()

    pending.append(lambda: by_core(ag_drain))
    fteam = [(1, 0), (1, 1), (0, 1)]

    def fdev(i):
        dh, dl = fteam[i]
        return at(x, rem(yh + dh, 2), c, z, rem(yl + dl, 2))

    def fdst(i, ks):
        return fall.at[ks, c, p] if fteam[i][1] == 0 else foth.at[yh, ks]

    def frcv(i, ks):
        dh, dl = fteam[i]
        return fall.at[ks, c, p + 1 - 2 * yh] if dl == 0 else foth.at[rem(yh + dh, 2), ks]

    gu, down = pl.ds(0, 2), pl.ds(2, 1)
    def factors_in(own, where):
        for i in where:
            recv(frcv(i, gu), ft_r.at[i])
        g = yh if own else 1 - yh
        for k in range(2):
            lanes = pl.ds(160 if own else 128, 32)
            lhs[yl, k, pl.ds(0, FB), lanes] = fall[k, c, 2 * x + g].T
            lhs[1 - yl, k, pl.ds(0, FB), lanes] = foth[g, k].T

    rowm = lax.broadcasted_iota(jnp.int32, (32, 256), 0) // 4
    lanem = lax.broadcasted_iota(jnp.int32, (32, 256), 1) // 128

    def hidden_rows():
        for i in range(8):
            g, cc = i // 4, i % 4
            for k in range(2):
                for gg in range(2):
                    of = yh if gg == 1 else 1 - yh
                    v = jnp.concatenate([ptt[of, k]] * 2, axis=1)
                    live = (rowm == 2 * cc + lanem) & (g == of)
                    rhs[i, k, pl.ds(128 + 32 * gg, 32)] = jnp.where(live, v, 0.0).astype(BF)

    def hidden(i):
        def rows(rb, _):
            r = pl.ds(pl.multiple_of(rb * HR, 16), HR)
            for t in range(2):
                ga = nn(lhs[t, 0, r], rhs[i, 0])
                up = nn(lhs[t, 1, r], rhs[i, 1])
                hbuf[i, t, r] = ((ga + ga * jnp.tanh(ga)) * up).astype(BF)
            return 0

        lax.fori_loop(0, FB // HR, rows, 0, unroll=HU)

    def chunk(j):
        return rem(j + 4 * (1 - yh), 8)

    sgn = 1 - 2 * c
    zn = rem(z + sgn + 8, 8)
    znd = at(x, yh, c, zn, yl)

    def part(d, i):
        return nn(dbuf[0, d], hbuf[i, 0]) + nn(dbuf[1, d], hbuf[i, 1])

    d0 = rem(z - sgn + 8, 8)

    def rsend(s, i, src):
        return rc(src, rcv.at[s, i], rs_s.at[s, i], rs_r.at[s, i], znd)


    def local_rows():
        for i in (6, 7, 3):
            loads[i].wait()
        for k in range(3):
            for m in range(8):
                fall[k, c, p, pl.ds(4 * m, 4)] = ftab[seeds[m], k]
        loads[4].wait()
        for k in range(3):
            for m in range(8):
                dk[k, pl.ds(4 * m, 4)] = dtab[seeds[m], k]

        eye = lax.broadcasted_iota(jnp.int32, (128, 256), 0) == rem(lax.broadcasted_iota(jnp.int32, (128, 256), 1), 128)
        for k in range(2):
            for i in range(8):
                rhs[i, k, 0:128] = jnp.where(eye, 1.0, 0.0).astype(BF)
            for t in range(2):
                lhs[t, k, :, pl.ds(128, 64)] = jnp.zeros((896, 64), BF)

    def base_half():
        send(bsend, brecv, bx_s, bx_r, partner)

    def base_scatter():
        bown[pl.ds(0, FB)] = partial_base(c)
        bown[pl.ds(FB, 32)] = jnp.zeros((32, 128), F32)
        recv(brecv, bx_r)
        for q in range(8):
            rows = pl.ds(112 * q, 112)
            ps[q // 4, q % 4] = (bown[rows] + brecv[rows].astype(F32)).astype(BF)
        for r in range(1, 4):
            xx = rem(x + r, 4)
            send(ps.at[:, xx], rsb.at[r], r1_s.at[r], r1_r.at[r], at(xx, yh, c, z, yl))

    def own_sum(h):
        mid = pl.ds(pl.multiple_of(112 * (4 * h + x), 16), 112)
        s = bown[mid] + brecv[mid].astype(F32)
        for r in range(1, 4):
            s += rsb[r, h].astype(F32)
        return s

    def base_mid():
        for r in range(1, 4):
            recv(rsb.at[r], r1_r.at[r])
        rsend2[...] = own_sum(1 - yh).astype(BF)
        send(rsend2, rrecv2, r1_s.at[0], r1_r.at[0], ypart)

    def base_sum():
        recv(rrecv2, r1_r.at[0])
        s = own_sum(yh) + rrecv2[...].astype(F32)
        s = jnp.where(c == 0, s * 0.5, s)
        bpiece(yl, c, own_row, 112)[...] = s.astype(BF)
        by_core(ag_one)

    def base_on():
        by_core(ag_two)

    def base_end():
        by_core(ag_end)
        send(lhs.at[:, c, :, pl.ds(0, 128)], lhs.at[:, c, :, pl.ds(0, 128)], bf_s, bf_r, partner)

    def base_other():
        recv(lhs.at[:, 1 - c, :, pl.ds(0, 128)], bf_r)

    def prompt_out():
        ptr = pt_v[...].astype(F32).T.astype(BF)
        psh[...] = jnp.zeros_like(psh)

        @pl.when(c == 0)
        def _():
            psh[:, 0:320] = ptr

        @pl.when(c == 1)
        def _():
            psh[:, 64:384] = ptr

        prb[c, p] = psh[toks]
        for r in range(1, 8):
            send(prb.at[c, p], prb.at[c, p], pr_s.at[r], pr_r.at[r], mate(2 * r))

    def prompt_on():
        for r in range(1, 8):
            recv(prb.at[c, rem(p - r + 8, 8)], pr_r.at[r])
        send(prb.at[c], prb.at[c], pr_s.at[0], pr_r.at[0], partner)

    def project():
        recv(prb.at[1 - c], pr_r.at[0])

        def proj_of(n, acc):
            cc, q = n // 8, rem(n, 8)
            lanes = pl.ds(pl.multiple_of(640 * q + 256 * cc, 128), 384)
            return acc + nt(prb[cc, q], dk[0:2, :, lanes].reshape(64, 384))

        acc = lax.fori_loop(0, 16, proj_of, jnp.zeros((16, 64), F32), unroll=4)
        acc = (acc / math.sqrt(D)).astype(BF).astype(F32)
        kk = lax.broadcasted_iota(jnp.int32, (16, 64), 1) // 32
        acc = jnp.where(kk == 0, acc * 0.25, acc * 0.5)
        pjs[...] = jnp.zeros_like(pjs)
        pjs[:, 0:64] = acc.astype(BF)
        pjb[yh, toks] = pjs[...]
        for r in range(1, 16):
            send(pjs, pjb.at[yh, toks], pj_s.at[r], pj_r.at[r], column(r))


    def project_in():
        for r in range(1, 16):
            hz, zz = rem(yh + r // 8, 2), rem(z - r % 8 + 8, 8)
            recv(pjb.at[hz, pl.ds(pl.multiple_of(16 * zz, 16), 16)], pj_r.at[r])
        for g in range(2):
            ptt[g] = pjb[g].astype(F32).T[0:64].reshape(2, 32, 128)
        hidden_rows()

    def y_first():
        ysend(0, 0)

    def y_first_b():
        ysend(0, 1)

    def y_second():
        ysend(1, 0)

    def y_second_b():
        ysend(1, 1)

    def x_first():
        wait_y(0, 0)
        own_x(0, 0)

    def x_first_b():
        wait_y(0, 1)
        own_x(0, 1)

    def x_second():
        wait_y(1, 0)
        own_x(1, 0)

    def x_second_b():
        wait_y(1, 1)
        own_x(1, 1)

    def down_out():
        send(fall.at[down, c, p], fdst(2, down), ft2_s.at[0], ft2_r.at[0], fdev(2))
        send(fall.at[down, c, p], fdst(0, down), ft2_s.at[1], ft2_r.at[1], fdev(0))

    def take_first():
        take[1, 0](0)
        take[3, 0](0)

    def take_first_b():
        take[1, 0](1)
        take[3, 0](1)

    def take_second():
        take[1, 1](0)
        take[3, 1](0)

    def take_second_b():
        take[1, 1](1)
        take[3, 1](1)

    def take_first_far():
        for part in range(2):
            take[2, 0](part)

    def first_in():
        for r in range(4):
            take_d(r, 0)

    def take_second_far():
        take[2, 1](0)

    def take_second_far_b():
        take[2, 1](1)

    def second_in():
        for r in range(4):
            take_d(r, 1)

    def factors_far():
        send(fall.at[gu, c, p], fdst(0, gu), ft_s.at[0], ft_r.at[0], fdev(0))

    def factors_diag():
        send(fall.at[gu, c, p], fdst(1, gu), ft_s.at[1], ft_r.at[1], fdev(1))

    def factors_near():
        send(fall.at[gu, c, p], fdst(2, gu), ft_s.at[2], ft_r.at[2], fdev(2))

    def factors_far_in():
        factors_in(False, (0, 1))

    def factors_near_in():
        factors_in(True, (2,))

    def hidden_ahead():
        def ahead(j, _):
            hidden(chunk(j))
            return 0

        lax.fori_loop(0, LEAD, ahead, 0)

    steps = dict(
        local_rows=local_rows, down_out=down_out,
        base_half=base_half, base_scatter=base_scatter, base_mid=base_mid, base_sum=base_sum, base_on=base_on, base_end=base_end,
        base_other=base_other, prompt_out=prompt_out, prompt_on=prompt_on, project=project,
        project_in=project_in, y_first=y_first, y_second=y_second, y_first_b=y_first_b, y_second_b=y_second_b, x_first=x_first, x_second=x_second, x_first_b=x_first_b, x_second_b=x_second_b,
        take_first=take_first, take_first_b=take_first_b, take_second_b=take_second_b, take_second=take_second, take_first_far=take_first_far, first_in=first_in,
        factors_far=factors_far, factors_diag=factors_diag, factors_near=factors_near, factors_far_in=factors_far_in,
        factors_near_in=factors_near_in, hidden_ahead=hidden_ahead,
    )
    for name in ORDER:
        steps[name]()

    def step_zero(j):
        i = chunk(j)
        snd[i] = part(d0, i).astype(BF)
        rsend(0, i, snd.at[i]).start()

    def first(j, _):
        i = chunk(j)
        p0 = part(d0, i).astype(BF)
        hidden(chunk(j + 1))
        snd[i] = p0
        rsend(0, i, snd.at[i]).start()
        pl.when(j == TB)(take_second)
        pl.when(j == TB2)(take_second_b)
        if TF <= 6:
            pl.when(j == TF)(take_second_far)
        if TF2 <= 6:
            pl.when(j == TF2)(take_second_far_b)
        return 0

    lax.fori_loop(0, 7, first, 0)
    if TF > 6:
        take_second_far()
    step_zero(7)
    if TF2 > 6:
        take_second_far_b()

    recv(frcv(0, down), ft2_r.at[1])

    def fpiece(i, other):
        return fall.at[:, c, 2 * rem(x - i + 4, 4) + (1 - yh if other else yh)]

    f_out, f_on = [], []
    for i in range(1, 4):
        f_out.append([rc(fpiece(0, h), fpiece(0, h), f_s.at[4 * h + i], f_r.at[4 * h + i], along_x[i]) for h in range(2)])
        f_on.append(rc(fpiece(i, 0), fpiece(i, 0), f_s.at[4 + i], f_r.at[4 + i], ypart))

    def factors_out(core):
        for d in f_out:
            for h in range(1 + core):
                d[h].start()

    def factors_drain(core):
        for d in f_out:
            for h in range(1 + core):
                d[h].wait_send()
        if core == 0:
            for d in f_on:
                d.wait_send()

    by_core(factors_out)
    pending.append(lambda: by_core(factors_drain))
    for m in range(8):
        fitall[c, p, pl.ds(m, 1)] = jnp.full((1, 128), fit[m], F32)

    def dlanes(q):
        return pl.ds(pl.multiple_of(640 * q, 128), 640)

    dall[:, c, p] = dk[:, :, dlanes(p)]
    for r in range(1, 8):
        q = rem(p + r, 8)
        send(dk.at[:, :, dlanes(q)], dall.at[:, c, p], d_s.at[r], d_r.at[r], mate(2 * r))
        send(fitall.at[c, p], fitall.at[c, p], q_s.at[r], q_r.at[r], mate(2 * r))

    second_in()

    fwd_f = rc(fall.at[:, c], fall.at[:, c], ff_s, ff_r, partner)
    pending.append(fwd_f.wait_send)

    def factors_on():
        @pl.when(c == 0)
        def _():
            for i in range(1, 4):
                recv(fpiece(i, 0), f_r.at[i])
            for d in f_on:
                d.start()

    def collect_f():
        @pl.when(c == 1)
        def _():
            for i in range(1, 4):
                recv(fpiece(i, 0), f_r.at[i])

        for i in range(1, 4):
            recv(fpiece(i, 1), f_r.at[4 + i])
        fwd_f.start()

    d_on = rc(dall.at[:, c], dall.at[:, c], d_s.at[0], d_r.at[0], partner)
    q_on = rc(fitall.at[c], fitall.at[c], q_s.at[0], q_r.at[0], partner)
    pending.extend([d_on.wait_send, q_on.wait_send])

    def factors_d_on():
        for r in range(1, 8):
            q = rem(p - r + 8, 8)
            recv(dall.at[:, c, q], d_r.at[r])
            recv(fitall.at[c, q], q_r.at[r])
        d_on.start()
        q_on.start()

    def collect_d():
        recv(dall.at[:, 1 - c], d_r.at[0])
        recv(fitall.at[1 - c], q_r.at[0])
        fv = fitall[...].reshape(128, 128)
        mean = jnp.sum(fv, axis=0, keepdims=True) / 128
        spread = jnp.sum((fv - mean) ** 2, axis=0, keepdims=True) / 128
        sc = (fv - mean) / jnp.sqrt(spread + 1.0)
        for i in range(16):
            v = jnp.broadcast_to(sc[8 * i : 8 * i + 8].reshape(8, 1, 128), (8, 4, 128))
            score[i // 8, i % 8] = v.reshape(32, 128)

    def weigh(k):
        def one(g, _):
            a, b = g // 8, rem(g, 8)
            sc = score[a, b]
            own = pl.ds(pl.multiple_of(256 * c, 128), 384)
            w = dall[k, a, b, :, own].astype(F32) * jnp.concatenate([sc] * 3, axis=1)
            wbuf[g] = w.astype(BF)
            return 0
        lax.fori_loop(0, 16, one, 0)
        wt[k] = wbuf[...].reshape(512, 384).T

    def delta(k, half):
        r = pl.ds(pl.multiple_of(64 * c + 160 * half, 16), 160)
        v = nn(wt[k, r], fall[k].reshape(512, FB)) * (1.0 / math.sqrt(512))
        del_ref[k, pl.ds(pl.multiple_of(160 * half, 16), 160)] = v.astype(BF)

    flips = [z + 1 - 2 * rem(z, 2), z + 2 - 4 * rem(z // 2, 2), z + 4 - 8 * (z // 4)]
    pd_out = [rc(pdc.at[k], pdb.at[k], pd_s.at[k], pd_r.at[k], at(x, yh, c, f, yl)) for k, f in enumerate(flips)]
    pending.extend(d.wait_send for d in pd_out)

    def down_sum(k):
        recv(pdb.at[k], pd_r.at[k])
        tot = pdc[k].astype(F32) + pdb[k].astype(F32)
        pdc[k + 1] = tot.astype(BF)
        pd_out[k + 1].start()

    def down_sums():
        recv(frcv(2, down), ft2_r.at[0])
        tot = jnp.zeros((32, 128), F32)
        for cc in range(4):
            i = 4 * yh + cc
            q = nn(fall[2, c, p], hbuf[i, yl]) + nn(foth[yh, 2], hbuf[i, 1 - yl])
            q = jnp.where(rowm == 2 * cc + lanem, q, 0.0)
            tot += q[:, :128] + q[:, 128:]
        pdc[0] = tot.astype(BF)
        pd_out[0].start()


    def noise_in():
        recv(pdb.at[2], pd_r.at[2])
        tot = pdc[2].astype(F32) + pdb[2].astype(F32)
        pdt[...] = (tot / math.sqrt(FFW)).astype(BF).astype(F32) * 0.5
        a2t[...] = dk[2, :, pl.ds(pl.multiple_of(640 * z + 256 * yl, 128), 384)].T

    def noise(j):
        live = rowm == 2 * j + lanem
        pm = jnp.where(live, jnp.concatenate([pdt[...]] * 2, axis=1), 0.0).astype(BF)
        for h in range(2):
            nbuf[h, j] = nn(a2t[pl.ds(pl.multiple_of(64 * yl + 160 * h, 16), 160)], pm)

    def place(n):
        m = n - 12
        late = jnp.where(rem(m + 16, 8) >= 4, 1, 0)
        s = jnp.where(n < 8, 1, jnp.where(n < 12, 2, jnp.where(n < 44, 3 + m // 8 - late, 6)))
        j = jnp.where(n < 8, n, jnp.where(n < 12, n - 8, jnp.where(n < 44, rem(m + 16, 8), n - 40)))
        return s, j

    def middle(n, _):
        s, j = place(n)
        i = chunk(j)
        pp = part(rem(z - sgn * (1 + s) + 16, 8), i)
        recv(rcv.at[s - 1, i], rs_r.at[s - 1, i])
        rcv[s - 1, i] = (pp + rcv[s - 1, i].astype(F32)).astype(BF)
        rsend(s, i, rcv.at[s - 1, i]).start()
        rsend(s - 1, i, rcv.at[s, i]).wait_send()

        @pl.when(n == PN)
        def _():
            down_sums()

        for k in range(2):
            pl.when(n == PN + 8 * (k + 1))(functools.partial(down_sum, k))

        @pl.when(n == NI)
        def _():
            noise_in()

        @pl.when((n > NI) & (n <= NI + 4))
        def _():
            noise(n - NI - 1)

        @pl.when(n == FX)
        def _():
            factors_on()

        @pl.when(n == CF)
        def _():
            collect_f()

        @pl.when(n == DX)
        def _():
            factors_d_on()

        m = n - CD

        @pl.when(m == 0)
        def _():
            collect_d()

        @pl.when((m >= 1) & (m < 4))
        def _():
            weigh(m - 1)

        @pl.when(m == 3)
        def _():
            recv(fall.at[:, 1 - c], ff_r)

        @pl.when((m >= 4) & (m < 4 + 6 * DS) & (rem(m, DS) == 0))
        def _():
            q = (m - 4) // DS
            delta(q // 2, rem(q, 2))

        @pl.when(n == 43)
        def _():
            for w in pending:
                w()

        return 0

    lax.fori_loop(0, 44, middle, 0)

    def last(j):
        i = chunk(j)
        pp = part(z, i)
        recv(rcv.at[6, i], rs_r.at[6, i])
        return pp + rcv[6, i].astype(F32)

    def last_far(j, _):
        fsnd[j] = last(j).astype(BF)
        rc(fsnd.at[j], fin.at[j], fs_s.at[j], fs_r.at[j], ypart).start()

        return 0

    lax.fori_loop(0, 4, last_far, 0)
    lax.fori_loop(44, 48, middle, 0)

    def put(j, h, w):
        for m in range(2):
            out_ref[2 * j + m, pl.ds(pl.multiple_of(160 * h, 16), 160)] = w[:, 128 * m : 128 * (m + 1)].astype(BF)

    def last_near(j, _):
        put(j, yh, last(j + 4) + nbuf[yh, j])
        return 0

    lax.fori_loop(0, 4, last_near, 0)

    def finish(j, _):
        rc(fsnd.at[j], fin.at[j], fs_s.at[j], fs_r.at[j], ypart).wait()
        put(j, 1 - yh, fin[j].astype(F32) + nbuf[1 - yh, j])
        return 0

    lax.fori_loop(0, 4, finish, 0)

    def drain(i, _):
        rsend(6, i, snd.at[i]).wait_send()
        return 0

    lax.fori_loop(0, 8, drain, 0)


def call_step(*arrays):
    arrays = [pltpu.with_memory_space_constraint(v, pltpu.HBM) for v in arrays]
    v = pl.BlockSpec(memory_space=pltpu.VMEM)
    a = pl.BlockSpec(memory_space=pltpu.HBM)
    dma = pltpu.SemaphoreType.DMA
    vm = pltpu.VMEM
    return pl.pallas_call(
        step_kernel,
        out_shape=[
            jax.ShapeDtypeStruct((8, 320, 128), BF),
            jax.ShapeDtypeStruct((3, 320, FB), BF),
        ],
        in_specs=[a] * 8,
        out_specs=[v, v],
        scratch_shapes=[
            pltpu.SMEM((8,), jnp.int32), pltpu.SMEM((8,), F32),
            vm((320, 128), BF), vm((2, 320, FB), BF), vm((2, 160, FB), BF), vm((16, 3, 4, D), BF), vm((16, 3, 4, FB), BF),
            vm((3, 32, D), BF), vm((3, 2, 8, 32, FB), BF), vm((2, 3, 32, FB), BF),
            vm((2, 8, 160, FB), BF), vm((8, 2, FB, 256), BF), vm((8, 160, 256), BF),
            vm((7, 8, 160, 256), BF), vm((4, 160, 256), BF), vm((4, 160, 256), BF),
            vm((896, 128), BF), vm((896, 128), BF), vm((896, 128), F32), vm((2, 4, 112, 128), BF),
            vm((4, 2, 112, 128), BF), vm((112, 128), BF), vm((112, 128), BF), vm((2, 2, 896, 192), BF), vm((8, 2, 192, 256), BF),
            vm((128, 384), BF), vm((2, 8, 16, 384), BF), vm((16, 128), BF), vm((2, 128, 128), BF),
            vm((2, 2, 32, 128), F32),
            vm((3, 32, 128), BF), vm((3, 32, 128), BF), vm((32, 128), F32), vm((3, 2, 8, 32, 640), BF),
            vm((2, 8, 8, 128), F32), vm((2, 8, 32, 128), F32), vm((3, 384, 512), BF), vm((384, 32), BF), vm((2, 4, 160, 256), F32), vm((16, 32, 384), BF),
            dma((8,)), dma(()), dma(()), dma((8,)), dma((8,)), dma((4,)), dma((4,)), dma((4, 4)), dma((4, 4)), dma(()), dma(()),
            dma((8,)), dma((8,)), dma((16,)), dma((16,)),
            dma((3,)), dma((3,)), dma((2,)), dma((2,)), dma((2, 2)), dma((2, 2)), dma((2,)), dma((2, 2, 2)), dma((4, 2, 2)), dma((4, 2, 2)),
            dma((4, 2, 2)), dma((4, 2, 2)), dma((7, 8)), dma((7, 8)), dma((4,)), dma((4,)),
            dma((8,)), dma((8,)), dma((8,)), dma((8,)), dma(()), dma(()), dma((16,)), dma((16,)),
            dma((16,)), dma((16,)),
        ],
        compiler_params=pltpu.CompilerParams(
            collective_id=0, has_side_effects=True, vmem_limit_bytes=44 << 20
        ),
        name="es_step",
    )(*arrays)


EMIT_LIM = 4 << 20


def emit_kernel(out, deltas, o_hbm, g_hbm, u_hbm, d_hbm, sems):
    pairs = [(deltas.at[0], g_hbm), (deltas.at[1], u_hbm), (deltas.at[2], d_hbm), (out, o_hbm)]
    copies = [pltpu.make_async_copy(a, b, sems.at[i]) for i, (a, b) in enumerate(pairs)]
    for d in copies:
        d.start()
    for d in copies:
        d.wait()


def emit(out, deltas):
    v = pl.BlockSpec(memory_space=pltpu.VMEM)
    a = pl.BlockSpec(memory_space=pltpu.HBM)
    one = jax.ShapeDtypeStruct((320, FB), BF)
    return pl.pallas_call(
        emit_kernel,
        out_shape=[jax.ShapeDtypeStruct((8, 320, 128), BF), one, one, one],
        in_specs=[v, v],
        out_specs=[a, a, a, a],
        scratch_shapes=[pltpu.SemaphoreType.DMA((4,))],
        compiler_params=pltpu.CompilerParams(vmem_limit_bytes=EMIT_LIM),
        name="emit",
    )(out, deltas)


def shards(prompt_acts, gate_weight, up_weight, down_weight, d_table, f_table, seeds, fitness):
    out, deltas = call_step(
        prompt_acts.T, gate_weight, up_weight, down_weight.T.reshape(2, 160, FB), d_table, f_table,
        seeds, fitness,
    )
    out, dg, du, dd = emit(out, deltas)
    return out.transpose(0, 2, 1), dg, du, dd.T


def solution(mesh):
    split = Mesh(mesh.devices.reshape(4, 2, 2, 8, 2), AX)
    placed = (
        P(None, MEMBER), P(MEMBER, TENSOR), P(MEMBER, TENSOR), P(TENSOR, MEMBER),
        P(MEMBER, None, None, None), P(MEMBER, None, None, TENSOR), P(MEMBER), P(MEMBER),
    )
    return jax.shard_map(
        shards, mesh=split, in_specs=placed,
        out_specs=(P(MEMBER, None, TENSOR), P(MEMBER, TENSOR), P(MEMBER, TENSOR), P(TENSOR, MEMBER)),
        check_vma=False,
    )
```

```python
import functools
import math

import jax
import jax.numpy as jnp
from jax import lax
from jax.experimental import pallas as pl
from jax.experimental.pallas import tpu as pltpu
from jax.sharding import Mesh
from jax.sharding import PartitionSpec as P

D = 5120
FFW = 13824
FB = 864
AX = ("x", "yh", "c", "z", "yl")
MEMBER = ("x", "yh", "c")
TENSOR = ("z", "yl")
MESH = pl.DeviceIdType.MESH
BF = jnp.bfloat16
F32 = jnp.float32
HR = 864
HU = 1
LEAD = 1
BG = 1
TB = 0
TB2 = 2
TF = 5
TF2 = 6
FX = 17
PN = 4
NI = 32
CF = 35
DX = 33
CD = 38
DS = 1
ORDER = (
    "y_second",
    "y_first",
    "y_first_b",
    "base_half",
    "y_second_b",
    "base_scatter",
    "prompt_out",
    "base_mid",
    "x_first",
    "base_sum",
    "x_first_b",
    "local_rows",
    "factors_far",
    "factors_diag",
    "prompt_on",
    "take_first",
    "base_on",
    "factors_near",
    "take_first_b",
    "x_second",
    "project",
    "factors_near_in",
    "x_second_b",
    "factors_far_in",
    "base_end",
    "take_first_far",
    "project_in",
    "base_other",
    "down_out",
    "hidden_ahead",
    "first_in",
)


def rem(a, n):
    return lax.rem(a, n)


def at(x, yh, c, z, yl):
    return {"x": x, "yh": yh, "c": c, "z": z, "yl": yl}


def tn(a, b):
    return lax.dot_general(a, b, (((0,), (0,)), ((), ())), preferred_element_type=F32)


def nt(a, b):
    return lax.dot_general(a, b, (((1,), (1,)), ((), ())), preferred_element_type=F32)


def nn(a, b):
    return jnp.dot(a, b, preferred_element_type=F32)


def step_kernel(
    pt_hbm, gw_hbm, uw_hbm, dt_hbm, dtab_hbm, ftab_hbm, seeds_hbm, fit_hbm,
    out_ref, del_ref,
    seeds, fit, pt_v, w_v, dt_v, dtab, ftab, dk, fall, foth, dbuf, hbuf, snd, rcv, fin, fsnd,
    bsend, brecv, bown, ps, rsb, rsend2, rrecv2, lhs, rhs, psh, prb, pjs, pjb, ptt,
    pdc, pdb, pdt, dall, fitall, score, wt, a2t, nbuf, wbuf,
    in_s, bx_s, bx_r, r1_s, r1_r, ag_s, ag_r, ah_s, ah_r, bf_s, bf_r, pr_s, pr_r, pj_s, pj_r,
    ft_s, ft_r, ft2_s, ft2_r, ys, yr, yloc, xo_s, xf_s, x_r, ds_s, ds_r, rs_s, rs_r, fs_s, fs_r,
    pd_s, pd_r, f_s, f_r, ff_s, ff_r, d_s, d_r, q_s, q_r,
):
    x, yh, c, z, yl = [lax.axis_index(a) for a in AX]
    y = 2 * yh + yl
    p = 2 * x + yh
    me = at(x, yh, c, z, yl)
    partner = at(x, yh, 1 - c, z, yl)
    ypart = at(x, 1 - yh, c, z, yl)
    pending = []

    def rc(src, dst, ss, rs, dev):
        return pltpu.make_async_remote_copy(
            src_ref=src, dst_ref=dst, send_sem=ss, recv_sem=rs, device_id=dev, device_id_type=MESH
        )

    def send(src, dst, ss, rs, dev):
        d = rc(src, dst, ss, rs, dev)
        d.start()
        pending.append(d.wait_send)

    def recv(dst, rs):
        rc(dst, dst, rs, rs, partner).wait_recv()

    loads = [
        (gw_hbm, w_v.at[0]), (uw_hbm, w_v.at[1]), (pt_hbm, pt_v), (ftab_hbm, ftab), (dtab_hbm, dtab),
        (dt_hbm, dt_v), (seeds_hbm, seeds), (fit_hbm, fit),
    ]
    loads = [pltpu.make_async_copy(a, b, in_s.at[i]) for i, (a, b) in enumerate(loads)]
    for i in (5, 2, 0, 1, 6, 7, 3, 4):
        loads[i].start()

    def plane(rel):
        ny = rem(y + rel % 4, 4)
        return at(rem(x + rel // 4, 4), ny // 2, c, z, rem(ny, 2))

    def mate(rel):
        q = rem(p + rel // 2, 8)
        return at(q // 2, rem(q, 2), rem(c + rel % 2, 2), z, yl)

    def column(rel):
        return at(x, rem(yh + rel // 8, 2), c, rem(z + rel % 8, 8), yl)

    ypeers = [at(x, h, yl, z, c) for h in range(2)]
    me_y = [(h == yh) & (c == yl) for h in range(2)]
    barrier = pltpu.get_barrier_semaphore()

    def greet(dev):
        pl.semaphore_signal(barrier, inc=1, device_id=dev, device_id_type=MESH)

    peers = [column(r) for r in (4, 12, 3, 5, 11, 13, 2, 6, 10, 14, 1, 7, 9, 15)]
    peers += [mate(r) for r in range(15, 0, -1)] + [plane(1), plane(3)]
    for o in peers:
        greet(o)
    @pl.when(c != yl)
    def _():
        for h in range(2):
            greet(ypeers[h])

    def partial_base(k):
        return tn(w_v[k], pt_v[...])

    for i in (0, 1, 2, 5):
        loads[i].wait()
    bsend[pl.ds(0, FB)] = partial_base(1 - c).astype(BF)
    bsend[pl.ds(FB, 32)] = jnp.zeros((32, 128), BF)
    n_peers = len(peers)
    @pl.when(c == yl)
    def _():
        pl.semaphore_wait(barrier, n_peers)

    @pl.when(c != yl)
    def _():
        pl.semaphore_wait(barrier, n_peers + 2)

    e, kz = rem(z, 2), z // 2

    def low(x0):
        m = rem(x0 - kz + 4, 4)
        return jnp.where(e == 0, jnp.where(m == 1, 0, 1), jnp.where(m == 3, 1, 0))

    def zblk(r, ab):
        x0 = rem(x - r + 4, 4)
        return 2 * x0 + (low(x0) if ab == 0 else 1 - low(x0))

    own_a = low(x)

    def half(b, part):
        return b.at[pl.ds(80 * part, 80)]

    def ycopy(h, part):
        dst = half(dbuf.at[yl, 2 * x + yh], part)
        return rc(half(dt_v.at[h], part), dst, ys.at[h, part], yr.at[yh, part], ypeers[h])

    def ylocal(h, part):
        return pltpu.make_async_copy(half(dt_hbm.at[h], part), half(dbuf.at[yl, 2 * x + yh], part), yloc.at[part])

    def ysend(ab, part):
        mine = yh == (own_a if ab == 0 else 1 - own_a)
        for h in range(2):
            @pl.when(mine & jnp.logical_not(me_y[h]))
            def _():
                ycopy(h, part).start()
            @pl.when(mine & me_y[h])
            def _():
                ylocal(h, part).start()

    def wait_y(ab, part):
        w = own_a if ab == 0 else 1 - own_a
        here = (w == yh) & (c == yl)

        @pl.when(jnp.logical_not(here))
        def _():
            recv(half(dbuf.at[c, 2 * x + w], part), yr.at[w, part])

        @pl.when(here)
        def _():
            ylocal(0, part).wait()

    def y_drain():
        for h in range(2):
            @pl.when(jnp.logical_not(me_y[h]))
            def _():
                for part in range(2):
                    ycopy(h, part).wait_send()

    pending.append(y_drain)
    xnb = [at(rem(x + 1, 4), yh, c, z, yl), at(rem(x + 3, 4), yh, c, z, yl)]

    def dsend(r, ab, part):
        b = half(dbuf.at[c, zblk(r, ab)], part)
        d = rc(b, b, ds_s.at[r, ab, part], ds_r.at[r, ab, part], partner)
        pending.append(d.wait_send)
        return d

    def own_x(ab, part):
        b = dbuf.at[c, zblk(0, ab)]
        dsend(0, ab, part).start()
        b = half(b, part)
        send(b, b, xo_s.at[0, ab, part], x_r.at[1, ab, part], xnb[0])
        send(b, b, xo_s.at[1, ab, part], x_r.at[3, ab, part], xnb[1])

    def taker(r, ab):
        b = dbuf.at[c, zblk(r, ab)]
        d2 = [dsend(r, ab, part) for part in range(2)]
        fwd = c == (0 if r == 1 else 1)
        hops = []
        for part in range(2 if r != 2 else 0):
            h = half(b, part)
            d = rc(h, h, xf_s.at[r, ab, part], x_r.at[2, ab, part], xnb[0 if r == 1 else 1])
            hops.append(d)
            pending.append(functools.partial(pl.when(fwd), d.wait_send))

        def run(part):
            recv(half(b, part), x_r.at[r, ab, part])
            if r != 2:
                pl.when(fwd)(hops[part].start)
            d2[part].start()

        return run

    take = {(r, ab): taker(r, ab) for r in (1, 3, 2) for ab in range(2)}

    def take_d(r, ab):
        for part in range(2):
            recv(half(dbuf.at[1 - c, zblk(r, ab)], part), ds_r.at[r, ab, part])

    toks = pl.ds(pl.multiple_of(16 * z, 16), 16)
    own_row = 4 * yh + x
    def bpiece(t, k, first, rows):
        return lhs.at[t, k, pl.ds(pl.multiple_of(112 * first, 16), rows), pl.ds(0, 128)]

    along_x = [at(rem(x + r, 4), yh, c, z, yl) for r in range(4)]
    along_y = [at(x, rem(y + r, 4) // 2, c, z, rem(y + r, 2)) for r in range(4)]
    stage1, stage2, got1, got2 = [], [], [], []
    for r in range(1, 4):
        b = bpiece(yl, c, own_row, 112)
        stage1.append((rc(b, b, ag_s.at[r], ag_r.at[r], along_x[r]), rc(b, b, ag_s.at[r], ag_r.at[r], along_y[r])))
        xx, yy = rem(x - r + 4, 4), rem(y - r + 4, 4)
        got1.append((bpiece(yl, c, 4 * yh + xx, 112), bpiece(rem(yy, 2), c, 4 * (yy // 2) + x, 112)))
        b = bpiece(yl, c, 4 * yh, 448)
        far = []
        for n in range(4):
            f = bpiece(n // 2, c, 4 * (n % 2) + x, 112)
            far.append(rc(f, f, ah_s.at[r, n], ah_r.at[r, n], along_x[r]))
        stage2.append(([rc(b, b, ah_s.at[r, 0], ah_r.at[r, 0], along_y[r])], far))
        got2.append((
            [bpiece(rem(yy, 2), c, 4 * (yy // 2), 448)],
            [bpiece(n // 2, c, 4 * (n % 2) + xx, 112) for n in range(4)],
        ))

    def by_core(f):
        for core in range(2):
            @pl.when(c == core)
            def _():
                f(core)

    def ag_one(core):
        for d in stage1:
            d[core].start()

    def ag_two(core):
        for g, r in zip(got1, range(1, 4)):
            recv(g[core], ag_r.at[r])
        for ds in stage2:
            for d in ds[core]:
                d.start()

    def ag_end(core):
        for g, r in zip(got2, range(1, 4)):
            for n, b in enumerate(g[core]):
                recv(b, ah_r.at[r, n])

    def ag_drain(core):
        for d in stage1:
            d[core].wait_send()
        for ds in stage2:
            for d in ds[core]:
                d.wait_send()

    pending.append(lambda: by_core(ag_drain))
    fteam = [(1, 0), (1, 1), (0, 1)]

    def fdev(i):
        dh, dl = fteam[i]
        return at(x, rem(yh + dh, 2), c, z, rem(yl + dl, 2))

    def fdst(i, ks):
        return fall.at[ks, c, p] if fteam[i][1] == 0 else foth.at[yh, ks]

    def frcv(i, ks):
        dh, dl = fteam[i]
        return fall.at[ks, c, p + 1 - 2 * yh] if dl == 0 else foth.at[rem(yh + dh, 2), ks]

    gu, down = pl.ds(0, 2), pl.ds(2, 1)
    def factors_in(own, where):
        for i in where:
            recv(frcv(i, gu), ft_r.at[i])
        g = yh if own else 1 - yh
        for k in range(2):
            lanes = pl.ds(160 if own else 128, 32)
            lhs[yl, k, pl.ds(0, FB), lanes] = fall[k, c, 2 * x + g].T
            lhs[1 - yl, k, pl.ds(0, FB), lanes] = foth[g, k].T

    rowm = lax.broadcasted_iota(jnp.int32, (32, 256), 0) // 4
    lanem = lax.broadcasted_iota(jnp.int32, (32, 256), 1) // 128

    def hidden_rows():
        for i in range(8):
            g, cc = i // 4, i % 4
            for k in range(2):
                for gg in range(2):
                    of = yh if gg == 1 else 1 - yh
                    v = jnp.concatenate([ptt[of, k]] * 2, axis=1)
                    live = (rowm == 2 * cc + lanem) & (g == of)
                    rhs[i, k, pl.ds(128 + 32 * gg, 32)] = jnp.where(live, v, 0.0).astype(BF)

    def hidden(i):
        def rows(rb, _):
            r = pl.ds(pl.multiple_of(rb * HR, 16), HR)
            for t in range(2):
                ga = nn(lhs[t, 0, r], rhs[i, 0])
                up = nn(lhs[t, 1, r], rhs[i, 1])
                hbuf[i, t, r] = ((ga + ga * jnp.tanh(ga)) * up).astype(BF)
            return 0

        lax.fori_loop(0, FB // HR, rows, 0, unroll=HU)

    def chunk(j):
        return rem(j + 4 * (1 - yh), 8)

    sgn = 1 - 2 * c
    zn = rem(z + sgn + 8, 8)
    znd = at(x, yh, c, zn, yl)

    def part(d, i):
        return nn(dbuf[0, d], hbuf[i, 0]) + nn(dbuf[1, d], hbuf[i, 1])

    d0 = rem(z - sgn + 8, 8)

    def rsend(s, i, src):
        return rc(src, rcv.at[s, i], rs_s.at[s, i], rs_r.at[s, i], znd)


    def local_rows():
        for i in (6, 7, 3):
            loads[i].wait()
        for k in range(3):
            for m in range(8):
                fall[k, c, p, pl.ds(4 * m, 4)] = ftab[seeds[m], k]
        loads[4].wait()
        for k in range(3):
            for m in range(8):
                dk[k, pl.ds(4 * m, 4)] = dtab[seeds[m], k]

        eye = lax.broadcasted_iota(jnp.int32, (128, 256), 0) == rem(lax.broadcasted_iota(jnp.int32, (128, 256), 1), 128)
        for k in range(2):
            for i in range(8):
                rhs[i, k, 0:128] = jnp.where(eye, 1.0, 0.0).astype(BF)
            for t in range(2):
                lhs[t, k, :, pl.ds(128, 64)] = jnp.zeros((896, 64), BF)

    def base_half():
        send(bsend, brecv, bx_s, bx_r, partner)

    def base_scatter():
        bown[pl.ds(0, FB)] = partial_base(c)
        bown[pl.ds(FB, 32)] = jnp.zeros((32, 128), F32)
        recv(brecv, bx_r)
        for q in range(8):
            rows = pl.ds(112 * q, 112)
            ps[q // 4, q % 4] = (bown[rows] + brecv[rows].astype(F32)).astype(BF)
        for r in range(1, 4):
            xx = rem(x + r, 4)
            send(ps.at[:, xx], rsb.at[r], r1_s.at[r], r1_r.at[r], at(xx, yh, c, z, yl))

    def own_sum(h):
        mid = pl.ds(pl.multiple_of(112 * (4 * h + x), 16), 112)
        s = bown[mid] + brecv[mid].astype(F32)
        for r in range(1, 4):
            s += rsb[r, h].astype(F32)
        return s

    def base_mid():
        for r in range(1, 4):
            recv(rsb.at[r], r1_r.at[r])
        rsend2[...] = own_sum(1 - yh).astype(BF)
        send(rsend2, rrecv2, r1_s.at[0], r1_r.at[0], ypart)

    def base_sum():
        recv(rrecv2, r1_r.at[0])
        s = own_sum(yh) + rrecv2[...].astype(F32)
        s = jnp.where(c == 0, s * 0.5, s)
        bpiece(yl, c, own_row, 112)[...] = s.astype(BF)
        by_core(ag_one)

    def base_on():
        by_core(ag_two)

    def base_end():
        by_core(ag_end)
        send(lhs.at[:, c, :, pl.ds(0, 128)], lhs.at[:, c, :, pl.ds(0, 128)], bf_s, bf_r, partner)

    def base_other():
        recv(lhs.at[:, 1 - c, :, pl.ds(0, 128)], bf_r)

    def prompt_out():
        ptr = pt_v[...].astype(F32).T.astype(BF)
        psh[...] = jnp.zeros_like(psh)

        @pl.when(c == 0)
        def _():
            psh[:, 0:320] = ptr

        @pl.when(c == 1)
        def _():
            psh[:, 64:384] = ptr

        prb[c, p] = psh[toks]
        for r in range(1, 8):
            send(prb.at[c, p], prb.at[c, p], pr_s.at[r], pr_r.at[r], mate(2 * r))

    def prompt_on():
        for r in range(1, 8):
            recv(prb.at[c, rem(p - r + 8, 8)], pr_r.at[r])
        send(prb.at[c], prb.at[c], pr_s.at[0], pr_r.at[0], partner)

    def project():
        recv(prb.at[1 - c], pr_r.at[0])

        def proj_of(n, acc):
            cc, q = n // 8, rem(n, 8)
            lanes = pl.ds(pl.multiple_of(640 * q + 256 * cc, 128), 384)
            return acc + nt(prb[cc, q], dk[0:2, :, lanes].reshape(64, 384))

        acc = lax.fori_loop(0, 16, proj_of, jnp.zeros((16, 64), F32), unroll=4)
        acc = (acc / math.sqrt(D)).astype(BF).astype(F32)
        kk = lax.broadcasted_iota(jnp.int32, (16, 64), 1) // 32
        acc = jnp.where(kk == 0, acc * 0.25, acc * 0.5)
        pjs[...] = jnp.zeros_like(pjs)
        pjs[:, 0:64] = acc.astype(BF)
        pjb[yh, toks] = pjs[...]
        for r in range(1, 16):
            send(pjs, pjb.at[yh, toks], pj_s.at[r], pj_r.at[r], column(r))


    def project_in():
        for r in range(1, 16):
            hz, zz = rem(yh + r // 8, 2), rem(z - r % 8 + 8, 8)
            recv(pjb.at[hz, pl.ds(pl.multiple_of(16 * zz, 16), 16)], pj_r.at[r])
        for g in range(2):
            ptt[g] = pjb[g].astype(F32).T[0:64].reshape(2, 32, 128)
        hidden_rows()

    def y_first():
        ysend(0, 0)

    def y_first_b():
        ysend(0, 1)

    def y_second():
        ysend(1, 0)

    def y_second_b():
        ysend(1, 1)

    def x_first():
        wait_y(0, 0)
        own_x(0, 0)

    def x_first_b():
        wait_y(0, 1)
        own_x(0, 1)

    def x_second():
        wait_y(1, 0)
        own_x(1, 0)

    def x_second_b():
        wait_y(1, 1)
        own_x(1, 1)

    def down_out():
        send(fall.at[down, c, p], fdst(2, down), ft2_s.at[0], ft2_r.at[0], fdev(2))
        send(fall.at[down, c, p], fdst(0, down), ft2_s.at[1], ft2_r.at[1], fdev(0))

    def take_first():
        take[1, 0](0)
        take[3, 0](0)

    def take_first_b():
        take[1, 0](1)
        take[3, 0](1)

    def take_second():
        take[1, 1](0)
        take[3, 1](0)

    def take_second_b():
        take[1, 1](1)
        take[3, 1](1)

    def take_first_far():
        for part in range(2):
            take[2, 0](part)

    def first_in():
        for r in range(4):
            take_d(r, 0)

    def take_second_far():
        take[2, 1](0)

    def take_second_far_b():
        take[2, 1](1)

    def second_in():
        for r in range(4):
            take_d(r, 1)

    def factors_far():
        send(fall.at[gu, c, p], fdst(0, gu), ft_s.at[0], ft_r.at[0], fdev(0))

    def factors_diag():
        send(fall.at[gu, c, p], fdst(1, gu), ft_s.at[1], ft_r.at[1], fdev(1))

    def factors_near():
        send(fall.at[gu, c, p], fdst(2, gu), ft_s.at[2], ft_r.at[2], fdev(2))

    def factors_far_in():
        factors_in(False, (0, 1))

    def factors_near_in():
        factors_in(True, (2,))

    def hidden_ahead():
        def ahead(j, _):
            hidden(chunk(j))
            return 0

        lax.fori_loop(0, LEAD, ahead, 0)

    steps = dict(
        local_rows=local_rows, down_out=down_out,
        base_half=base_half, base_scatter=base_scatter, base_mid=base_mid, base_sum=base_sum, base_on=base_on, base_end=base_end,
        base_other=base_other, prompt_out=prompt_out, prompt_on=prompt_on, project=project,
        project_in=project_in, y_first=y_first, y_second=y_second, y_first_b=y_first_b, y_second_b=y_second_b, x_first=x_first, x_second=x_second, x_first_b=x_first_b, x_second_b=x_second_b,
        take_first=take_first, take_first_b=take_first_b, take_second_b=take_second_b, take_second=take_second, take_first_far=take_first_far, first_in=first_in,
        factors_far=factors_far, factors_diag=factors_diag, factors_near=factors_near, factors_far_in=factors_far_in,
        factors_near_in=factors_near_in, hidden_ahead=hidden_ahead,
    )
    for name in ORDER:
        steps[name]()

    def step_zero(j):
        i = chunk(j)
        snd[i] = part(d0, i).astype(BF)
        rsend(0, i, snd.at[i]).start()

    def first(j, _):
        i = chunk(j)
        p0 = part(d0, i).astype(BF)
        hidden(chunk(j + 1))
        snd[i] = p0
        rsend(0, i, snd.at[i]).start()
        pl.when(j == TB)(take_second)
        pl.when(j == TB2)(take_second_b)
        if TF <= 6:
            pl.when(j == TF)(take_second_far)
        if TF2 <= 6:
            pl.when(j == TF2)(take_second_far_b)
        return 0

    lax.fori_loop(0, 7, first, 0)
    if TF > 6:
        take_second_far()
    step_zero(7)
    if TF2 > 6:
        take_second_far_b()


    def fpiece(i, other):
        return fall.at[:, c, 2 * rem(x - i + 4, 4) + (1 - yh if other else yh)]

    f_out, f_on = [], []
    for i in range(1, 4):
        f_out.append([rc(fpiece(0, h), fpiece(0, h), f_s.at[4 * h + i], f_r.at[4 * h + i], along_x[i]) for h in range(2)])
        f_on.append(rc(fpiece(i, 0), fpiece(i, 0), f_s.at[4 + i], f_r.at[4 + i], ypart))

    def factors_out(core):
        for d in f_out:
            for h in range(1 + core):
                d[h].start()

    def factors_drain(core):
        for d in f_out:
            for h in range(1 + core):
                d[h].wait_send()
        if core == 0:
            for d in f_on:
                d.wait_send()

    pending.append(lambda: by_core(factors_drain))
    def dlanes(q):
        return pl.ds(pl.multiple_of(640 * q, 128), 640)

    d_out = []
    for r in range(1, 8):
        q = rem(p + r, 8)
        d_out.append(rc(dk.at[:, :, dlanes(q)], dall.at[:, c, p], d_s.at[r], d_r.at[r], mate(2 * r)))
        d_out.append(rc(fitall.at[c, p], fitall.at[c, p], q_s.at[r], q_r.at[r], mate(2 * r)))
    pending.extend(d.wait_send for d in d_out)

    def background():
        recv(frcv(0, down), ft2_r.at[1])
        by_core(factors_out)
        for m in range(8):
            fitall[c, p, pl.ds(m, 1)] = jnp.full((1, 128), fit[m], F32)
        dall[:, c, p] = dk[:, :, dlanes(p)]
        for d in d_out:
            d.start()

    second_in()

    fwd_f = rc(fall.at[:, c], fall.at[:, c], ff_s, ff_r, partner)
    pending.append(fwd_f.wait_send)

    def factors_on():
        @pl.when(c == 0)
        def _():
            for i in range(1, 4):
                recv(fpiece(i, 0), f_r.at[i])
            for d in f_on:
                d.start()

    def collect_f():
        @pl.when(c == 1)
        def _():
            for i in range(1, 4):
                recv(fpiece(i, 0), f_r.at[i])

        for i in range(1, 4):
            recv(fpiece(i, 1), f_r.at[4 + i])
        fwd_f.start()

    d_on = rc(dall.at[:, c], dall.at[:, c], d_s.at[0], d_r.at[0], partner)
    q_on = rc(fitall.at[c], fitall.at[c], q_s.at[0], q_r.at[0], partner)
    pending.extend([d_on.wait_send, q_on.wait_send])

    def factors_d_on():
        for r in range(1, 8):
            q = rem(p - r + 8, 8)
            recv(dall.at[:, c, q], d_r.at[r])
            recv(fitall.at[c, q], q_r.at[r])
        d_on.start()
        q_on.start()

    def collect_d():
        recv(dall.at[:, 1 - c], d_r.at[0])
        recv(fitall.at[1 - c], q_r.at[0])
        fv = fitall[...].reshape(128, 128)
        mean = jnp.sum(fv, axis=0, keepdims=True) / 128
        spread = jnp.sum((fv - mean) ** 2, axis=0, keepdims=True) / 128
        sc = (fv - mean) / jnp.sqrt(spread + 1.0)
        for i in range(16):
            v = jnp.broadcast_to(sc[8 * i : 8 * i + 8].reshape(8, 1, 128), (8, 4, 128))
            score[i // 8, i % 8] = v.reshape(32, 128)

    def weigh(k):
        def one(g, _):
            a, b = g // 8, rem(g, 8)
            sc = score[a, b]
            own = pl.ds(pl.multiple_of(256 * c, 128), 384)
            w = dall[k, a, b, :, own].astype(F32) * jnp.concatenate([sc] * 3, axis=1)
            wbuf[g] = w.astype(BF)
            return 0
        lax.fori_loop(0, 16, one, 0)
        wt[k] = wbuf[...].reshape(512, 384).T

    def delta(k, half):
        r = pl.ds(pl.multiple_of(64 * c + 160 * half, 16), 160)
        v = nn(wt[k, r], fall[k].reshape(512, FB)) * (1.0 / math.sqrt(512))
        del_ref[k, pl.ds(pl.multiple_of(160 * half, 16), 160)] = v.astype(BF)

    flips = [z + 1 - 2 * rem(z, 2), z + 2 - 4 * rem(z // 2, 2), z + 4 - 8 * (z // 4)]
    pd_out = [rc(pdc.at[k], pdb.at[k], pd_s.at[k], pd_r.at[k], at(x, yh, c, f, yl)) for k, f in enumerate(flips)]
    pending.extend(d.wait_send for d in pd_out)

    def down_sum(k):
        recv(pdb.at[k], pd_r.at[k])
        tot = pdc[k].astype(F32) + pdb[k].astype(F32)
        pdc[k + 1] = tot.astype(BF)
        pd_out[k + 1].start()

    def down_sums():
        recv(frcv(2, down), ft2_r.at[0])
        tot = jnp.zeros((32, 128), F32)
        for cc in range(4):
            i = 4 * yh + cc
            q = nn(fall[2, c, p], hbuf[i, yl]) + nn(foth[yh, 2], hbuf[i, 1 - yl])
            q = jnp.where(rowm == 2 * cc + lanem, q, 0.0)
            tot += q[:, :128] + q[:, 128:]
        pdc[0] = tot.astype(BF)
        pd_out[0].start()


    def noise_in():
        recv(pdb.at[2], pd_r.at[2])
        tot = pdc[2].astype(F32) + pdb[2].astype(F32)
        pdt[...] = (tot / math.sqrt(FFW)).astype(BF).astype(F32) * 0.5
        a2t[...] = dk[2, :, pl.ds(pl.multiple_of(640 * z + 256 * yl, 128), 384)].T

    def noise(j):
        live = rowm == 2 * j + lanem
        pm = jnp.where(live, jnp.concatenate([pdt[...]] * 2, axis=1), 0.0).astype(BF)
        for h in range(2):
            nbuf[h, j] = nn(a2t[pl.ds(pl.multiple_of(64 * yl + 160 * h, 16), 160)], pm)

    def place(n):
        m = n - 12
        late = jnp.where(rem(m + 16, 8) >= 4, 1, 0)
        s = jnp.where(n < 8, 1, jnp.where(n < 12, 2, jnp.where(n < 44, 3 + m // 8 - late, 6)))
        j = jnp.where(n < 8, n, jnp.where(n < 12, n - 8, jnp.where(n < 44, rem(m + 16, 8), n - 40)))
        return s, j

    def middle(n, _):
        s, j = place(n)
        i = chunk(j)
        pp = part(rem(z - sgn * (1 + s) + 16, 8), i)
        recv(rcv.at[s - 1, i], rs_r.at[s - 1, i])
        rcv[s - 1, i] = (pp + rcv[s - 1, i].astype(F32)).astype(BF)
        rsend(s, i, rcv.at[s - 1, i]).start()
        rsend(s - 1, i, rcv.at[s, i]).wait_send()

        @pl.when(n == BG)
        def _():
            background()

        @pl.when(n == PN)
        def _():
            down_sums()

        for k in range(2):
            pl.when(n == PN + 8 * (k + 1))(functools.partial(down_sum, k))

        @pl.when(n == NI)
        def _():
            noise_in()

        @pl.when((n > NI) & (n <= NI + 4))
        def _():
            noise(n - NI - 1)

        @pl.when(n == FX)
        def _():
            factors_on()

        @pl.when(n == CF)
        def _():
            collect_f()

        @pl.when(n == DX)
        def _():
            factors_d_on()

        m = n - CD

        @pl.when(m == 0)
        def _():
            collect_d()

        @pl.when((m >= 1) & (m < 4))
        def _():
            weigh(m - 1)

        @pl.when(m == 3)
        def _():
            recv(fall.at[:, 1 - c], ff_r)

        @pl.when((m >= 4) & (m < 4 + 6 * DS) & (rem(m, DS) == 0))
        def _():
            q = (m - 4) // DS
            delta(q // 2, rem(q, 2))

        @pl.when(n == 43)
        def _():
            for w in pending:
                w()

        return 0

    lax.fori_loop(0, 44, middle, 0)

    def last(j):
        i = chunk(j)
        pp = part(z, i)
        recv(rcv.at[6, i], rs_r.at[6, i])
        return pp + rcv[6, i].astype(F32)

    def last_far(j, _):
        fsnd[j] = last(j).astype(BF)
        rc(fsnd.at[j], fin.at[j], fs_s.at[j], fs_r.at[j], ypart).start()

        return 0

    lax.fori_loop(0, 4, last_far, 0)
    lax.fori_loop(44, 48, middle, 0)

    def put(j, h, w):
        for m in range(2):
            out_ref[2 * j + m, pl.ds(pl.multiple_of(160 * h, 16), 160)] = w[:, 128 * m : 128 * (m + 1)].astype(BF)

    def last_near(j, _):
        put(j, yh, last(j + 4) + nbuf[yh, j])
        return 0

    lax.fori_loop(0, 4, last_near, 0)

    def finish(j, _):
        rc(fsnd.at[j], fin.at[j], fs_s.at[j], fs_r.at[j], ypart).wait()
        put(j, 1 - yh, fin[j].astype(F32) + nbuf[1 - yh, j])
        return 0

    lax.fori_loop(0, 4, finish, 0)

    def drain(i, _):
        rsend(6, i, snd.at[i]).wait_send()
        return 0

    lax.fori_loop(0, 8, drain, 0)


def call_step(*arrays):
    arrays = [pltpu.with_memory_space_constraint(v, pltpu.HBM) for v in arrays]
    v = pl.BlockSpec(memory_space=pltpu.VMEM)
    a = pl.BlockSpec(memory_space=pltpu.HBM)
    dma = pltpu.SemaphoreType.DMA
    vm = pltpu.VMEM
    return pl.pallas_call(
        step_kernel,
        out_shape=[
            jax.ShapeDtypeStruct((8, 320, 128), BF),
            jax.ShapeDtypeStruct((3, 320, FB), BF),
        ],
        in_specs=[a] * 8,
        out_specs=[v, v],
        scratch_shapes=[
            pltpu.SMEM((8,), jnp.int32), pltpu.SMEM((8,), F32),
            vm((320, 128), BF), vm((2, 320, FB), BF), vm((2, 160, FB), BF), vm((16, 3, 4, D), BF), vm((16, 3, 4, FB), BF),
            vm((3, 32, D), BF), vm((3, 2, 8, 32, FB), BF), vm((2, 3, 32, FB), BF),
            vm((2, 8, 160, FB), BF), vm((8, 2, FB, 256), BF), vm((8, 160, 256), BF),
            vm((7, 8, 160, 256), BF), vm((4, 160, 256), BF), vm((4, 160, 256), BF),
            vm((896, 128), BF), vm((896, 128), BF), vm((896, 128), F32), vm((2, 4, 112, 128), BF),
            vm((4, 2, 112, 128), BF), vm((112, 128), BF), vm((112, 128), BF), vm((2, 2, 896, 192), BF), vm((8, 2, 192, 256), BF),
            vm((128, 384), BF), vm((2, 8, 16, 384), BF), vm((16, 128), BF), vm((2, 128, 128), BF),
            vm((2, 2, 32, 128), F32),
            vm((3, 32, 128), BF), vm((3, 32, 128), BF), vm((32, 128), F32), vm((3, 2, 8, 32, 640), BF),
            vm((2, 8, 8, 128), F32), vm((2, 8, 32, 128), F32), vm((3, 384, 512), BF), vm((384, 32), BF), vm((2, 4, 160, 256), F32), vm((16, 32, 384), BF),
            dma((8,)), dma(()), dma(()), dma((8,)), dma((8,)), dma((4,)), dma((4,)), dma((4, 4)), dma((4, 4)), dma(()), dma(()),
            dma((8,)), dma((8,)), dma((16,)), dma((16,)),
            dma((3,)), dma((3,)), dma((2,)), dma((2,)), dma((2, 2)), dma((2, 2)), dma((2,)), dma((2, 2, 2)), dma((4, 2, 2)), dma((4, 2, 2)),
            dma((4, 2, 2)), dma((4, 2, 2)), dma((7, 8)), dma((7, 8)), dma((4,)), dma((4,)),
            dma((8,)), dma((8,)), dma((8,)), dma((8,)), dma(()), dma(()), dma((16,)), dma((16,)),
            dma((16,)), dma((16,)),
        ],
        compiler_params=pltpu.CompilerParams(
            collective_id=0, has_side_effects=True, vmem_limit_bytes=44 << 20
        ),
        name="es_step",
    )(*arrays)


EMIT_LIM = 4 << 20


def emit_kernel(out, deltas, o_hbm, g_hbm, u_hbm, d_hbm, sems):
    pairs = [(deltas.at[0], g_hbm), (deltas.at[1], u_hbm), (deltas.at[2], d_hbm), (out, o_hbm)]
    copies = [pltpu.make_async_copy(a, b, sems.at[i]) for i, (a, b) in enumerate(pairs)]
    for d in copies:
        d.start()
    for d in copies:
        d.wait()


def emit(out, deltas):
    v = pl.BlockSpec(memory_space=pltpu.VMEM)
    a = pl.BlockSpec(memory_space=pltpu.HBM)
    one = jax.ShapeDtypeStruct((320, FB), BF)
    return pl.pallas_call(
        emit_kernel,
        out_shape=[jax.ShapeDtypeStruct((8, 320, 128), BF), one, one, one],
        in_specs=[v, v],
        out_specs=[a, a, a, a],
        scratch_shapes=[pltpu.SemaphoreType.DMA((4,))],
        compiler_params=pltpu.CompilerParams(vmem_limit_bytes=EMIT_LIM),
        name="emit",
    )(out, deltas)


def shards(prompt_acts, gate_weight, up_weight, down_weight, d_table, f_table, seeds, fitness):
    out, deltas = call_step(
        prompt_acts.T, gate_weight, up_weight, down_weight.T.reshape(2, 160, FB), d_table, f_table,
        seeds, fitness,
    )
    out, dg, du, dd = emit(out, deltas)
    return out.transpose(0, 2, 1), dg, du, dd.T


def solution(mesh):
    split = Mesh(mesh.devices.reshape(4, 2, 2, 8, 2), AX)
    placed = (
        P(None, MEMBER), P(MEMBER, TENSOR), P(MEMBER, TENSOR), P(TENSOR, MEMBER),
        P(MEMBER, None, None, None), P(MEMBER, None, None, TENSOR), P(MEMBER), P(MEMBER),
    )
    return jax.shard_map(
        shards, mesh=split, in_specs=placed,
        out_specs=(P(MEMBER, None, TENSOR), P(MEMBER, TENSOR), P(MEMBER, TENSOR), P(TENSOR, MEMBER)),
        check_vma=False,
    )
```

```python
import functools
import math

import jax
import jax.numpy as jnp
from jax import lax
from jax.experimental import pallas as pl
from jax.experimental.pallas import tpu as pltpu
from jax.sharding import Mesh
from jax.sharding import PartitionSpec as P

D = 5120
FFW = 13824
FB = 864
AX = ("x", "yh", "c", "z", "yl")
MEMBER = ("x", "yh", "c")
TENSOR = ("z", "yl")
MESH = pl.DeviceIdType.MESH
BF = jnp.bfloat16
F32 = jnp.float32
HR = 864
HU = 1
LEAD = 1
TB = 0
TB2 = 2
TF = 5
TF2 = 6
FX = 17
PN = 4
NI = 32
CF = 35
DX = 33
CD = 38
DS = 1
ORDER = (
    "y_second",
    "y_first",
    "y_first_b",
    "base_half",
    "y_second_b",
    "base_scatter",
    "prompt_out",
    "base_mid",
    "x_first",
    "base_sum",
    "x_first_b",
    "local_rows",
    "factors_far",
    "factors_diag",
    "prompt_on",
    "take_first",
    "base_on",
    "factors_near",
    "take_first_b",
    "x_second",
    "project",
    "factors_near_in",
    "x_second_b",
    "factors_far_in",
    "base_end",
    "take_first_far",
    "project_in",
    "base_other",
    "down_out",
    "hidden_ahead",
    "first_in",
)


def rem(a, n):
    return lax.rem(a, n)


def at(x, yh, c, z, yl):
    return {"x": x, "yh": yh, "c": c, "z": z, "yl": yl}


def tn(a, b):
    return lax.dot_general(a, b, (((0,), (0,)), ((), ())), preferred_element_type=F32)


def nt(a, b):
    return lax.dot_general(a, b, (((1,), (1,)), ((), ())), preferred_element_type=F32)


def nn(a, b):
    return jnp.dot(a, b, preferred_element_type=F32)


def step_kernel(
    pt_hbm, gw_hbm, uw_hbm, dt_hbm, dtab_hbm, ftab_hbm, seeds_hbm, fit_hbm,
    out_ref, del_ref,
    seeds, fit, pt_v, w_v, dt_v, dtab, ftab, dk, fall, foth, dbuf, hbuf, snd, rcv, fin, fsnd,
    bsend, brecv, bown, ps, rsb, rsend2, rrecv2, lhs, rhs, psh, prb, pjs, pjb, ptt,
    pdc, pdb, pdt, dall, fitall, score, wt, a2t, nbuf, wbuf,
    in_s, bx_s, bx_r, r1_s, r1_r, ag_s, ag_r, ah_s, ah_r, bf_s, bf_r, pr_s, pr_r, pj_s, pj_r,
    ft_s, ft_r, ft2_s, ft2_r, ys, yr, yloc, xo_s, xf_s, x_r, ds_s, ds_r, rs_s, rs_r, fs_s, fs_r,
    pd_s, pd_r, f_s, f_r, ff_s, ff_r, d_s, d_r, q_s, q_r,
):
    x, yh, c, z, yl = [lax.axis_index(a) for a in AX]
    y = 2 * yh + yl
    p = 2 * x + yh
    me = at(x, yh, c, z, yl)
    partner = at(x, yh, 1 - c, z, yl)
    ypart = at(x, 1 - yh, c, z, yl)
    pending = []

    def rc(src, dst, ss, rs, dev):
        return pltpu.make_async_remote_copy(
            src_ref=src, dst_ref=dst, send_sem=ss, recv_sem=rs, device_id=dev, device_id_type=MESH
        )

    def send(src, dst, ss, rs, dev):
        d = rc(src, dst, ss, rs, dev)
        d.start()
        pending.append(d.wait_send)

    def recv(dst, rs):
        rc(dst, dst, rs, rs, partner).wait_recv()

    loads = [
        (gw_hbm, w_v.at[0]), (uw_hbm, w_v.at[1]), (pt_hbm, pt_v), (ftab_hbm, ftab), (dtab_hbm, dtab),
        (dt_hbm, dt_v), (seeds_hbm, seeds), (fit_hbm, fit),
    ]
    loads = [pltpu.make_async_copy(a, b, in_s.at[i]) for i, (a, b) in enumerate(loads)]
    for i in (5, 2, 0, 1, 6, 7, 3, 4):
        loads[i].start()

    def plane(rel):
        ny = rem(y + rel % 4, 4)
        return at(rem(x + rel // 4, 4), ny // 2, c, z, rem(ny, 2))

    def mate(rel):
        q = rem(p + rel // 2, 8)
        return at(q // 2, rem(q, 2), rem(c + rel % 2, 2), z, yl)

    def column(rel):
        return at(x, rem(yh + rel // 8, 2), c, rem(z + rel % 8, 8), yl)

    ypeers = [at(x, h, yl, z, c) for h in range(2)]
    me_y = [(h == yh) & (c == yl) for h in range(2)]
    barrier = pltpu.get_barrier_semaphore()

    def greet(dev):
        pl.semaphore_signal(barrier, inc=1, device_id=dev, device_id_type=MESH)

    peers = [column(r) for r in (4, 12, 3, 5, 11, 13, 2, 6, 10, 14, 1, 7, 9, 15)]
    peers += [mate(r) for r in range(15, 0, -1)] + [plane(1), plane(3)]
    for o in peers:
        greet(o)
    @pl.when(c != yl)
    def _():
        for h in range(2):
            greet(ypeers[h])

    def partial_base(k):
        return tn(w_v[k], pt_v[...])

    n_peers = len(peers)
    @pl.when(c == yl)
    def _():
        pl.semaphore_wait(barrier, n_peers)

    @pl.when(c != yl)
    def _():
        pl.semaphore_wait(barrier, n_peers + 2)

    e, kz = rem(z, 2), z // 2

    def low(x0):
        m = rem(x0 - kz + 4, 4)
        return jnp.where(e == 0, jnp.where(m == 1, 0, 1), jnp.where(m == 3, 1, 0))

    def zblk(r, ab):
        x0 = rem(x - r + 4, 4)
        return 2 * x0 + (low(x0) if ab == 0 else 1 - low(x0))

    own_a = low(x)

    def half(b, part):
        return b.at[pl.ds(80 * part, 80)]

    def ycopy(h, part):
        dst = half(dbuf.at[yl, 2 * x + yh], part)
        return rc(half(dt_hbm.at[h], part), dst, ys.at[h, part], yr.at[yh, part], ypeers[h])

    def ylocal(h, part):
        return pltpu.make_async_copy(half(dt_hbm.at[h], part), half(dbuf.at[yl, 2 * x + yh], part), yloc.at[part])

    def ysend(ab, part):
        mine = yh == (own_a if ab == 0 else 1 - own_a)
        for h in range(2):
            @pl.when(mine & jnp.logical_not(me_y[h]))
            def _():
                ycopy(h, part).start()
            @pl.when(mine & me_y[h])
            def _():
                ylocal(h, part).start()

    def wait_y(ab, part):
        w = own_a if ab == 0 else 1 - own_a
        here = (w == yh) & (c == yl)

        @pl.when(jnp.logical_not(here))
        def _():
            recv(half(dbuf.at[c, 2 * x + w], part), yr.at[w, part])

        @pl.when(here)
        def _():
            ylocal(0, part).wait()

    def y_drain():
        for h in range(2):
            @pl.when(jnp.logical_not(me_y[h]))
            def _():
                for part in range(2):
                    ycopy(h, part).wait_send()

    pending.append(y_drain)
    xnb = [at(rem(x + 1, 4), yh, c, z, yl), at(rem(x + 3, 4), yh, c, z, yl)]

    def dsend(r, ab, part):
        b = half(dbuf.at[c, zblk(r, ab)], part)
        d = rc(b, b, ds_s.at[r, ab, part], ds_r.at[r, ab, part], partner)
        pending.append(d.wait_send)
        return d

    def own_x(ab, part):
        b = dbuf.at[c, zblk(0, ab)]
        dsend(0, ab, part).start()
        b = half(b, part)
        send(b, b, xo_s.at[0, ab, part], x_r.at[1, ab, part], xnb[0])
        send(b, b, xo_s.at[1, ab, part], x_r.at[3, ab, part], xnb[1])

    def taker(r, ab):
        b = dbuf.at[c, zblk(r, ab)]
        d2 = [dsend(r, ab, part) for part in range(2)]
        fwd = c == (0 if r == 1 else 1)
        hops = []
        for part in range(2 if r != 2 else 0):
            h = half(b, part)
            d = rc(h, h, xf_s.at[r, ab, part], x_r.at[2, ab, part], xnb[0 if r == 1 else 1])
            hops.append(d)
            pending.append(functools.partial(pl.when(fwd), d.wait_send))

        def run(part):
            recv(half(b, part), x_r.at[r, ab, part])
            if r != 2:
                pl.when(fwd)(hops[part].start)
            d2[part].start()

        return run

    take = {(r, ab): taker(r, ab) for r in (1, 3, 2) for ab in range(2)}

    def take_d(r, ab):
        for part in range(2):
            recv(half(dbuf.at[1 - c, zblk(r, ab)], part), ds_r.at[r, ab, part])

    toks = pl.ds(pl.multiple_of(16 * z, 16), 16)
    own_row = 4 * yh + x
    def bpiece(t, k, first, rows):
        return lhs.at[t, k, pl.ds(pl.multiple_of(112 * first, 16), rows), pl.ds(0, 128)]

    along_x = [at(rem(x + r, 4), yh, c, z, yl) for r in range(4)]
    along_y = [at(x, rem(y + r, 4) // 2, c, z, rem(y + r, 2)) for r in range(4)]
    stage1, stage2, got1, got2 = [], [], [], []
    for r in range(1, 4):
        b = bpiece(yl, c, own_row, 112)
        stage1.append((rc(b, b, ag_s.at[r], ag_r.at[r], along_x[r]), rc(b, b, ag_s.at[r], ag_r.at[r], along_y[r])))
        xx, yy = rem(x - r + 4, 4), rem(y - r + 4, 4)
        got1.append((bpiece(yl, c, 4 * yh + xx, 112), bpiece(rem(yy, 2), c, 4 * (yy // 2) + x, 112)))
        b = bpiece(yl, c, 4 * yh, 448)
        far = []
        for n in range(4):
            f = bpiece(n // 2, c, 4 * (n % 2) + x, 112)
            far.append(rc(f, f, ah_s.at[r, n], ah_r.at[r, n], along_x[r]))
        stage2.append(([rc(b, b, ah_s.at[r, 0], ah_r.at[r, 0], along_y[r])], far))
        got2.append((
            [bpiece(rem(yy, 2), c, 4 * (yy // 2), 448)],
            [bpiece(n // 2, c, 4 * (n % 2) + xx, 112) for n in range(4)],
        ))

    def by_core(f):
        for core in range(2):
            @pl.when(c == core)
            def _():
                f(core)

    def ag_one(core):
        for d in stage1:
            d[core].start()

    def ag_two(core):
        for g, r in zip(got1, range(1, 4)):
            recv(g[core], ag_r.at[r])
        for ds in stage2:
            for d in ds[core]:
                d.start()

    def ag_end(core):
        for g, r in zip(got2, range(1, 4)):
            for n, b in enumerate(g[core]):
                recv(b, ah_r.at[r, n])

    def ag_drain(core):
        for d in stage1:
            d[core].wait_send()
        for ds in stage2:
            for d in ds[core]:
                d.wait_send()

    pending.append(lambda: by_core(ag_drain))
    fteam = [(1, 0), (1, 1), (0, 1)]

    def fdev(i):
        dh, dl = fteam[i]
        return at(x, rem(yh + dh, 2), c, z, rem(yl + dl, 2))

    def fdst(i, ks):
        return fall.at[ks, c, p] if fteam[i][1] == 0 else foth.at[yh, ks]

    def frcv(i, ks):
        dh, dl = fteam[i]
        return fall.at[ks, c, p + 1 - 2 * yh] if dl == 0 else foth.at[rem(yh + dh, 2), ks]

    gu, down = pl.ds(0, 2), pl.ds(2, 1)
    def factors_in(own, where):
        for i in where:
            recv(frcv(i, gu), ft_r.at[i])
        g = yh if own else 1 - yh
        for k in range(2):
            lanes = pl.ds(160 if own else 128, 32)
            lhs[yl, k, pl.ds(0, FB), lanes] = fall[k, c, 2 * x + g].T
            lhs[1 - yl, k, pl.ds(0, FB), lanes] = foth[g, k].T

    rowm = lax.broadcasted_iota(jnp.int32, (32, 256), 0) // 4
    lanem = lax.broadcasted_iota(jnp.int32, (32, 256), 1) // 128

    def hidden_rows():
        for i in range(8):
            g, cc = i // 4, i % 4
            for k in range(2):
                for gg in range(2):
                    of = yh if gg == 1 else 1 - yh
                    v = jnp.concatenate([ptt[of, k]] * 2, axis=1)
                    live = (rowm == 2 * cc + lanem) & (g == of)
                    rhs[i, k, pl.ds(128 + 32 * gg, 32)] = jnp.where(live, v, 0.0).astype(BF)

    def hidden(i):
        def rows(rb, _):
            r = pl.ds(pl.multiple_of(rb * HR, 16), HR)
            for t in range(2):
                ga = nn(lhs[t, 0, r], rhs[i, 0])
                up = nn(lhs[t, 1, r], rhs[i, 1])
                hbuf[i, t, r] = ((ga + ga * jnp.tanh(ga)) * up).astype(BF)
            return 0

        lax.fori_loop(0, FB // HR, rows, 0, unroll=HU)

    def chunk(j):
        return rem(j + 4 * (1 - yh), 8)

    sgn = 1 - 2 * c
    zn = rem(z + sgn + 8, 8)
    znd = at(x, yh, c, zn, yl)

    def part(d, i):
        return nn(dbuf[0, d], hbuf[i, 0]) + nn(dbuf[1, d], hbuf[i, 1])

    d0 = rem(z - sgn + 8, 8)

    def rsend(s, i, src):
        return rc(src, rcv.at[s, i], rs_s.at[s, i], rs_r.at[s, i], znd)


    def local_rows():
        for i in (6, 7, 3):
            loads[i].wait()
        for k in range(3):
            for m in range(8):
                fall[k, c, p, pl.ds(4 * m, 4)] = ftab[seeds[m], k]
        loads[4].wait()
        for k in range(3):
            for m in range(8):
                dk[k, pl.ds(4 * m, 4)] = dtab[seeds[m], k]

        eye = lax.broadcasted_iota(jnp.int32, (128, 256), 0) == rem(lax.broadcasted_iota(jnp.int32, (128, 256), 1), 128)
        for k in range(2):
            for i in range(8):
                rhs[i, k, 0:128] = jnp.where(eye, 1.0, 0.0).astype(BF)
            for t in range(2):
                lhs[t, k, :, pl.ds(128, 64)] = jnp.zeros((896, 64), BF)

    def base_half():
        for i in (0, 1, 2, 5):
            loads[i].wait()
        bsend[pl.ds(0, FB)] = partial_base(1 - c).astype(BF)
        bsend[pl.ds(FB, 32)] = jnp.zeros((32, 128), BF)
        send(bsend, brecv, bx_s, bx_r, partner)

    def base_scatter():
        bown[pl.ds(0, FB)] = partial_base(c)
        bown[pl.ds(FB, 32)] = jnp.zeros((32, 128), F32)
        recv(brecv, bx_r)
        for q in range(8):
            rows = pl.ds(112 * q, 112)
            ps[q // 4, q % 4] = (bown[rows] + brecv[rows].astype(F32)).astype(BF)
        for r in range(1, 4):
            xx = rem(x + r, 4)
            send(ps.at[:, xx], rsb.at[r], r1_s.at[r], r1_r.at[r], at(xx, yh, c, z, yl))

    def own_sum(h):
        mid = pl.ds(pl.multiple_of(112 * (4 * h + x), 16), 112)
        s = bown[mid] + brecv[mid].astype(F32)
        for r in range(1, 4):
            s += rsb[r, h].astype(F32)
        return s

    def base_mid():
        for r in range(1, 4):
            recv(rsb.at[r], r1_r.at[r])
        rsend2[...] = own_sum(1 - yh).astype(BF)
        send(rsend2, rrecv2, r1_s.at[0], r1_r.at[0], ypart)

    def base_sum():
        recv(rrecv2, r1_r.at[0])
        s = own_sum(yh) + rrecv2[...].astype(F32)
        s = jnp.where(c == 0, s * 0.5, s)
        bpiece(yl, c, own_row, 112)[...] = s.astype(BF)
        by_core(ag_one)

    def base_on():
        by_core(ag_two)

    def base_end():
        by_core(ag_end)
        send(lhs.at[:, c, :, pl.ds(0, 128)], lhs.at[:, c, :, pl.ds(0, 128)], bf_s, bf_r, partner)

    def base_other():
        recv(lhs.at[:, 1 - c, :, pl.ds(0, 128)], bf_r)

    def prompt_out():
        ptr = pt_v[...].astype(F32).T.astype(BF)
        psh[...] = jnp.zeros_like(psh)

        @pl.when(c == 0)
        def _():
            psh[:, 0:320] = ptr

        @pl.when(c == 1)
        def _():
            psh[:, 64:384] = ptr

        prb[c, p] = psh[toks]
        for r in range(1, 8):
            send(prb.at[c, p], prb.at[c, p], pr_s.at[r], pr_r.at[r], mate(2 * r))

    def prompt_on():
        for r in range(1, 8):
            recv(prb.at[c, rem(p - r + 8, 8)], pr_r.at[r])
        send(prb.at[c], prb.at[c], pr_s.at[0], pr_r.at[0], partner)

    def project():
        recv(prb.at[1 - c], pr_r.at[0])

        def proj_of(n, acc):
            cc, q = n // 8, rem(n, 8)
            lanes = pl.ds(pl.multiple_of(640 * q + 256 * cc, 128), 384)
            return acc + nt(prb[cc, q], dk[0:2, :, lanes].reshape(64, 384))

        acc = lax.fori_loop(0, 16, proj_of, jnp.zeros((16, 64), F32), unroll=4)
        acc = (acc / math.sqrt(D)).astype(BF).astype(F32)
        kk = lax.broadcasted_iota(jnp.int32, (16, 64), 1) // 32
        acc = jnp.where(kk == 0, acc * 0.25, acc * 0.5)
        pjs[...] = jnp.zeros_like(pjs)
        pjs[:, 0:64] = acc.astype(BF)
        pjb[yh, toks] = pjs[...]
        for r in range(1, 16):
            send(pjs, pjb.at[yh, toks], pj_s.at[r], pj_r.at[r], column(r))


    def project_in():
        for r in range(1, 16):
            hz, zz = rem(yh + r // 8, 2), rem(z - r % 8 + 8, 8)
            recv(pjb.at[hz, pl.ds(pl.multiple_of(16 * zz, 16), 16)], pj_r.at[r])
        for g in range(2):
            ptt[g] = pjb[g].astype(F32).T[0:64].reshape(2, 32, 128)
        hidden_rows()

    def y_first():
        ysend(0, 0)

    def y_first_b():
        ysend(0, 1)

    def y_second():
        ysend(1, 0)

    def y_second_b():
        ysend(1, 1)

    def x_first():
        wait_y(0, 0)
        own_x(0, 0)

    def x_first_b():
        wait_y(0, 1)
        own_x(0, 1)

    def x_second():
        wait_y(1, 0)
        own_x(1, 0)

    def x_second_b():
        wait_y(1, 1)
        own_x(1, 1)

    def down_out():
        send(fall.at[down, c, p], fdst(2, down), ft2_s.at[0], ft2_r.at[0], fdev(2))
        send(fall.at[down, c, p], fdst(0, down), ft2_s.at[1], ft2_r.at[1], fdev(0))

    def take_first():
        take[1, 0](0)
        take[3, 0](0)

    def take_first_b():
        take[1, 0](1)
        take[3, 0](1)

    def take_second():
        take[1, 1](0)
        take[3, 1](0)

    def take_second_b():
        take[1, 1](1)
        take[3, 1](1)

    def take_first_far():
        for part in range(2):
            take[2, 0](part)

    def first_in():
        for r in range(4):
            take_d(r, 0)

    def take_second_far():
        take[2, 1](0)

    def take_second_far_b():
        take[2, 1](1)

    def second_in():
        for r in range(4):
            take_d(r, 1)

    def factors_far():
        send(fall.at[gu, c, p], fdst(0, gu), ft_s.at[0], ft_r.at[0], fdev(0))

    def factors_diag():
        send(fall.at[gu, c, p], fdst(1, gu), ft_s.at[1], ft_r.at[1], fdev(1))

    def factors_near():
        send(fall.at[gu, c, p], fdst(2, gu), ft_s.at[2], ft_r.at[2], fdev(2))

    def factors_far_in():
        factors_in(False, (0, 1))

    def factors_near_in():
        factors_in(True, (2,))

    def hidden_ahead():
        def ahead(j, _):
            hidden(chunk(j))
            return 0

        lax.fori_loop(0, LEAD, ahead, 0)

    steps = dict(
        local_rows=local_rows, down_out=down_out,
        base_half=base_half, base_scatter=base_scatter, base_mid=base_mid, base_sum=base_sum, base_on=base_on, base_end=base_end,
        base_other=base_other, prompt_out=prompt_out, prompt_on=prompt_on, project=project,
        project_in=project_in, y_first=y_first, y_second=y_second, y_first_b=y_first_b, y_second_b=y_second_b, x_first=x_first, x_second=x_second, x_first_b=x_first_b, x_second_b=x_second_b,
        take_first=take_first, take_first_b=take_first_b, take_second_b=take_second_b, take_second=take_second, take_first_far=take_first_far, first_in=first_in,
        factors_far=factors_far, factors_diag=factors_diag, factors_near=factors_near, factors_far_in=factors_far_in,
        factors_near_in=factors_near_in, hidden_ahead=hidden_ahead,
    )
    for name in ORDER:
        steps[name]()

    def step_zero(j):
        i = chunk(j)
        snd[i] = part(d0, i).astype(BF)
        rsend(0, i, snd.at[i]).start()

    def first(j, _):
        i = chunk(j)
        p0 = part(d0, i).astype(BF)
        hidden(chunk(j + 1))
        snd[i] = p0
        rsend(0, i, snd.at[i]).start()
        pl.when(j == TB)(take_second)
        pl.when(j == TB2)(take_second_b)
        if TF <= 6:
            pl.when(j == TF)(take_second_far)
        if TF2 <= 6:
            pl.when(j == TF2)(take_second_far_b)
        return 0

    lax.fori_loop(0, 7, first, 0)
    if TF > 6:
        take_second_far()
    step_zero(7)
    if TF2 > 6:
        take_second_far_b()

    recv(frcv(0, down), ft2_r.at[1])

    def fpiece(i, other):
        return fall.at[:, c, 2 * rem(x - i + 4, 4) + (1 - yh if other else yh)]

    f_out, f_on = [], []
    for i in range(1, 4):
        f_out.append([rc(fpiece(0, h), fpiece(0, h), f_s.at[4 * h + i], f_r.at[4 * h + i], along_x[i]) for h in range(2)])
        f_on.append(rc(fpiece(i, 0), fpiece(i, 0), f_s.at[4 + i], f_r.at[4 + i], ypart))

    def factors_out(core):
        for d in f_out:
            for h in range(1 + core):
                d[h].start()

    def factors_drain(core):
        for d in f_out:
            for h in range(1 + core):
                d[h].wait_send()
        if core == 0:
            for d in f_on:
                d.wait_send()

    by_core(factors_out)
    pending.append(lambda: by_core(factors_drain))
    for m in range(8):
        fitall[c, p, pl.ds(m, 1)] = jnp.full((1, 128), fit[m], F32)

    def dlanes(q):
        return pl.ds(pl.multiple_of(640 * q, 128), 640)

    dall[:, c, p] = dk[:, :, dlanes(p)]
    for r in range(1, 8):
        q = rem(p + r, 8)
        send(dk.at[:, :, dlanes(q)], dall.at[:, c, p], d_s.at[r], d_r.at[r], mate(2 * r))
        send(fitall.at[c, p], fitall.at[c, p], q_s.at[r], q_r.at[r], mate(2 * r))

    second_in()

    fwd_f = rc(fall.at[:, c], fall.at[:, c], ff_s, ff_r, partner)
    pending.append(fwd_f.wait_send)

    def factors_on():
        @pl.when(c == 0)
        def _():
            for i in range(1, 4):
                recv(fpiece(i, 0), f_r.at[i])
            for d in f_on:
                d.start()

    def collect_f():
        @pl.when(c == 1)
        def _():
            for i in range(1, 4):
                recv(fpiece(i, 0), f_r.at[i])

        for i in range(1, 4):
            recv(fpiece(i, 1), f_r.at[4 + i])
        fwd_f.start()

    d_on = rc(dall.at[:, c], dall.at[:, c], d_s.at[0], d_r.at[0], partner)
    q_on = rc(fitall.at[c], fitall.at[c], q_s.at[0], q_r.at[0], partner)
    pending.extend([d_on.wait_send, q_on.wait_send])

    def factors_d_on():
        for r in range(1, 8):
            q = rem(p - r + 8, 8)
            recv(dall.at[:, c, q], d_r.at[r])
            recv(fitall.at[c, q], q_r.at[r])
        d_on.start()
        q_on.start()

    def collect_d():
        recv(dall.at[:, 1 - c], d_r.at[0])
        recv(fitall.at[1 - c], q_r.at[0])
        fv = fitall[...].reshape(128, 128)
        mean = jnp.sum(fv, axis=0, keepdims=True) / 128
        spread = jnp.sum((fv - mean) ** 2, axis=0, keepdims=True) / 128
        sc = (fv - mean) / jnp.sqrt(spread + 1.0)
        for i in range(16):
            v = jnp.broadcast_to(sc[8 * i : 8 * i + 8].reshape(8, 1, 128), (8, 4, 128))
            score[i // 8, i % 8] = v.reshape(32, 128)

    def weigh(k):
        def one(g, _):
            a, b = g // 8, rem(g, 8)
            sc = score[a, b]
            own = pl.ds(pl.multiple_of(256 * c, 128), 384)
            w = dall[k, a, b, :, own].astype(F32) * jnp.concatenate([sc] * 3, axis=1)
            wbuf[g] = w.astype(BF)
            return 0
        lax.fori_loop(0, 16, one, 0)
        wt[k] = wbuf[...].reshape(512, 384).T

    def delta(k, half):
        r = pl.ds(pl.multiple_of(64 * c + 160 * half, 16), 160)
        v = nn(wt[k, r], fall[k].reshape(512, FB)) * (1.0 / math.sqrt(512))
        del_ref[k, pl.ds(pl.multiple_of(160 * half, 16), 160)] = v.astype(BF)

    flips = [z + 1 - 2 * rem(z, 2), z + 2 - 4 * rem(z // 2, 2), z + 4 - 8 * (z // 4)]
    pd_out = [rc(pdc.at[k], pdb.at[k], pd_s.at[k], pd_r.at[k], at(x, yh, c, f, yl)) for k, f in enumerate(flips)]
    pending.extend(d.wait_send for d in pd_out)

    def down_sum(k):
        recv(pdb.at[k], pd_r.at[k])
        tot = pdc[k].astype(F32) + pdb[k].astype(F32)
        pdc[k + 1] = tot.astype(BF)
        pd_out[k + 1].start()

    def down_sums():
        recv(frcv(2, down), ft2_r.at[0])
        tot = jnp.zeros((32, 128), F32)
        for cc in range(4):
            i = 4 * yh + cc
            q = nn(fall[2, c, p], hbuf[i, yl]) + nn(foth[yh, 2], hbuf[i, 1 - yl])
            q = jnp.where(rowm == 2 * cc + lanem, q, 0.0)
            tot += q[:, :128] + q[:, 128:]
        pdc[0] = tot.astype(BF)
        pd_out[0].start()


    def noise_in():
        recv(pdb.at[2], pd_r.at[2])
        tot = pdc[2].astype(F32) + pdb[2].astype(F32)
        pdt[...] = (tot / math.sqrt(FFW)).astype(BF).astype(F32) * 0.5
        a2t[...] = dk[2, :, pl.ds(pl.multiple_of(640 * z + 256 * yl, 128), 384)].T

    def noise(j):
        live = rowm == 2 * j + lanem
        pm = jnp.where(live, jnp.concatenate([pdt[...]] * 2, axis=1), 0.0).astype(BF)
        for h in range(2):
            nbuf[h, j] = nn(a2t[pl.ds(pl.multiple_of(64 * yl + 160 * h, 16), 160)], pm)

    def place(n):
        m = n - 12
        late = jnp.where(rem(m + 16, 8) >= 4, 1, 0)
        s = jnp.where(n < 8, 1, jnp.where(n < 12, 2, jnp.where(n < 44, 3 + m // 8 - late, 6)))
        j = jnp.where(n < 8, n, jnp.where(n < 12, n - 8, jnp.where(n < 44, rem(m + 16, 8), n - 40)))
        return s, j

    def middle(n, _):
        s, j = place(n)
        i = chunk(j)
        pp = part(rem(z - sgn * (1 + s) + 16, 8), i)
        recv(rcv.at[s - 1, i], rs_r.at[s - 1, i])
        rcv[s - 1, i] = (pp + rcv[s - 1, i].astype(F32)).astype(BF)
        rsend(s, i, rcv.at[s - 1, i]).start()
        rsend(s - 1, i, rcv.at[s, i]).wait_send()

        @pl.when(n == PN)
        def _():
            down_sums()

        for k in range(2):
            pl.when(n == PN + 8 * (k + 1))(functools.partial(down_sum, k))

        @pl.when(n == NI)
        def _():
            noise_in()

        @pl.when((n > NI) & (n <= NI + 4))
        def _():
            noise(n - NI - 1)

        @pl.when(n == FX)
        def _():
            factors_on()

        @pl.when(n == CF)
        def _():
            collect_f()

        @pl.when(n == DX)
        def _():
            factors_d_on()

        m = n - CD

        @pl.when(m == 0)
        def _():
            collect_d()

        @pl.when((m >= 1) & (m < 4))
        def _():
            weigh(m - 1)

        @pl.when(m == 3)
        def _():
            recv(fall.at[:, 1 - c], ff_r)

        @pl.when((m >= 4) & (m < 4 + 6 * DS) & (rem(m, DS) == 0))
        def _():
            q = (m - 4) // DS
            delta(q // 2, rem(q, 2))

        @pl.when(n == 43)
        def _():
            for w in pending:
                w()

        return 0

    lax.fori_loop(0, 44, middle, 0)

    def last(j):
        i = chunk(j)
        pp = part(z, i)
        recv(rcv.at[6, i], rs_r.at[6, i])
        return pp + rcv[6, i].astype(F32)

    def last_far(j, _):
        fsnd[j] = last(j).astype(BF)
        rc(fsnd.at[j], fin.at[j], fs_s.at[j], fs_r.at[j], ypart).start()

        return 0

    lax.fori_loop(0, 4, last_far, 0)
    lax.fori_loop(44, 48, middle, 0)

    def put(j, h, w):
        for m in range(2):
            out_ref[2 * j + m, pl.ds(pl.multiple_of(160 * h, 16), 160)] = w[:, 128 * m : 128 * (m + 1)].astype(BF)

    def last_near(j, _):
        put(j, yh, last(j + 4) + nbuf[yh, j])
        return 0

    lax.fori_loop(0, 4, last_near, 0)

    def finish(j, _):
        rc(fsnd.at[j], fin.at[j], fs_s.at[j], fs_r.at[j], ypart).wait()
        put(j, 1 - yh, fin[j].astype(F32) + nbuf[1 - yh, j])
        return 0

    lax.fori_loop(0, 4, finish, 0)

    def drain(i, _):
        rsend(6, i, snd.at[i]).wait_send()
        return 0

    lax.fori_loop(0, 8, drain, 0)


def call_step(*arrays):
    arrays = [pltpu.with_memory_space_constraint(v, pltpu.HBM) for v in arrays]
    v = pl.BlockSpec(memory_space=pltpu.VMEM)
    a = pl.BlockSpec(memory_space=pltpu.HBM)
    dma = pltpu.SemaphoreType.DMA
    vm = pltpu.VMEM
    return pl.pallas_call(
        step_kernel,
        out_shape=[
            jax.ShapeDtypeStruct((8, 320, 128), BF),
            jax.ShapeDtypeStruct((3, 320, FB), BF),
        ],
        in_specs=[a] * 8,
        out_specs=[v, v],
        scratch_shapes=[
            pltpu.SMEM((8,), jnp.int32), pltpu.SMEM((8,), F32),
            vm((320, 128), BF), vm((2, 320, FB), BF), vm((2, 160, FB), BF), vm((16, 3, 4, D), BF), vm((16, 3, 4, FB), BF),
            vm((3, 32, D), BF), vm((3, 2, 8, 32, FB), BF), vm((2, 3, 32, FB), BF),
            vm((2, 8, 160, FB), BF), vm((8, 2, FB, 256), BF), vm((8, 160, 256), BF),
            vm((7, 8, 160, 256), BF), vm((4, 160, 256), BF), vm((4, 160, 256), BF),
            vm((896, 128), BF), vm((896, 128), BF), vm((896, 128), F32), vm((2, 4, 112, 128), BF),
            vm((4, 2, 112, 128), BF), vm((112, 128), BF), vm((112, 128), BF), vm((2, 2, 896, 192), BF), vm((8, 2, 192, 256), BF),
            vm((128, 384), BF), vm((2, 8, 16, 384), BF), vm((16, 128), BF), vm((2, 128, 128), BF),
            vm((2, 2, 32, 128), F32),
            vm((3, 32, 128), BF), vm((3, 32, 128), BF), vm((32, 128), F32), vm((3, 2, 8, 32, 640), BF),
            vm((2, 8, 8, 128), F32), vm((2, 8, 32, 128), F32), vm((3, 384, 512), BF), vm((384, 32), BF), vm((2, 4, 160, 256), F32), vm((16, 32, 384), BF),
            dma((8,)), dma(()), dma(()), dma((8,)), dma((8,)), dma((4,)), dma((4,)), dma((4, 4)), dma((4, 4)), dma(()), dma(()),
            dma((8,)), dma((8,)), dma((16,)), dma((16,)),
            dma((3,)), dma((3,)), dma((2,)), dma((2,)), dma((2, 2)), dma((2, 2)), dma((2,)), dma((2, 2, 2)), dma((4, 2, 2)), dma((4, 2, 2)),
            dma((4, 2, 2)), dma((4, 2, 2)), dma((7, 8)), dma((7, 8)), dma((4,)), dma((4,)),
            dma((8,)), dma((8,)), dma((8,)), dma((8,)), dma(()), dma(()), dma((16,)), dma((16,)),
            dma((16,)), dma((16,)),
        ],
        compiler_params=pltpu.CompilerParams(
            collective_id=0, has_side_effects=True, vmem_limit_bytes=44 << 20
        ),
        name="es_step",
    )(*arrays)


EMIT_LIM = 4 << 20


def emit_kernel(out, deltas, o_hbm, g_hbm, u_hbm, d_hbm, sems):
    pairs = [(deltas.at[0], g_hbm), (deltas.at[1], u_hbm), (deltas.at[2], d_hbm), (out, o_hbm)]
    copies = [pltpu.make_async_copy(a, b, sems.at[i]) for i, (a, b) in enumerate(pairs)]
    for d in copies:
        d.start()
    for d in copies:
        d.wait()


def emit(out, deltas):
    v = pl.BlockSpec(memory_space=pltpu.VMEM)
    a = pl.BlockSpec(memory_space=pltpu.HBM)
    one = jax.ShapeDtypeStruct((320, FB), BF)
    return pl.pallas_call(
        emit_kernel,
        out_shape=[jax.ShapeDtypeStruct((8, 320, 128), BF), one, one, one],
        in_specs=[v, v],
        out_specs=[a, a, a, a],
        scratch_shapes=[pltpu.SemaphoreType.DMA((4,))],
        compiler_params=pltpu.CompilerParams(vmem_limit_bytes=EMIT_LIM),
        name="emit",
    )(out, deltas)


def shards(prompt_acts, gate_weight, up_weight, down_weight, d_table, f_table, seeds, fitness):
    out, deltas = call_step(
        prompt_acts.T, gate_weight, up_weight, down_weight.T.reshape(2, 160, FB), d_table, f_table,
        seeds, fitness,
    )
    out, dg, du, dd = emit(out, deltas)
    return out.transpose(0, 2, 1), dg, du, dd.T


def solution(mesh):
    split = Mesh(mesh.devices.reshape(4, 2, 2, 8, 2), AX)
    placed = (
        P(None, MEMBER), P(MEMBER, TENSOR), P(MEMBER, TENSOR), P(TENSOR, MEMBER),
        P(MEMBER, None, None, None), P(MEMBER, None, None, TENSOR), P(MEMBER), P(MEMBER),
    )
    return jax.shard_map(
        shards, mesh=split, in_specs=placed,
        out_specs=(P(MEMBER, None, TENSOR), P(MEMBER, TENSOR), P(MEMBER, TENSOR), P(TENSOR, MEMBER)),
        check_vma=False,
    )
```
